16 devices in a mesh: rep: 4 (over y, z, core), dp: 4 (over x).
Axes of the slice: x: 4, y: 2, z: 1, core: 2. Of those that a mesh axis runs over, the one named last changes fastest.
The devices are a block of a 4x4x8 slice.
Arguments:
- x: bfloat16 [16, 4096, 768], P(('rep', 'dp')), parts along dimension 0
- dy: bfloat16 [16, 4096, 768], P(('rep', 'dp')), parts along dimension 0
- w_gate: bfloat16 [2, 768, 3072], replicated
- w_up: bfloat16 [2, 768, 3072], replicated
- w_down: bfloat16 [2, 3072, 768], replicated
- m_w_gate: float32 [2, 768, 3072], P(None, 'dp')
- m_w_up: float32 [2, 768, 3072], P(None, 'dp')
- m_w_down: float32 [2, 3072, 768], P(None, 'dp')
- v_w_gate: float32 [2, 768, 3072], P(None, 'dp')
- v_w_up: float32 [2, 768, 3072], P(None, 'dp')
- v_w_down: float32 [2, 3072, 768], P(None, 'dp')
Outputs:
- output 1: bfloat16 [8, 768, 3072], P('rep'), parts along dimension 0
- output 2: bfloat16 [8, 768, 3072], P('rep'), parts along dimension 0
- output 3: bfloat16 [8, 3072, 768], P('rep'), parts along dimension 0
- output 4: float32 [8, 768, 3072], P('rep', 'dp'), parts along dimension 0
- output 5: float32 [8, 768, 3072], P('rep', 'dp'), parts along dimension 0
- output 6: float32 [8, 3072, 768], P('rep', 'dp'), parts along dimension 0
- output 7: float32 [8, 768, 3072], P('rep', 'dp'), parts along dimension 0
- output 8: float32 [8, 768, 3072], P('rep', 'dp'), parts along dimension 0
- output 9: float32 [8, 3072, 768], P('rep', 'dp'), parts along dimension 0
There are 4 independent parts. The reference program is written for one: setup_inputs(seed, part) draws one part's arguments, and reference() takes and returns one part's arrays. A program takes and returns all parts, laid end to end along the dimension named above; an argument that names none is the same for every part.
All inputs are finite; a program needn't handle non-finite values.
Results may differ from the reference program's by a relative error of at most 0.022.
Values are sent between devices in bfloat16 or wider.
A program may use at most 768 MiB of HBM per device.

```python
import jax
import jax.numpy as jnp
from jax import lax

SEQUENCES = 4
TOKENS = 4096
D = 768
FF = 3072
LAYERS = 2
NAMES = ("w_gate", "w_up", "w_down")
SHAPES = {"w_gate": (LAYERS, D, FF), "w_up": (LAYERS, D, FF), "w_down": (LAYERS, FF, D)}


def bump(key, n, height):
    away = (jnp.arange(n, dtype=jnp.int32) - jax.random.randint(key, (), 0, n, jnp.int32)) % n
    return jnp.where(away < n // 8, height, 1.0)


def together(key, own, strength):
    shared = jax.random.normal(key, own.shape[1:], jnp.float32)
    return (own + strength * shared) * lax.rsqrt(1 + strength * strength)


def setup_inputs(seed: int = 0, part: int = 0) -> dict:
    kx, kdy, ka, kb, kz, kf, kh, kl, *keys = jax.random.split(jax.random.key(seed), 8 + 3 * len(NAMES))
    kx, kdy, ka, kb = (jax.random.fold_in(k, part) for k in (kx, kdy, ka, kb))
    kw, km, kv = (keys[i::3] for i in range(3))
    shape = (SEQUENCES, TOKENS, D)
    much_x, much_dy = jax.random.uniform(kz, (2,), jnp.float32, 0.0, 1.0)
    loud = 2.0 ** jax.random.uniform(jax.random.fold_in(kz, 1), (), jnp.float32, -1.0, 2.0)
    layers = 2.0 ** jax.random.uniform(kl, (LAYERS, 1, 1), jnp.float32, -1.0, 1.0)
    x = together(ka, jax.random.normal(kx, shape, jnp.float32), much_x) * bump(kf, D, 4.0)
    dy = together(kb, jax.random.normal(kdy, shape, jnp.float32), much_dy)
    drawn = {"x": x.astype(jnp.bfloat16), "dy": (loud * dy * (SEQUENCES * TOKENS) ** -0.5).astype(jnp.bfloat16)}
    for key, name in zip(kw, NAMES, strict=True):
        w = jax.random.normal(key, SHAPES[name], jnp.float32) * SHAPES[name][1] ** -0.5
        drawn[name] = (w * {"w_gate": 1.0, "w_up": bump(kh, FF, 4.0), "w_down": layers}[name]).astype(jnp.bfloat16)
    for key, name in zip(km, NAMES, strict=True):
        drawn[f"m_{name}"] = 0.1 * jax.random.normal(key, SHAPES[name], jnp.float32)
    for key, name in zip(kv, NAMES, strict=True):
        drawn[f"v_{name}"] = jax.random.uniform(key, SHAPES[name], jnp.float32, 0.005, 0.015)
    return drawn


def matmul(a, w):
    return jnp.dot(a, w, preferred_element_type=jnp.float32).astype(jnp.bfloat16)


def normed(h):
    wide = h.astype(jnp.float32)
    scale = lax.rsqrt(jnp.mean(wide**2, -1, keepdims=True) + 1e-6)
    return (wide * scale).astype(jnp.bfloat16)


def layer(h, w):
    a = normed(h)
    gate = jnp.dot(a, w["w_gate"], preferred_element_type=jnp.float32)
    up = jnp.dot(a, w["w_up"], preferred_element_type=jnp.float32)
    return h + matmul((jax.nn.silu(gate) * up).astype(jnp.bfloat16), w["w_down"])


def adamw(w, m, v, g):
    m = 0.9 * m + 0.1 * g
    v = 0.95 * v + 0.05 * g * g
    step = m * lax.rsqrt(v + 1e-8) + 0.1 * w
    return (w - 0.02 * step).astype(jnp.bfloat16), m, v


def clipped(gradients, sum_of_squares, count):
    factor = jnp.minimum(1.0, 0.5 * lax.rsqrt(sum_of_squares / count + 1e-30))
    return [g * factor for g in gradients]


def stack(weights, h):
    return lax.scan(lambda h, w: (layer(h, w), None), h, weights)[0]


def reference(x, dy, w_gate, w_up, w_down, m_w_gate, m_w_up, m_w_down, v_w_gate, v_w_up, v_w_down):
    weights = dict(zip(NAMES, (w_gate, w_up, w_down), strict=True))

    def take(so_far, sequence):
        h, by_y = sequence
        _, back = jax.vjp(lambda w: stack(w, h), weights)
        return jax.tree.map(lambda total, term: total + term.astype(jnp.float32), so_far, back(by_y)[0]), None

    none_yet = {name: jnp.zeros(w.shape, jnp.float32) for name, w in weights.items()}
    by_weights, _ = lax.scan(take, none_yet, (x, dy))
    gradients = [by_weights[name].astype(jnp.bfloat16).astype(jnp.float32) for name in NAMES]
    gradients = clipped(gradients, sum(jnp.sum(g * g) for g in gradients), sum(g.size for g in gradients))
    new = [
        adamw(w.astype(jnp.float32), m, v, g)
        for w, m, v, g in zip((w_gate, w_up, w_down), (m_w_gate, m_w_up, m_w_down), (v_w_gate, v_w_up, v_w_down), gradients, strict=True)
    ]
    return tuple(one[which] for which in range(3) for one in new)
```

```python
import functools

import jax
import jax.numpy as jnp
from jax import lax
from jax.experimental import pallas as pl
from jax.experimental.pallas import tpu as pltpu
from jax.sharding import PartitionSpec as P

F32, BF16 = jnp.float32, jnp.bfloat16
STRIPE = 256
VMEM_LIMIT = 60 << 20


def dot(a, b):
    return jnp.dot(a, b, preferred_element_type=F32)


def dot_nt(a, b):
    return lax.dot_general(a, b, (((1,), (1,)), ((), ())), preferred_element_type=F32)


def sigmoid(x):
    return 0.5 * jnp.tanh(0.5 * x) + 0.5


def normed(h):
    wide = h.astype(F32)
    scale = lax.rsqrt(jnp.mean(wide * wide, -1, keepdims=True) + 1e-6)
    return (wide * scale).astype(BF16)


def cost(flops, read_and_written):
    return pl.CostEstimate(flops=int(flops), bytes_accessed=int(read_and_written), transcendentals=0)


def params(**more):
    return pltpu.CompilerParams(vmem_limit_bytes=VMEM_LIMIT, **more)


def nbytes(*arrays):
    return sum(a.size * jnp.dtype(a.dtype).itemsize for a in arrays)


def once(shape, index_map):
    return pl.BlockSpec(shape, index_map, pipeline_mode=pl.Buffered(1))


def forward_kernel(chunks, width, x, dy, wg, wu, wd, *rest):
    gates, ups, (a_t, h1, a1, a1_t, dy_t, act) = rest[:chunks], rest[chunks : 2 * chunks], rest[2 * chunks :]
    ff = wg.shape[2]
    group = ff // chunks
    a = normed(x[...])
    a_t[...] = a.T
    dy_t[...] = dy[...].T
    for lo in range(0, ff, width):
        g, u = dot(a, wg[0, :, lo : lo + width]), dot(a, wu[0, :, lo : lo + width])
        act[:, lo : lo + width] = (g * sigmoid(g) * u).astype(BF16)
        for at in range(lo, lo + width, STRIPE):
            owner, c = divmod(at // STRIPE, chunks)
            to, fr = slice(owner * STRIPE, (owner + 1) * STRIPE), slice(at - lo, at - lo + STRIPE)
            gates[c][:, to] = g[:, fr]
            ups[c][:, to] = u[:, fr]
    y = dot(act[...], wd[0]).astype(BF16)
    h = (x[...].astype(F32) + y.astype(F32)).astype(BF16)
    h1[...] = h
    n = normed(h)
    a1[...] = n
    a1_t[...] = n.T


def forward(x, dy, w_gate, w_up, w_down, chunks, tm=512, width=512):
    t, d = x.shape
    ff = w_gate.shape[2]
    row, col = pl.BlockSpec((tm, d), lambda m: (m, 0)), pl.BlockSpec((d, tm), lambda m: (0, m))
    wide = pl.BlockSpec((tm, ff // chunks), lambda m: (m, 0))
    out = [jax.ShapeDtypeStruct((t, ff // chunks), F32)] * (2 * chunks) + [
        jax.ShapeDtypeStruct(s, BF16) for s in ((d, t), (t, d), (t, d), (d, t), (d, t))
    ]
    outs = pl.pallas_call(
        functools.partial(forward_kernel, chunks, width),
        grid=(t // tm,),
        in_specs=[row, row]
        + [once((1, d, ff), lambda m: (0, 0, 0))] * 2
        + [once((1, ff, d), lambda m: (0, 0, 0))],
        out_specs=[wide] * (2 * chunks) + [col, row, row, col, col],
        out_shape=out,
        scratch_shapes=[pltpu.VMEM((tm, ff), BF16)],
        compiler_params=params(),
        cost_estimate=cost(6 * t * d * ff, nbytes(*out)),
        name="forward",
    )(x, dy, w_gate, w_up, w_down)
    return outs[:chunks], outs[chunks : 2 * chunks], *outs[2 * chunks :]


def put_gradients(owners, gacc, uacc, dacc, to_right, to_left, own, right_a, left_b):
    me = lax.axis_index("dp")
    rows = gacc.shape[1] // owners
    half = own.shape[0] // 2
    for o in range(owners):
        turn = lax.rem(o - me + owners, owners)
        pieces = [(j * rows, gacc, j) for j in range(owners)]
        pieces += [((owners + j) * rows, uacc, j) for j in range(owners)]

        def put(ref_a, at_a, ref_b, at_b):
            def store(at, value):
                n = value.shape[0]
                if at + n <= half:
                    ref_a[at_a + at : at_a + at + n, :] = value
                else:
                    ref_b[at_b + at - half : at_b + at - half + n, :] = value

            for at, acc, j in pieces:
                store(at, acc[j, o * rows : (o + 1) * rows, :].astype(BF16))
            down = dacc[o].T.astype(BF16)
            base = 2 * owners * rows
            for q in range(down.shape[1] // STRIPE):
                store(base + q * STRIPE, down[:, q * STRIPE : (q + 1) * STRIPE])

        pl.when(turn == 0)(functools.partial(put, own, 0, own, half))
        pl.when(turn == 1)(functools.partial(put, right_a, 0, to_right, half))
        pl.when(turn == 2)(functools.partial(put, to_right, 0, to_left, 0))
        pl.when(turn == 3)(functools.partial(put, to_left, half, left_b, 0))


def backward_parts(g, u, dact):
    dact = dact.astype(BF16).astype(F32)
    s = sigmoid(g)
    silu = g * s
    act = (silu * u).astype(BF16)
    du = (dact * silu).astype(BF16)
    dg = (dact * u * (s + silu * (1 - s))).astype(BF16)
    return act, dg, du


def start_sums(*accs):
    @pl.when(pl.program_id(0) == 0)
    def _():
        for acc in accs:
            acc[...] = jnp.zeros_like(acc)


def last_step():
    return pl.when(pl.program_id(0) == pl.num_programs(0) - 1)


def top_kernel(owners, pair, a, a_t, dy, dy_t, *rest):
    wg, wu, wd = (rest[i * owners : (i + 1) * owners] for i in range(3))
    dg_out, du_out, *outs, gacc, uacc, dacc = rest[3 * owners :]
    start_sums(gacc, uacc, dacc)
    for j in range(0, owners, pair):
        js = range(j, j + pair)
        g = dot(a[...], jnp.concatenate([wg[k][0] for k in js], 1))
        u = dot(a[...], jnp.concatenate([wu[k][0] for k in js], 1))
        dact = dot_nt(dy[...], jnp.concatenate([wd[k][0] for k in js], 0))
        act, dg, du = backward_parts(g, u, dact)
        dg_out[:, j * STRIPE : (j + pair) * STRIPE] = dg
        du_out[:, j * STRIPE : (j + pair) * STRIPE] = du
        for acc, left, right in ((gacc, a_t, dg), (uacc, a_t, du), (dacc, dy_t, act)):
            both = dot(left[...], right)
            for i, k in enumerate(js):
                acc[k] += both[:, i * STRIPE : (i + 1) * STRIPE]
    last_step()(lambda: put_gradients(owners, gacc, uacc, dacc, *outs))


def bottom_kernel(owners, pair, a_t, dy, dy_t, gate, up, *rest):
    wd = rest[:owners]
    *outs, gacc, uacc, dacc = rest[owners:]
    start_sums(gacc, uacc, dacc)
    for j in range(0, owners, pair):
        js = range(j, j + pair)
        c = slice(j * STRIPE, (j + pair) * STRIPE)
        dact = dot_nt(dy[...], jnp.concatenate([wd[k][0] for k in js], 0))
        act, dg, du = backward_parts(gate[:, c], up[:, c], dact)
        for acc, left, right in ((gacc, a_t, dg), (uacc, a_t, du), (dacc, dy_t, act)):
            both = dot(left[...], right)
            for i, k in enumerate(js):
                acc[k] += both[:, i * STRIPE : (i + 1) * STRIPE]
    last_step()(lambda: put_gradients(owners, gacc, uacc, dacc, *outs))


def gradient_outs(owners, d):
    block = 3 * d
    shapes = [(block, STRIPE)] * 3 + [(block // 2, STRIPE)] * 2
    return [jax.ShapeDtypeStruct(s, BF16) for s in shapes], [once(s, lambda m: (0, 0)) for s in shapes]


def stripe_specs(owners, chunks, layer, c, d):
    across = [once((1, d, STRIPE), lambda m, j=j: (layer, 0, j * chunks + c)) for j in range(owners)]
    down = [once((1, STRIPE, d), lambda m, j=j: (layer, j * chunks + c, 0)) for j in range(owners)]
    return across, down


def top_gradients(owners, chunks, c, layer, a, a_t, dy, dy_t, w_gate, w_up, w_down, tm=1024, pair=2):
    t, d = a.shape
    width = owners * STRIPE
    row, col = pl.BlockSpec((tm, d), lambda m: (m, 0)), pl.BlockSpec((d, tm), lambda m: (0, m))
    wide = pl.BlockSpec((tm, width), lambda m: (m, 0))
    across, down = stripe_specs(owners, chunks, layer, c, d)
    shapes, specs = gradient_outs(owners, d)
    shapes = [jax.ShapeDtypeStruct((t, width), BF16)] * 2 + shapes
    dg, du, *outs = pl.pallas_call(
        functools.partial(top_kernel, owners, pair),
        grid=(t // tm,),
        in_specs=[row, col, row, col] + across + across + down,
        out_specs=[wide, wide] + specs,
        out_shape=shapes,
        scratch_shapes=[pltpu.VMEM((owners, d, STRIPE), F32)] * 3,
        compiler_params=params(),
        cost_estimate=cost(12 * t * d * width, nbytes(a, a_t, dy, dy_t, *shapes)),
        name="top_gradients",
    )(a, a_t, dy, dy_t, *[w_gate] * owners, *[w_up] * owners, *[w_down] * owners)
    return dg, du, outs


def bottom_gradients(owners, chunks, c, layer, a_t, dy, dy_t, gate, up, w_down, tm=512, pair=2):
    d, t = a_t.shape
    width = owners * STRIPE
    row, col = pl.BlockSpec((tm, d), lambda m: (m, 0)), pl.BlockSpec((d, tm), lambda m: (0, m))
    wide = pl.BlockSpec((tm, width), lambda m: (m, 0))
    _, down = stripe_specs(owners, chunks, layer, c, d)
    shapes, specs = gradient_outs(owners, d)
    return pl.pallas_call(
        functools.partial(bottom_kernel, owners, pair),
        grid=(t // tm,),
        in_specs=[col, row, col, wide, wide] + down,
        out_specs=specs,
        out_shape=shapes,
        scratch_shapes=[pltpu.VMEM((owners, d, STRIPE), F32)] * 3,
        compiler_params=params(),
        cost_estimate=cost(8 * t * d * width, nbytes(a_t, dy, dy_t, gate, up, *shapes)),
        name="bottom_gradients",
    )(a_t, dy, dy_t, gate, up, *[w_down] * owners)


def states_kernel(chunks, owners, h, dy, wg, wu, *rest):
    dgs, dus, (dh, dh_t) = rest[:chunks], rest[chunks : 2 * chunks], rest[2 * chunks :]

    def through(pieces, w):
        left = jnp.concatenate([p[...] for p in pieces], 1)
        at = [(j * chunks + c) * STRIPE for c in range(chunks) for j in range(owners)]
        right = jnp.concatenate([w[0, :, i : i + STRIPE] for i in at], 1)
        return dot_nt(left, right).astype(BF16).astype(F32)

    da = (through(dgs, wg) + through(dus, wu)).astype(BF16).astype(F32)
    wide = h[...].astype(F32)
    mean = jnp.mean(wide * wide, -1, keepdims=True) + 1e-6
    scale = lax.rsqrt(mean)
    dmean = jnp.sum(da * wide, -1, keepdims=True) * (-0.5 * scale / mean)
    back = (da * scale + wide * (dmean * (2.0 / wide.shape[1]))).astype(BF16)
    out = (dy[...].astype(F32) + back.astype(F32)).astype(BF16)
    dh[...] = out
    dh_t[...] = out.T


def states(owners, chunks, layer, h, dy, w_gate, w_up, dgs, dus, tm=512):
    t, d = h.shape
    ff = w_gate.shape[2]
    row, col = pl.BlockSpec((tm, d), lambda m: (m, 0)), pl.BlockSpec((d, tm), lambda m: (0, m))
    wide = pl.BlockSpec((tm, ff // chunks), lambda m: (m, 0))
    return pl.pallas_call(
        functools.partial(states_kernel, chunks, owners),
        grid=(t // tm,),
        in_specs=[row, row] + [once((1, d, ff), lambda m: (layer, 0, 0))] * 2 + [wide] * (2 * chunks),
        out_specs=[row, col],
        out_shape=[jax.ShapeDtypeStruct((t, d), BF16), jax.ShapeDtypeStruct((d, t), BF16)],
        compiler_params=params(),
        cost_estimate=cost(4 * t * d * ff, nbytes(*dgs, *dus, h, dy)),
        name="states",
    )(h, dy, w_gate, w_up, *dgs, *dus)


def finish_kernel(so_far, own, from_left, from_right, left_a, right_b, g, squares):
    i = pl.program_id(0)

    @pl.when(i == 0)
    def _():
        squares[...] = so_far[...]

    def add(plain, summed):
        total = own[...].astype(F32) + plain[...].astype(F32) + summed[...].astype(F32)
        total = total.astype(BF16)
        g[...] = total
        total = total.astype(F32)
        squares[...] += jnp.sum((total * total).reshape(-1, 8, 128 * (STRIPE // 128)), 0)

    half = pl.num_programs(0) // 2
    pl.when(i < half)(lambda: add(from_right, left_a))
    pl.when(i >= half)(lambda: add(from_left, right_b))


def finish(so_far, own, from_left, from_right, left_a, right_b, steps=4):
    rows = own.shape[0] // steps
    half = steps // 2
    block = lambda f: pl.BlockSpec((rows, STRIPE), lambda i: (f(i), 0))
    squares = pl.BlockSpec((8, STRIPE), lambda i: (0, 0))
    second = lambda i: half + lax.rem(i, half)
    return pl.pallas_call(
        finish_kernel,
        grid=(steps,),
        in_specs=[
            squares,
            block(lambda i: i),
            block(lambda i: jnp.maximum(i, half)),
            block(lambda i: half + jnp.minimum(i, half - 1)),
            block(lambda i: jnp.minimum(i, half - 1)),
            block(lambda i: jnp.maximum(i - half, 0)),
        ],
        out_specs=[block(lambda i: i), squares],
        out_shape=[jax.ShapeDtypeStruct(own.shape, BF16), jax.ShapeDtypeStruct((8, STRIPE), F32)],
        compiler_params=params(),
        cost_estimate=cost(4 * own.size, 4 * nbytes(own)),
        name="finish",
    )(so_far, own, from_left, from_right, left_a, right_b)


def around(n):
    right = [(i, (i + 1) % n) for i in range(n)]
    left = [(i, (i - 1) % n) for i in range(n)]
    across = [(i, (i + 2) % n) for i in range(n)]
    return right, left, across


def wide_add(a, b):
    return (a.astype(F32) + b.astype(F32)).astype(BF16)


def reduce_chunk(n, so_far, to_right, to_left, own, right_a, left_b):
    right, left, _ = around(n)
    half = own.shape[0] // 2
    from_left = lax.ppermute(to_right, "dp", right)
    from_right = lax.ppermute(to_left, "dp", left)
    left_a = lax.ppermute(wide_add(right_a, from_left[:half]), "dp", right)
    right_b = lax.ppermute(wide_add(left_b, from_right[:half]), "dp", left)
    return finish(so_far, own, from_left, from_right, left_a, right_b)


def adam_kernel(layers, chunks, tall, count, *refs):
    sums, (w, m, v), refs = refs[:4], refs[4:7], refs[7:]
    gs, (w_out, m_out, v_out) = refs[: layers * chunks], refs[layers * chunks :]
    total = sum(jnp.sum(s[...]) for s in sums)
    factor = jnp.minimum(1.0, 0.5 * lax.rsqrt(jnp.full((1, 1), total) / count + 1e-30))
    for layer in range(layers):
        for c in range(chunks):
            at = slice(c * STRIPE, (c + 1) * STRIPE)
            i = (layer, at, slice(None)) if tall else (layer, slice(None), at)
            g = gs[layer * chunks + c][...].astype(F32) * factor
            m_new = 0.9 * m[i] + 0.1 * g
            v_new = 0.95 * v[i] + 0.05 * g * g
            old = w[i].astype(F32)
            step = m_new * lax.rsqrt(v_new + 1e-8) + 0.1 * old
            w_out[i] = (old - 0.02 * step).astype(BF16)
            m_out[i] = m_new
            v_out[i] = v_new


def adam(me, sums, w, m, v, gs, at, count, chunks, tall):
    layers, rows, columns = m.shape
    width = STRIPE if tall else STRIPE * chunks
    g_rows = STRIPE if tall else rows
    small = pl.BlockSpec((8, STRIPE), lambda i, me: (0, 0))
    block = pl.BlockSpec((layers, rows, width), lambda i, me: (0, 0, i))
    out = [jax.ShapeDtypeStruct(m.shape, BF16)] + [jax.ShapeDtypeStruct(m.shape, F32)] * 2

    def body(me_ref, *refs):
        adam_kernel(layers, chunks, tall, count, *refs)

    return pl.pallas_call(
        body,
        grid_spec=pltpu.PrefetchScalarGridSpec(
            num_scalar_prefetch=1,
            grid=(columns // width,),
            in_specs=[small] * 4
            + [pl.BlockSpec((layers, rows, width), lambda i, me: (0, me[0], i)), block, block]
            + [pl.BlockSpec((g_rows, STRIPE), lambda i, me: (at // g_rows + i, 0))] * len(gs),
            out_specs=[block] * 3,
        ),
        out_shape=out,
        compiler_params=params(),
        cost_estimate=cost(16 * m.size, 22 * m.size),
        name="adam",
    )(me, *sums, w, m, v, *gs)


def place_kernel(me_ref, *refs):
    *pieces, out = refs
    i = pl.program_id(0)
    for k, piece in enumerate(pieces):
        pl.when(i == k)(lambda piece=piece: out.__setitem__(..., piece[...]))


def place(me, own, from_left, from_right, rows_all):
    layers, rows, columns = own.shape
    turn = lambda i: jnp.where(i == 0, 0, jnp.where(i == 1, 3, 1))
    return pl.pallas_call(
        place_kernel,
        grid_spec=pltpu.PrefetchScalarGridSpec(
            num_scalar_prefetch=1,
            grid=(3,),
            in_specs=[once((layers, rows, columns), lambda i, me: (0, 0, 0))] * 3,
            out_specs=pl.BlockSpec(
                (layers, rows, columns), lambda i, me: (0, lax.rem(me[0] + turn(i), rows_all // rows), 0)
            ),
        ),
        out_shape=jax.ShapeDtypeStruct((layers, rows_all, columns), own.dtype),
        compiler_params=params(),
        cost_estimate=cost(own.size, 6 * nbytes(own)),
        name="place",
    )(me, own, from_left, from_right)


def place_last_kernel(me_ref, whole, first, second, out):
    i = pl.program_id(0)
    pl.when(i == 0)(lambda: out.__setitem__(..., first[...]))
    pl.when(i == 1)(lambda: out.__setitem__(..., second[...]))


def place_last(me, whole, first, second):
    layers, rows_all, columns = whole.shape
    rows = first.shape[1]
    piece = once((1, rows, columns), lambda i, me: (0, 0, 0))
    return pl.pallas_call(
        place_last_kernel,
        grid_spec=pltpu.PrefetchScalarGridSpec(
            num_scalar_prefetch=1,
            grid=(2,),
            in_specs=[pl.BlockSpec(memory_space=pl.ANY), piece, piece],
            out_specs=pl.BlockSpec((1, rows, columns), lambda i, me: (i, lax.rem(me[0] + 2, rows_all // rows), 0)),
        ),
        out_shape=jax.ShapeDtypeStruct(whole.shape, whole.dtype),
        input_output_aliases={1: 0},
        compiler_params=params(),
        cost_estimate=cost(first.size, 4 * nbytes(first)),
        name="place_last",
    )(me, whole, first, second)


def gather(n, me, own, rows_all):
    right, left, _ = around(n)
    from_left = lax.ppermute(own, "dp", right)
    from_right = lax.ppermute(own, "dp", left)
    first = lax.ppermute(from_left[:1], "dp", right)
    second = lax.ppermute(from_right[1:], "dp", left)
    return place_last(me, place(me, own, from_left, from_right, rows_all), first, second)


def solution(mesh):
    n = mesh.shape["dp"]

    def step(x, dy, w_gate, w_up, w_down, m_gate, m_up, m_down, v_gate, v_up, v_down):
        x, dy = x[0], dy[0]
        layers, d, ff = w_gate.shape
        chunks = ff // (n * STRIPE)
        me = lax.axis_index("dp").astype(jnp.int32).reshape(1)

        gates, ups, a0_t, h1, a1, a1_t, dy_t = forward(x, dy, w_gate, w_up, w_down, chunks)
        squares = jnp.zeros((8, STRIPE), F32)
        dgs, dus, top, bottom = [], [], [], []
        for c in range(chunks):
            dg, du, parts = top_gradients(n, chunks, c, 1, a1, a1_t, dy, dy_t, w_gate, w_up, w_down)
            dgs.append(dg)
            dus.append(du)
            top.append(parts)
        dh, dh_t = states(n, chunks, 1, h1, dy, w_gate, w_up, dgs, dus)
        for c in range(chunks):
            bottom.append(bottom_gradients(n, chunks, c, 0, a0_t, dh, dh_t, gates[c], ups[c], w_down))
        gs = []
        for parts in top + bottom:
            g, squares = reduce_chunk(n, squares, *parts)
            gs.append(g)
        gs = gs[chunks:] + gs[:chunks]

        right, left, across = around(n)
        sums = [squares] + [lax.ppermute(squares, "dp", way) for way in (right, left, across)]
        count = 3 * w_gate.size
        new = []
        for w, m, v, at, tall in (
            (w_gate, m_gate, v_gate, 0, False),
            (w_up, m_up, v_up, d, False),
            (w_down, m_down, v_down, 2 * d, True),
        ):
            new.append(adam(me, sums, w, m, v, gs, at, count, chunks, tall))
        whole = [gather(n, me, one[0], w.shape[1]) for one, w in zip(new, (w_gate, w_up, w_down), strict=True)]
        return (*whole, *(one[1] for one in new), *(one[2] for one in new))

    seq, part, rows = P(("rep", "dp"), None, None), P("rep", None, None), P("rep", "dp", None)
    state = P(None, "dp", None)
    return jax.shard_map(
        step,
        mesh=mesh,
        in_specs=(seq, seq) + (P(None, None, None),) * 3 + (state,) * 6,
        out_specs=(part,) * 3 + (rows,) * 6,
        check_vma=False,
    )
```

```python
import functools

import jax
import jax.numpy as jnp
from jax import lax
from jax.experimental import pallas as pl
from jax.experimental.pallas import tpu as pltpu
from jax.sharding import PartitionSpec as P

F32, BF16 = jnp.float32, jnp.bfloat16
STRIPE = 128
VMEM_LIMIT = 60 << 20


def dot(a, b):
    return jnp.dot(a, b, preferred_element_type=F32)


def dot_nt(a, b):
    return lax.dot_general(a, b, (((1,), (1,)), ((), ())), preferred_element_type=F32)


def sigmoid(x):
    return 0.5 * jnp.tanh(0.5 * x) + 0.5


def normed(h):
    wide = h.astype(F32)
    scale = lax.rsqrt(jnp.mean(wide * wide, -1, keepdims=True) + 1e-6)
    return (wide * scale).astype(BF16)


def cost(flops, read_and_written):
    return pl.CostEstimate(flops=int(flops), bytes_accessed=int(read_and_written), transcendentals=0)


def params(**more):
    return pltpu.CompilerParams(vmem_limit_bytes=VMEM_LIMIT, **more)


def nbytes(*arrays):
    return sum(a.size * jnp.dtype(a.dtype).itemsize for a in arrays)


def once(shape, index_map):
    return pl.BlockSpec(shape, index_map, pipeline_mode=pl.Buffered(1))


def stripes(n, chunks, c):
    return [slice((o * chunks + c) * STRIPE, (o * chunks + c + 1) * STRIPE) for o in range(n)]


def forward_kernel(n, chunks, x, dy, wg, wu, wd, gate, up, a_t, h1, a1, a1_t, dy_t, act):
    a = normed(x[...])
    a_t[...] = a.T
    dy_t[...] = dy[...].T
    width = n * STRIPE
    for c in range(chunks):
        at = stripes(n, chunks, c)
        g = dot(a, jnp.concatenate([wg[0, :, s] for s in at], 1))
        u = dot(a, jnp.concatenate([wu[0, :, s] for s in at], 1))
        gate[c] = g
        up[c] = u
        act[:, c * width : (c + 1) * width] = (g * sigmoid(g) * u).astype(BF16)
    down = jnp.concatenate([wd[0, s, :] for c in range(chunks) for s in stripes(n, chunks, c)], 0)
    y = dot(act[...], down).astype(BF16)
    h = (x[...].astype(F32) + y.astype(F32)).astype(BF16)
    h1[...] = h
    out = normed(h)
    a1[...] = out
    a1_t[...] = out.T


def forward(n, chunks, x, dy, w_gate, w_up, w_down, tm=512):
    t, d = x.shape
    ff = w_gate.shape[2]
    row, col = pl.BlockSpec((tm, d), lambda m: (m, 0)), pl.BlockSpec((d, tm), lambda m: (0, m))
    wide = pl.BlockSpec((chunks, tm, n * STRIPE), lambda m: (0, m, 0))
    out = [jax.ShapeDtypeStruct((chunks, t, n * STRIPE), F32)] * 2 + [
        jax.ShapeDtypeStruct(s, BF16) for s in ((d, t), (t, d), (t, d), (d, t), (d, t))
    ]
    return pl.pallas_call(
        functools.partial(forward_kernel, n, chunks),
        grid=(t // tm,),
        in_specs=[row, row]
        + [once((1, d, ff), lambda m: (0, 0, 0))] * 2
        + [once((1, ff, d), lambda m: (0, 0, 0))],
        out_specs=[wide, wide, col, row, row, col, col],
        out_shape=out,
        scratch_shapes=[pltpu.VMEM((tm, ff), BF16)],
        compiler_params=params(),
        cost_estimate=cost(6 * t * d * ff, nbytes(*out)),
        name="forward",
    )(x, dy, w_gate, w_up, w_down)


def neighbours(n):
    me = lax.axis_index("dp")
    return lax.rem(me + 1, n), lax.rem(me + 2, n), lax.rem(me + n - 1, n)


def greet(devices):
    barrier = pltpu.get_barrier_semaphore()
    for device in devices:
        pl.semaphore_signal(barrier, inc=1, device_id={"dp": device}, device_id_type=pl.DeviceIdType.MESH)
    pl.semaphore_wait(barrier, len(devices))


def remote(src, dst, send, recv, device):
    return pltpu.make_async_remote_copy(
        src_ref=src, dst_ref=dst, send_sem=send, recv_sem=recv, device_id={"dp": device}, device_id_type=pl.DeviceIdType.MESH
    )


class Ring:
    def __init__(self, n, raw, got, mid, send, recv):
        half = raw.shape[1] // 2
        self.a, self.b = pl.ds(0, half), pl.ds(half, half)
        self.raw, self.got, self.mid = raw, got, mid
        self.send, self.recv = send, recv
        self.right, _, self.left = neighbours(n)

    def copy(self, k):
        source = (
            lambda: self.raw.at[2, self.a],
            lambda: self.raw.at[1, self.b],
            lambda: self.mid.at[0],
            lambda: self.raw.at[2, self.b],
            lambda: self.raw.at[3, self.a],
            lambda: self.mid.at[1],
        )[k]()
        return remote(source, self.got.at[k], self.send.at[k], self.recv.at[k], self.right if k < 3 else self.left)

    def begin(self):
        for k in (0, 3, 1, 4):
            self.copy(k).start()

    def go_on(self):
        for k, owner, half in ((0, 1, self.a), (3, 3, self.b)):
            self.copy(k).wait_recv()
            self.mid[k // 3] = (self.raw[owner, half].astype(F32) + self.got[k].astype(F32)).astype(BF16)
            self.copy(k + 2).start()

    def end(self, out, squares):
        for plain, summed, half in ((4, 2, self.a), (1, 5, self.b)):
            self.copy(plain).wait_recv()
            self.copy(summed).wait_recv()
            total = self.raw[0, half].astype(F32) + self.got[plain].astype(F32) + self.got[summed].astype(F32)
            total = total.astype(BF16)
            out[0, half] = total
            total = total.astype(F32)
            squares[...] += jnp.sum((total * total).reshape(-1, 8, total.shape[1]), 0)

    def sent(self, *which):
        for k in which:
            self.copy(k).wait_send()


def lay_out(n, raw, gacc, uacc, dacc):
    me = lax.axis_index("dp")
    rows = gacc.shape[0] // n
    for o in range(n):
        turn = lax.rem(o - me + n, n)
        raw[turn, :rows] = gacc[o * rows : (o + 1) * rows].astype(BF16)
        raw[turn, rows : 2 * rows] = uacc[o * rows : (o + 1) * rows].astype(BF16)
        for q in range(n):
            raw[turn, 2 * rows :, q * STRIPE : (q + 1) * STRIPE] = dacc[
                q * rows : (q + 1) * rows, o * STRIPE : (o + 1) * STRIPE
            ].astype(BF16)


def backward_parts(g, u, dact):
    dact = dact.astype(BF16).astype(F32)
    s = sigmoid(g)
    silu = g * s
    act = (silu * u).astype(BF16)
    du = (dact * silu).astype(BF16)
    dg = (dact * u * (s + silu * (1 - s))).astype(BF16)
    return act, dg, du


def states_gradient(da1, da2, h, dy):
    da = (da1.astype(BF16).astype(F32) + da2.astype(BF16).astype(F32)).astype(BF16).astype(F32)
    wide = h.astype(F32)
    mean = jnp.mean(wide * wide, -1, keepdims=True) + 1e-6
    scale = lax.rsqrt(mean)
    dmean = jnp.sum(da * wide, -1, keepdims=True) * (-0.5 * scale / mean)
    back = (da * scale + wide * (dmean * (2.0 / wide.shape[1]))).astype(BF16)
    return (dy.astype(F32) + back.astype(F32)).astype(BF16)


def top_kernel(n, chunks, tiles, *refs):
    a, a_t, dy, dy_t, h, *refs = refs
    wg, wu, wd, refs = refs[:n], refs[n : 2 * n], refs[2 * n : 3 * n], refs[3 * n :]
    dh, dh_t, g_out, last, squares_out, gacc, uacc, dacc, da, raw, got, mid, squares, send, recv, local = refs
    c, i = pl.program_id(0), pl.program_id(1)
    tm = a.shape[0]
    right, _, left = neighbours(n)
    before = jnp.maximum(c - 1, 0)
    slot = lax.rem(before, 2)
    ring = Ring(n, raw, got.at[slot], mid, send.at[slot], recv.at[slot])

    @pl.when((c == 0) & (i == 0))
    def _():
        greet((right, left))
        squares[...] = jnp.zeros_like(squares)

    @pl.when((c > 0) & (i == 0))
    def _():
        ring.begin()

    @pl.when(i == 0)
    def _():
        for acc in (gacc, uacc, dacc):
            acc[...] = jnp.zeros_like(acc)

    rows = pl.ds(pl.multiple_of(i * tm, tm), tm)

    @pl.when(c == 0)
    def _():
        da[:, rows, :] = jnp.zeros((2, tm, a.shape[1]), F32)

    pair = 2
    first, then = [], []
    for j in range(0, n, pair):
        js = range(j, j + pair)
        w1 = jnp.concatenate([wg[k][0] for k in js], 1)
        w2 = jnp.concatenate([wu[k][0] for k in js], 1)
        w3 = jnp.concatenate([wd[k][0] for k in js], 0)
        first.append((slice(j * STRIPE, (j + pair) * STRIPE), w1, w2, dot(a[...], w1), dot(a[...], w2), dot_nt(dy[...], w3)))
    for to, w1, w2, g, u, dact in first:
        act, dg, du = backward_parts(g, u, dact)
        gacc[:, to] += dot(a_t[...], dg)
        uacc[:, to] += dot(a_t[...], du)
        dacc[:, to] += dot(dy_t[...], act)
        da[0, rows, :] += dot_nt(dg, w1)
        da[1, rows, :] += dot_nt(du, w2)

    @pl.when(c == chunks - 1)
    def _():
        out = states_gradient(da[0, rows, :], da[1, rows, :], h[...], dy[...])
        dh[...] = out
        dh_t[...] = out.T

    pl.when((c > 0) & (i == tiles // 2 - 1))(ring.go_on)

    @pl.when((c > 0) & (i == tiles - 1))
    def _():
        ring.end(g_out, squares)
        ring.sent(*range(6))

    @pl.when(i == tiles - 1)
    def _():
        lay_out(n, raw, gacc, uacc, dacc)

    @pl.when((c == chunks - 1) & (i == tiles - 1))
    def _():
        copy = pltpu.make_async_copy(raw, last, local)
        copy.start()
        squares_out[...] = squares[...]
        copy.wait()


def stripe_specs(n, chunks, layer, d, chunk):
    across = [pl.BlockSpec((1, d, STRIPE), lambda *at, j=j: (layer, 0, j * chunks + chunk(*at))) for j in range(n)]
    down = [pl.BlockSpec((1, STRIPE, d), lambda *at, j=j: (layer, j * chunks + chunk(*at), 0)) for j in range(n)]
    return across, down


def top(n, chunks, layer, a, a_t, dy, dy_t, h, w_gate, w_up, w_down, tm=512):
    t, d = a.shape
    width, tiles, block = n * STRIPE, t // tm, 3 * d // n
    row, col = pl.BlockSpec((tm, d), lambda c, i: (i, 0)), pl.BlockSpec((d, tm), lambda c, i: (0, i))
    at_end = lambda c, i: jnp.where(c == chunks - 1, i, 0)
    row_end, col_end = pl.BlockSpec((tm, d), lambda c, i: (at_end(c, i), 0)), pl.BlockSpec((d, tm), lambda c, i: (0, at_end(c, i)))
    across, down = stripe_specs(n, chunks, layer, d, lambda c, i: c)
    shapes = [
        jax.ShapeDtypeStruct((t, d), BF16),
        jax.ShapeDtypeStruct((d, t), BF16),
        jax.ShapeDtypeStruct((chunks - 1, block, width), BF16),
        jax.ShapeDtypeStruct((n, block, width), BF16),
        jax.ShapeDtypeStruct((8, width), F32),
    ]
    return pl.pallas_call(
        functools.partial(top_kernel, n, chunks, tiles),
        grid=(chunks, tiles),
        in_specs=[row, col, row, col, row_end] + across + across + down,
        out_specs=[
            row_end,
            col_end,
            pl.BlockSpec((1, block, width), lambda c, i: (jnp.maximum(c - 1, 0), 0, 0)),
            pl.BlockSpec(memory_space=pl.ANY),
            pl.BlockSpec((8, width), lambda c, i: (0, 0)),
        ],
        out_shape=shapes,
        scratch_shapes=[pltpu.VMEM((d, width), F32)] * 3
        + [
            pltpu.VMEM((2, t, d), F32),
            pltpu.VMEM((n, block, width), BF16),
            pltpu.VMEM((2, 6, block // 2, width), BF16),
            pltpu.VMEM((2, block // 2, width), BF16),
            pltpu.VMEM((8, width), F32),
            pltpu.SemaphoreType.DMA((2, 6)),
            pltpu.SemaphoreType.DMA((2, 6)),
            pltpu.SemaphoreType.DMA,
        ],
        compiler_params=pltpu.CompilerParams(vmem_limit_bytes=67043328, collective_id=0, has_side_effects=True),
        cost_estimate=cost(16 * t * d * width * chunks, chunks * nbytes(a, a_t, dy, dy_t)),
        name="top",
    )(a, a_t, dy, dy_t, h, *[w_gate] * n, *[w_up] * n, *[w_down] * n)


def bottom_kernel(n, chunks, tiles, *refs):
    a_t, dy, dy_t, gate, up, *refs = refs
    wd, refs = refs[:n], refs[n:]
    first, squares_in, g_out, squares_out, gacc, uacc, dacc, raw, got, mid, squares, send, recv, local, others, to, fro = refs
    c, i = pl.program_id(0), pl.program_id(1)
    right, opposite, left = neighbours(n)

    def ring(k):
        slot = lax.rem(k, 2)
        return Ring(n, raw.at[slot], got.at[k], mid.at[slot], send.at[k], recv.at[k])

    @pl.when((c == 0) & (i == 0))
    def _():
        copy = pltpu.make_async_copy(first, raw.at[0], local)
        copy.start()
        greet((right, opposite, left))
        squares[...] = squares_in[...]
        copy.wait()

    @pl.when(i == 0)
    def _():
        ring(c).begin()
        for acc in (gacc, uacc, dacc):
            acc[...] = jnp.zeros_like(acc)

    @pl.when(c < chunks)
    def _():
        pair = 2
        first = []
        for j in range(0, n, pair):
            w = jnp.concatenate([wd[k][0] for k in range(j, j + pair)], 0)
            first.append((slice(j * STRIPE, (j + pair) * STRIPE), dot_nt(dy[...], w)))
        for to, dact in first:
            act, dg, du = backward_parts(gate[0, :, to], up[0, :, to], dact)
            gacc[:, to] += dot(a_t[...], dg)
            uacc[:, to] += dot(a_t[...], du)
            dacc[:, to] += dot(dy_t[...], act)

    @pl.when((c > 0) & (i == tiles // 4))
    def _():
        before = ring(c - 1)
        before.end(g_out, squares)
        before.sent(*range(6))

    pl.when(i == tiles // 2)(lambda: ring(c).go_on())

    @pl.when((c < chunks) & (i == tiles - 1))
    def _():
        lay_out(n, raw.at[lax.rem(c + 1, 2)], gacc, uacc, dacc)

    @pl.when((c == chunks) & (i == tiles - 1))
    def _():
        final = ring(c)
        final.end(g_out, squares)
        final.sent(*range(6))
        copies = [
            remote(squares, others.at[k], to.at[k], fro.at[k], device) for k, device in enumerate((right, opposite, left))
        ]
        for copy in copies:
            copy.start()
        for copy in copies:
            copy.wait()
        squares_out[...] = squares[...] + (others[0] + others[1] + others[2])


def bottom(n, chunks, layer, a_t, dy, dy_t, gate, up, w_down, first, squares, tm=1024):
    d, t = a_t.shape
    width, tiles, block = n * STRIPE, t // tm, 3 * d // n
    tile = lambda c, i: jnp.where(c < chunks, i, tiles - 1)
    chunk = lambda c, i: jnp.minimum(c, chunks - 1)
    row, col = pl.BlockSpec((tm, d), lambda c, i: (tile(c, i), 0)), pl.BlockSpec((d, tm), lambda c, i: (0, tile(c, i)))
    wide = pl.BlockSpec((1, tm, width), lambda c, i: (chunk(c, i), tile(c, i), 0))
    small = pl.BlockSpec((8, width), lambda c, i: (0, 0))
    _, down = stripe_specs(n, chunks, layer, d, chunk)
    done = lambda c, i: jnp.where((c == chunks) & (i == tiles - 1), chunks, jnp.maximum(c - 1, 0))
    return pl.pallas_call(
        functools.partial(bottom_kernel, n, chunks, tiles),
        grid=(chunks + 1, tiles),
        in_specs=[col, row, col, wide, wide] + down + [pl.BlockSpec(memory_space=pl.ANY), small],
        out_specs=[pl.BlockSpec((1, block, width), lambda c, i: (done(c, i), 0, 0)), small],
        out_shape=[
            jax.ShapeDtypeStruct((chunks + 1, block, width), BF16),
            jax.ShapeDtypeStruct((8, width), F32),
        ],
        scratch_shapes=[pltpu.VMEM((d, width), F32)] * 3
        + [
            pltpu.VMEM((2, n, block, width), BF16),
            pltpu.VMEM((chunks + 1, 6, block // 2, width), BF16),
            pltpu.VMEM((2, 2, block // 2, width), BF16),
            pltpu.VMEM((8, width), F32),
            pltpu.SemaphoreType.DMA((chunks + 1, 6)),
            pltpu.SemaphoreType.DMA((chunks + 1, 6)),
            pltpu.SemaphoreType.DMA,
            pltpu.VMEM((3, 8, width), F32),
            pltpu.SemaphoreType.DMA((3,)),
            pltpu.SemaphoreType.DMA((3,)),
        ],
        compiler_params=pltpu.CompilerParams(vmem_limit_bytes=VMEM_LIMIT, collective_id=1, has_side_effects=True),
        cost_estimate=cost(8 * t * d * width * chunks, nbytes(gate, up) + chunks * nbytes(a_t, dy, dy_t)),
        name="bottom",
    )(a_t, dy, dy_t, gate, up, *[w_down] * n, first, squares)


def adam_kernel(chunks, tall, count, squares, w, m, v, g_top, g_bottom, w_out, m_out, v_out):
    factor = jnp.minimum(1.0, 0.5 * lax.rsqrt(jnp.full((1, 1), jnp.sum(squares[...])) / count + 1e-30))
    for layer in range(m.shape[0]):
        for c in range(chunks):
            at = slice(c * STRIPE, (c + 1) * STRIPE)
            i = (layer, at, slice(None)) if tall else (layer, slice(None), at)
            g = g_bottom[c + 1] if layer == 0 else g_bottom[0] if c == chunks - 1 else g_top[c]
            g = g.astype(F32)
            if tall:
                g = jnp.concatenate([g[:, q : q + STRIPE].T for q in range(0, g.shape[1], STRIPE)], 1)
            g = g * factor
            m_new = 0.9 * m[i] + 0.1 * g
            v_new = 0.95 * v[i] + 0.05 * g * g
            old = w[i].astype(F32)
            step = m_new * lax.rsqrt(v_new + 1e-8) + 0.1 * old
            w_out[i] = (old - 0.02 * step).astype(BF16)
            m_out[i] = m_new
            v_out[i] = v_new


def adam(me, squares, w, m, v, g_top, g_bottom, which, count, chunks, tall):
    layers, rows, columns = m.shape
    g_rows = g_top.shape[1] // 3
    g_width = 2 * STRIPE if tall else STRIPE
    width = 2 * g_rows if tall else STRIPE * chunks
    block = pl.BlockSpec((layers, rows, width), lambda i, me: (0, 0, i))
    out = [jax.ShapeDtypeStruct(m.shape, BF16)] + [jax.ShapeDtypeStruct(m.shape, F32)] * 2

    def body(me_ref, *refs):
        adam_kernel(chunks, tall, count, *refs)

    return pl.pallas_call(
        body,
        grid_spec=pltpu.PrefetchScalarGridSpec(
            num_scalar_prefetch=1,
            grid=(columns // width,),
            in_specs=[pl.BlockSpec(squares.shape, lambda i, me: (0, 0))]
            + [pl.BlockSpec((layers, rows, width), lambda i, me: (0, me[0], i)), block, block]
            + [pl.BlockSpec((g.shape[0], g_rows, g_width), lambda i, me: (0, which, i)) for g in (g_top, g_bottom)],
            out_specs=[block] * 3,
        ),
        out_shape=out,
        compiler_params=params(),
        cost_estimate=cost(16 * m.size, 22 * m.size),
        name="adam",
    )(me, squares, w, m, v, g_top, g_bottom)


def place_kernel(me_ref, *refs):
    *pieces, out = refs
    i = pl.program_id(0)
    for k, piece in enumerate(pieces):
        pl.when(i == k)(lambda piece=piece: out.__setitem__(..., piece[...]))


def place(me, own, from_left, from_right, rows_all):
    layers, rows, columns = own.shape
    turn = lambda i: jnp.where(i == 0, 0, jnp.where(i == 1, 3, 1))
    return pl.pallas_call(
        place_kernel,
        grid_spec=pltpu.PrefetchScalarGridSpec(
            num_scalar_prefetch=1,
            grid=(3,),
            in_specs=[once((layers, rows, columns), lambda i, me: (0, 0, 0))] * 3,
            out_specs=pl.BlockSpec(
                (layers, rows, columns), lambda i, me: (0, lax.rem(me[0] + turn(i), rows_all // rows), 0)
            ),
        ),
        out_shape=jax.ShapeDtypeStruct((layers, rows_all, columns), own.dtype),
        compiler_params=params(),
        cost_estimate=cost(own.size, 6 * nbytes(own)),
        name="place",
    )(me, own, from_left, from_right)


def place_last_kernel(me_ref, whole, first, second, out):
    i = pl.program_id(0)
    pl.when(i == 0)(lambda: out.__setitem__(..., first[...]))
    pl.when(i == 1)(lambda: out.__setitem__(..., second[...]))


def place_last(me, whole, first, second):
    layers, rows_all, columns = whole.shape
    rows = first.shape[1]
    piece = once((1, rows, columns), lambda i, me: (0, 0, 0))
    return pl.pallas_call(
        place_last_kernel,
        grid_spec=pltpu.PrefetchScalarGridSpec(
            num_scalar_prefetch=1,
            grid=(2,),
            in_specs=[pl.BlockSpec(memory_space=pl.ANY), piece, piece],
            out_specs=pl.BlockSpec((1, rows, columns), lambda i, me: (i, lax.rem(me[0] + 2, rows_all // rows), 0)),
        ),
        out_shape=jax.ShapeDtypeStruct(whole.shape, whole.dtype),
        input_output_aliases={1: 0},
        compiler_params=params(),
        cost_estimate=cost(first.size, 4 * nbytes(first)),
        name="place_last",
    )(me, whole, first, second)


def around(n):
    right = [(i, (i + 1) % n) for i in range(n)]
    left = [(i, (i - 1) % n) for i in range(n)]
    return right, left


def gather(n, me, own, rows_all):
    right, left = around(n)
    from_left = lax.ppermute(own, "dp", right)
    from_right = lax.ppermute(own, "dp", left)
    first = lax.ppermute(from_left[:1], "dp", right)
    second = lax.ppermute(from_right[1:], "dp", left)
    return place_last(me, place(me, own, from_left, from_right, rows_all), first, second)


def solution(mesh):
    n = mesh.shape["dp"]

    def step(x, dy, w_gate, w_up, w_down, m_gate, m_up, m_down, v_gate, v_up, v_down):
        x, dy = x[0], dy[0]
        chunks = w_gate.shape[2] // (n * STRIPE)
        me = lax.axis_index("dp").astype(jnp.int32).reshape(1)

        gate, up, a0_t, h1, a1, a1_t, dy_t = forward(n, chunks, x, dy, w_gate, w_up, w_down)
        dh, dh_t, g_top, last, squares = top(n, chunks, 1, a1, a1_t, dy, dy_t, h1, w_gate, w_up, w_down)
        g_bottom, squares = bottom(n, chunks, 0, a0_t, dh, dh_t, gate, up, w_down, last, squares)

        count = 3 * w_gate.size
        new = []
        for which, (w, m, v) in enumerate(((w_gate, m_gate, v_gate), (w_up, m_up, v_up), (w_down, m_down, v_down))):
            new.append(adam(me, squares, w, m, v, g_top, g_bottom, which, count, chunks, which == 2))
        whole = [gather(n, me, one[0], w.shape[1]) for one, w in zip(new, (w_gate, w_up, w_down), strict=True)]
        return (*whole, *(one[1] for one in new), *(one[2] for one in new))

    seq, part, rows = P(("rep", "dp"), None, None), P("rep", None, None), P("rep", "dp", None)
    state = P(None, "dp", None)
    return jax.shard_map(
        step,
        mesh=mesh,
        in_specs=(seq, seq) + (P(None, None, None),) * 3 + (state,) * 6,
        out_specs=(part,) * 3 + (rows,) * 6,
        check_vma=False,
    )
```

```python
import functools

import jax
import jax.numpy as jnp
from jax import lax
from jax.experimental import pallas as pl
from jax.experimental.pallas import tpu as pltpu
from jax.sharding import PartitionSpec as P


F32, BF16 = jnp.float32, jnp.bfloat16
STRIPE = 128
VMEM_LIMIT = 60 << 20
PIECES = ((0, 0, 1), (0, 1, 3), (2, 0, 2), (1, 0, 3), (1, 3, 1))


def dot(a, b):
    return jnp.dot(a, b, preferred_element_type=F32)


def dot_nt(a, b):
    return lax.dot_general(a, b, (((1,), (1,)), ((), ())), preferred_element_type=F32)


def sigmoid(x):
    return 0.5 * jnp.tanh(0.5 * x) + 0.5


def normed(h):
    wide = h.astype(F32)
    scale = lax.rsqrt(jnp.mean(wide * wide, -1, keepdims=True) + 1e-6)
    return (wide * scale).astype(BF16)


def cost(flops, read_and_written):
    return pl.CostEstimate(flops=int(flops), bytes_accessed=int(read_and_written), transcendentals=0)


def params(**more):
    return pltpu.CompilerParams(vmem_limit_bytes=VMEM_LIMIT, **more)


def nbytes(*arrays):
    return sum(a.size * jnp.dtype(a.dtype).itemsize for a in arrays)


def once(shape, index_map):
    return pl.BlockSpec(shape, index_map, pipeline_mode=pl.Buffered(1))


def stripes(n, chunks, c):
    return [slice((o * chunks + c) * STRIPE, (o * chunks + c + 1) * STRIPE) for o in range(n)]


def forward_kernel(n, chunks, tiles, *refs):
    x_first, x_next, x_before, dy, wg, wu, wd, *refs = refs
    gate, up, a_t, h1, a1, a1_t, dy_t, act, normal, y = refs
    m = pl.program_id(0)
    width = n * STRIPE

    def finish():
        h = (x_before[...].astype(F32) + y[...].astype(F32)).astype(BF16)
        h1[...] = h
        out = normed(h)
        a1[...] = out
        a1_t[...] = out.T

    @pl.when(m == 0)
    def _():
        normal[0] = normed(x_first[...])

    @pl.when(m < tiles)
    def _():
        a = normal[lax.rem(m, 2)]

        def dots(c):
            for o, w in ((gate, wg), (up, wu)):
                o[c] = dot(a, jnp.concatenate([w[0, :, s] for s in stripes(n, chunks, c)], 1))

        dots(0)
        for c in range(chunks):
            if c + 1 < chunks:
                dots(c + 1)
            g = gate[c]
            act[:, c * width : (c + 1) * width] = (g * sigmoid(g) * up[c]).astype(BF16)
        a_t[...] = a.T
        dy_t[...] = dy[...].T
        finish()
        down = jnp.concatenate([wd[0, s, :] for c in range(chunks) for s in stripes(n, chunks, c)], 0)
        y[...] = dot(act[...], down).astype(BF16)
        normal[lax.rem(m + 1, 2)] = normed(x_next[...])

    pl.when(m == tiles)(finish)


def forward(n, chunks, x, dy, w_gate, w_up, w_down, tm=256):
    t, d = x.shape
    ff, tiles, width = w_gate.shape[2], t // tm, n * STRIPE
    here, before = lambda m: jnp.minimum(m, tiles - 1), lambda m: jnp.maximum(m - 1, 0)
    row = lambda at: pl.BlockSpec((tm, d), lambda m: (at(m), 0))
    col = lambda at: pl.BlockSpec((d, tm), lambda m: (0, at(m)))
    wide = pl.BlockSpec((chunks, tm, width), lambda m: (0, here(m), 0))
    out = [jax.ShapeDtypeStruct((chunks, t, width), F32)] * 2 + [
        jax.ShapeDtypeStruct(s, BF16) for s in ((d, t), (t, d), (t, d), (d, t), (d, t))
    ]
    return pl.pallas_call(
        functools.partial(forward_kernel, n, chunks, tiles),
        grid=(tiles + 1,),
        in_specs=[once((tm, d), lambda m: (0, 0)), row(lambda m: jnp.minimum(m + 1, tiles - 1)), row(before), row(here)]
        + [once((1, d, ff), lambda m: (0, 0, 0))] * 2
        + [once((1, ff, d), lambda m: (0, 0, 0))],
        out_specs=[wide] * 2 + [col(here), row(before), row(before), col(before), col(here)],
        out_shape=out,
        scratch_shapes=[
            pltpu.VMEM((tm, ff), BF16),
            pltpu.VMEM((2, tm, d), BF16),
            pltpu.VMEM((tm, d), BF16),
        ],
        compiler_params=params(),
        cost_estimate=cost(6 * t * d * ff, nbytes(*out)),
        name="forward",
    )(x, x, x, dy, w_gate, w_up, w_down)


def neighbours(n):
    me = lax.axis_index("dp")
    return lax.rem(me + 1, n), lax.rem(me + 2, n), lax.rem(me + n - 1, n)


def greet(devices):
    barrier = pltpu.get_barrier_semaphore()
    for device in devices:
        pl.semaphore_signal(barrier, inc=1, device_id={"dp": device}, device_id_type=pl.DeviceIdType.MESH)
    pl.semaphore_wait(barrier, len(devices))


def remote(src, dst, send, recv, device):
    return pltpu.make_async_remote_copy(
        src_ref=src, dst_ref=dst, send_sem=send, recv_sem=recv, device_id={"dp": device}, device_id_type=pl.DeviceIdType.MESH
    )


class Ring:
    def __init__(self, n, raw, got, mid, send, recv):
        half = raw.shape[1] // 2
        self.a, self.b = pl.ds(0, half), pl.ds(half, half)
        self.raw, self.got, self.mid = raw, got, mid
        self.send, self.recv = send, recv
        self.right, _, self.left = neighbours(n)

    def copy(self, k):
        source = (
            lambda: self.raw.at[2, self.a],
            lambda: self.raw.at[1, self.b],
            lambda: self.mid.at[0],
            lambda: self.raw.at[2, self.b],
            lambda: self.raw.at[3, self.a],
            lambda: self.mid.at[1],
        )[k]()
        return remote(source, self.got.at[k], self.send.at[k], self.recv.at[k], self.right if k < 3 else self.left)

    def begin(self, which=(0, 3, 1, 4)):
        for k in which:
            self.copy(k).start()

    def go_on(self):
        for k, owner, half in ((0, 1, self.a), (3, 3, self.b)):
            self.copy(k).wait_recv()
            self.mid[k // 3] = (self.raw[owner, half].astype(F32) + self.got[k].astype(F32)).astype(BF16)
            self.copy(k + 2).start()

    def end(self, out, squares):
        for plain, summed, half in ((4, 2, self.a), (1, 5, self.b)):
            self.copy(plain).wait_recv()
            self.copy(summed).wait_recv()
            total = self.raw[0, half].astype(F32) + self.got[plain].astype(F32) + self.got[summed].astype(F32)
            total = total.astype(BF16)
            out[0, half] = total
            total = total.astype(F32)
            squares[...] += jnp.sum((total * total).reshape(-1, 8, total.shape[1]), 0)

    def sent(self, *which):
        for k in which:
            self.copy(k).wait_send()


def lay_out(n, raw, gacc, uacc, dacc):
    me = lax.axis_index("dp")
    rows = gacc.shape[0] // n
    for o in range(n):
        turn = lax.rem(o - me + n, n)
        raw[turn, :rows] = gacc[o * rows : (o + 1) * rows].astype(BF16)
        raw[turn, rows : 2 * rows] = uacc[o * rows : (o + 1) * rows].astype(BF16)
        for q in range(n):
            raw[turn, 2 * rows :, q * STRIPE : (q + 1) * STRIPE] = dacc[
                q * rows : (q + 1) * rows, o * STRIPE : (o + 1) * STRIPE
            ].astype(BF16)


def backward_parts(g, u, dact):
    dact = dact.astype(BF16).astype(F32)
    s = sigmoid(g)
    silu = g * s
    act = (silu * u).astype(BF16)
    du = (dact * silu).astype(BF16)
    dg = (dact * u * (s + silu * (1 - s))).astype(BF16)
    return act, dg, du


def states_gradient(da, h, dy):
    da = da.astype(BF16).astype(F32)
    wide = h.astype(F32)
    mean = jnp.mean(wide * wide, -1, keepdims=True) + 1e-6
    scale = lax.rsqrt(mean)
    dmean = jnp.sum(da * wide, -1, keepdims=True) * (-0.5 * scale / mean)
    back = (da * scale + wide * (dmean * (2.0 / wide.shape[1]))).astype(BF16)
    return (dy.astype(F32) + back.astype(F32)).astype(BF16)


def fetch(chunks, layer, whole, part, sems, c):
    n = sems.shape[0]
    for o in range(n):
        at = pl.ds(pl.multiple_of((o * chunks + c) * STRIPE, STRIPE), STRIPE)
        yield pltpu.make_async_copy(whole.at[layer, :, at], part.at[:, o * STRIPE : (o + 1) * STRIPE], sems.at[o])


def top_kernel(n, chunks, tiles, layer, *refs):
    a, a_t, dy, dy_t, h, wd, wg, wu, *refs = refs
    dh, dh_t, g_out, last, squares_out, *refs = refs
    gacc, uacc, dacc, da, raw, got, mid, squares, send, recv, local, wg_part, wu_part, w_sems = refs
    c, i = pl.program_id(0), pl.program_id(1)
    tm = a.shape[0]
    right, _, left = neighbours(n)
    before = jnp.maximum(c - 1, 0)
    slot, here, there = lax.rem(before, 2), lax.rem(c, 2), lax.rem(c + 1, 2)
    ring = Ring(n, raw, got.at[slot], mid, send.at[slot], recv.at[slot])

    def weights(c, slot):
        yield from fetch(chunks, layer, wg, wg_part.at[slot], w_sems.at[slot, 0], c)
        yield from fetch(chunks, layer, wu, wu_part.at[slot], w_sems.at[slot, 1], c)

    @pl.when(i == 0)
    def _():
        @pl.when(c == 0)
        def _():
            for copy in weights(c, here):
                copy.start()
            greet((right, left))
            squares[...] = jnp.zeros_like(squares)

        @pl.when(c > 0)
        def _():
            ring.begin()

        for copy in weights(c, here):
            copy.wait()

        @pl.when(c < chunks - 1)
        def _():
            for copy in weights(c + 1, there):
                copy.start()

    rows = pl.ds(pl.multiple_of(i * tm, tm), tm)
    pair = 2

    def work(at_end):
        parts = []
        for j in range(0, n, pair):
            to = slice(j * STRIPE, (j + pair) * STRIPE)
            w1, w2 = wg_part[here, :, to], wu_part[here, :, to]
            w3 = wd[0, j : j + pair, 0].reshape(pair * STRIPE, wd.shape[4])
            parts.append((to, w1, w2, dot(a[...], w1), dot(a[...], w2), dot_nt(dy[...], w3)))

        def states(fresh, dg, du, w1, w2):
            more = dot_nt(jnp.concatenate([dg, du], 1), jnp.concatenate([w1, w2], 1))
            da[rows, :] = jnp.where(fresh, 0.0, da[rows, :]) + more

        def weight_gradients(to, act, dg, du):
            for acc, left, right in ((gacc, a_t, dg), (uacc, a_t, du), (dacc, dy_t, act)):
                acc[:, to] = jnp.where(i == 0, 0.0, acc[:, to]) + dot(left[...], right)

        later = []
        for k, (to, w1, w2, g, u, dact) in enumerate(parts):
            fresh = (c == 0) & (k == 0)
            act, dg, du = backward_parts(g, u, dact)
            if at_end:
                states(fresh, dg, du, w1, w2)
                later.append((to, act, dg, du))
            else:
                weight_gradients(to, act, dg, du)
                states(fresh, dg, du, w1, w2)
        for one in later:
            weight_gradients(*one)
        if at_end:
            out = states_gradient(da[rows, :], h[...], dy[...])
            dh[...] = out
            dh_t[...] = out.T

    pl.when(c < chunks - 1)(lambda: work(False))
    pl.when(c == chunks - 1)(lambda: work(True))
    pl.when((c > 0) & (i == tiles // 2 - 1))(ring.go_on)

    @pl.when(i == tiles - 1)
    def _():
        @pl.when(c > 0)
        def _():
            ring.end(g_out, squares)
            ring.sent(*range(6))

        lay_out(n, raw, gacc, uacc, dacc)

        @pl.when(c == chunks - 1)
        def _():
            copy = pltpu.make_async_copy(raw, last, local)
            copy.start()
            squares_out[...] = squares[...]
            copy.wait()


def by_owner(n, w_down):
    layers, ff, d = w_down.shape
    return w_down.reshape(layers, n, ff // (n * STRIPE), STRIPE, d)


def top(n, chunks, layer, a, a_t, dy, dy_t, h, w_gate, w_up, w_down, tm=1024):
    t, d = a.shape
    width, tiles, block = n * STRIPE, t // tm, 3 * d // n
    row, col = pl.BlockSpec((tm, d), lambda c, i: (i, 0)), pl.BlockSpec((d, tm), lambda c, i: (0, i))
    at_end = lambda c, i: jnp.where(c == chunks - 1, i, 0)
    row_end, col_end = pl.BlockSpec((tm, d), lambda c, i: (at_end(c, i), 0)), pl.BlockSpec((d, tm), lambda c, i: (0, at_end(c, i)))
    down = pl.BlockSpec((1, n, 1, STRIPE, d), lambda c, i: (layer, 0, c, 0, 0))
    shapes = [
        jax.ShapeDtypeStruct((t, d), BF16),
        jax.ShapeDtypeStruct((d, t), BF16),
        jax.ShapeDtypeStruct((chunks - 1, block, width), BF16),
        jax.ShapeDtypeStruct((n, block, width), BF16),
        jax.ShapeDtypeStruct((8, width), F32),
    ]
    return pl.pallas_call(
        functools.partial(top_kernel, n, chunks, tiles, layer),
        grid=(chunks, tiles),
        in_specs=[row, col, row, col, row_end, down] + [pl.BlockSpec(memory_space=pl.ANY)] * 2,
        out_specs=[
            row_end,
            col_end,
            pl.BlockSpec((1, block, width), lambda c, i: (jnp.maximum(c - 1, 0), 0, 0)),
            pl.BlockSpec(memory_space=pl.ANY),
            pl.BlockSpec((8, width), lambda c, i: (0, 0)),
        ],
        out_shape=shapes,
        scratch_shapes=[pltpu.VMEM((d, width), F32)] * 3
        + [
            pltpu.VMEM((t, d), F32),
            pltpu.VMEM((n, block, width), BF16),
            pltpu.VMEM((2, 6, block // 2, width), BF16),
            pltpu.VMEM((2, block // 2, width), BF16),
            pltpu.VMEM((8, width), F32),
            pltpu.SemaphoreType.DMA((2, 6)),
            pltpu.SemaphoreType.DMA((2, 6)),
            pltpu.SemaphoreType.DMA,
            pltpu.VMEM((2, d, width), BF16),
            pltpu.VMEM((2, d, width), BF16),
            pltpu.SemaphoreType.DMA((2, 2, n)),
        ],
        compiler_params=pltpu.CompilerParams(vmem_limit_bytes=67043328, collective_id=0, has_side_effects=True),
        cost_estimate=cost(16 * t * d * width * chunks, chunks * nbytes(a, a_t, dy, dy_t)),
        name="top",
    )(a, a_t, dy, dy_t, h, by_owner(n, w_down), w_gate, w_up)


def bottom_kernel(n, chunks, tiles, *refs):
    a_t, dy, dy_t, gate, up, *refs = refs
    wd, *refs = refs
    first, squares_in, g_out, squares_out, gacc, uacc, dacc, raw, got, mid, squares, send, recv, local, others, to, fro = refs
    c, i = pl.program_id(0), pl.program_id(1)
    right, opposite, left = neighbours(n)

    def ring(k):
        slot = lax.rem(k, 2)
        return Ring(n, raw.at[slot], got.at[k], mid.at[slot], send.at[k], recv.at[k])

    @pl.when((c == 0) & (i == 0))
    def _():
        copy = pltpu.make_async_copy(first, raw.at[0], local)
        copy.start()
        greet((right, opposite, left))
        squares[...] = squares_in[...]
        copy.wait()

    @pl.when(i == 0)
    def _():
        ring(c).begin((0, 3))

    @pl.when(c < chunks)
    def _():
        pair = 2
        parts = []
        for j in range(0, n, pair):
            w = wd[0, j : j + pair, 0].reshape(pair * STRIPE, wd.shape[4])
            parts.append((slice(j * STRIPE, (j + pair) * STRIPE), dot_nt(dy[...], w)))
        for to, dact in parts:
            act, dg, du = backward_parts(gate[0, :, to], up[0, :, to], dact)
            for acc, left, right in ((gacc, a_t, dg), (uacc, a_t, du), (dacc, dy_t, act)):
                acc[:, to] = jnp.where(i == 0, 0.0, acc[:, to]) + dot(left[...], right)

    @pl.when(i == tiles // 4)
    def _():
        @pl.when(c > 0)
        def _():
            before = ring(c - 1)
            before.end(g_out, squares)
            before.sent(*range(6))

        ring(c).begin((1, 4))

    pl.when(i == tiles // 2)(lambda: ring(c).go_on())

    @pl.when((c < chunks) & (i == tiles - 1))
    def _():
        lay_out(n, raw.at[lax.rem(c + 1, 2)], gacc, uacc, dacc)

    @pl.when((c == chunks) & (i == tiles - 1))
    def _():
        final = ring(c)
        final.end(g_out, squares)
        final.sent(*range(6))
        copies = [
            remote(squares, others.at[k], to.at[k], fro.at[k], device) for k, device in enumerate((right, opposite, left))
        ]
        for copy in copies:
            copy.start()
        for copy in copies:
            copy.wait()
        squares_out[...] = squares[...] + (others[0] + others[1] + others[2])


def bottom(n, chunks, layer, a_t, dy, dy_t, gate, up, w_down, first, squares, tm=1024):
    d, t = a_t.shape
    width, tiles, block = n * STRIPE, t // tm, 3 * d // n
    tile = lambda c, i: jnp.where(c < chunks, i, tiles - 1)
    chunk = lambda c: jnp.minimum(c, chunks - 1)
    row, col = pl.BlockSpec((tm, d), lambda c, i: (tile(c, i), 0)), pl.BlockSpec((d, tm), lambda c, i: (0, tile(c, i)))
    wide = pl.BlockSpec((1, tm, width), lambda c, i: (chunk(c), tile(c, i), 0))
    small = pl.BlockSpec((8, width), lambda c, i: (0, 0))
    down = pl.BlockSpec((1, n, 1, STRIPE, d), lambda c, i: (layer, 0, chunk(c), 0, 0))
    done = lambda c, i: jnp.where((c == chunks) & (i == tiles - 1), chunks, jnp.maximum(c - 1, 0))
    return pl.pallas_call(
        functools.partial(bottom_kernel, n, chunks, tiles),
        grid=(chunks + 1, tiles),
        in_specs=[col, row, col, wide, wide, down, pl.BlockSpec(memory_space=pl.ANY), small],
        out_specs=[pl.BlockSpec((1, block, width), lambda c, i: (done(c, i), 0, 0)), small],
        out_shape=[
            jax.ShapeDtypeStruct((chunks + 1, block, width), BF16),
            jax.ShapeDtypeStruct((8, width), F32),
        ],
        scratch_shapes=[pltpu.VMEM((d, width), F32)] * 3
        + [
            pltpu.VMEM((2, n, block, width), BF16),
            pltpu.VMEM((chunks + 1, 6, block // 2, width), BF16),
            pltpu.VMEM((2, 2, block // 2, width), BF16),
            pltpu.VMEM((8, width), F32),
            pltpu.SemaphoreType.DMA((chunks + 1, 6)),
            pltpu.SemaphoreType.DMA((chunks + 1, 6)),
            pltpu.SemaphoreType.DMA,
            pltpu.VMEM((3, 8, width), F32),
            pltpu.SemaphoreType.DMA((3,)),
            pltpu.SemaphoreType.DMA((3,)),
        ],
        compiler_params=pltpu.CompilerParams(vmem_limit_bytes=VMEM_LIMIT, collective_id=1, has_side_effects=True),
        cost_estimate=cost(8 * t * d * width * chunks, nbytes(gate, up) + chunks * nbytes(a_t, dy, dy_t)),
        name="bottom",
    )(a_t, dy, dy_t, gate, up, by_owner(n, w_down), first, squares)


def adam_kernel(chunks, tall, count, squares, w, m, v, g_top, g_bottom, *refs):
    *w_out, m_out, v_out = refs
    factor = jnp.minimum(1.0, 0.5 * lax.rsqrt(jnp.full((1, 1), jnp.sum(squares[...])) / count + 1e-30))

    def work(layer, c, g):
        at = pl.ds(pl.multiple_of(c * STRIPE, STRIPE), STRIPE)
        i = (at, slice(None)) if tall else (slice(None), at)
        g = g.astype(F32)
        if tall:
            g = jnp.concatenate([g[:, q : q + STRIPE].T for q in range(0, g.shape[1], STRIPE)], 1)
        g = g * factor
        m_new = 0.9 * m[layer, *i] + 0.1 * g
        v_new = 0.95 * v[layer, *i] + 0.05 * g * g
        old = w[layer, *i].astype(F32)
        step = m_new * lax.rsqrt(v_new + 1e-8) + 0.1 * old
        w_out[layer][i] = (old - 0.02 * step).astype(BF16)
        m_out[layer, *i] = m_new
        v_out[layer, *i] = v_new

    @pl.loop(0, chunks - 1)
    def _(c):
        work(0, c, g_bottom[c + 1])
        work(1, c, g_top[c])

    work(0, chunks - 1, g_bottom[chunks])
    work(1, chunks - 1, g_bottom[0])


def adam(me, squares, w, m, v, g_top, g_bottom, which, count, chunks, tall, first, blocks, begun):
    layers, rows, _ = m.shape
    g_rows = g_top.shape[1] // 3
    g_width, width = (2 * STRIPE, 2 * g_rows) if tall else (STRIPE, STRIPE * chunks)
    block = pl.BlockSpec((layers, rows, width), lambda i, me: (0, 0, first + i))
    out = [jax.ShapeDtypeStruct((rows, width * blocks), BF16)] * layers + [jax.ShapeDtypeStruct(m.shape, F32)] * 2
    fixed = list(begun)

    def body(me_ref, *refs):
        adam_kernel(chunks, tall, count, *refs[:6], *refs[6 + len(fixed) :])

    outs = pl.pallas_call(
        body,
        grid_spec=pltpu.PrefetchScalarGridSpec(
            num_scalar_prefetch=1,
            grid=(blocks,),
            in_specs=[pl.BlockSpec(squares.shape, lambda i, me: (0, 0))]
            + [pl.BlockSpec((layers, rows, width), lambda i, me: (0, me[0], first + i)), block, block]
            + [pl.BlockSpec((g.shape[0], g_rows, g_width), lambda i, me: (0, which, first + i)) for g in (g_top, g_bottom)]
            + [pl.BlockSpec(memory_space=pl.ANY)] * len(fixed),
            out_specs=[pl.BlockSpec((rows, width), lambda i, me: (0, i))] * layers + [block, block],
        ),
        out_shape=out,
        input_output_aliases={7 + k: layers + k for k in range(len(fixed))},
        compiler_params=params(),
        cost_estimate=cost(16 * rows * width * blocks * layers, 22 * rows * width * blocks * layers),
        name="adam",
    )(me, squares, w, m, v, g_top, g_bottom, *fixed)
    return outs[:layers], outs[layers:]


def place_kernel(sources, me_ref, *refs):
    pieces, out = refs[:sources], refs[-1]
    k = pl.program_id(1)
    for at, piece in enumerate(pieces):
        pl.when(k == at)(lambda piece=piece: out.__setitem__(0, piece[...]))


def place(me, shape, pieces, first, blocks, begun):
    arrays, where = zip(*pieces, strict=True)
    rows, width = arrays[0].shape[0], arrays[0].shape[1] // blocks
    n = shape[1] // rows

    def at(j, k, me):
        layer, turn = 0, 0
        for i, (its_layer, its_turn) in enumerate(where):
            layer, turn = jnp.where(k == i, its_layer, layer), jnp.where(k == i, its_turn, turn)
        return layer, lax.rem(me[0] + turn, n), first + j

    fixed = list(begun)
    return pl.pallas_call(
        functools.partial(place_kernel, len(arrays)),
        grid_spec=pltpu.PrefetchScalarGridSpec(
            num_scalar_prefetch=1,
            grid=(blocks, len(arrays)),
            in_specs=[pl.BlockSpec((rows, width), lambda j, k, me: (0, j))] * len(arrays)
            + [pl.BlockSpec(memory_space=pl.ANY)] * len(fixed),
            out_specs=pl.BlockSpec((1, rows, width), at),
        ),
        out_shape=jax.ShapeDtypeStruct(shape, arrays[0].dtype),
        input_output_aliases={1 + len(arrays): 0} if fixed else {},
        compiler_params=params(),
        cost_estimate=cost(arrays[0].size, 4 * nbytes(*arrays)),
        name="place",
    )(me, *arrays, *fixed)


def send_around(n, own):
    right, left = [(i, (i + 1) % n) for i in range(n)], [(i, (i - 1) % n) for i in range(n)]

    def send(one, way):
        return lax.ppermute(one, "dp", way)

    l0, r1 = send(own[0], right), send(own[1], left)
    l1, r0 = send(own[1], right), send(own[0], left)
    return (l0, l1), (r0, r1), lambda: (send(l0, right), send(r1, left))


def solution(mesh):
    n = mesh.shape["dp"]

    def step(x, dy, w_gate, w_up, w_down, m_gate, m_up, m_down, v_gate, v_up, v_down):
        x, dy = x[0], dy[0]
        chunks = w_gate.shape[2] // (n * STRIPE)
        me = lax.axis_index("dp").astype(jnp.int32).reshape(1)

        gate, up, a0_t, h1, a1, a1_t, dy_t = forward(n, chunks, x, dy, w_gate, w_up, w_down)
        dh, dh_t, g_top, last, squares = top(n, chunks, 1, a1, a1_t, dy, dy_t, h1, w_gate, w_up, w_down)
        g_bottom, squares = bottom(n, chunks, 0, a0_t, dh, dh_t, gate, up, w_down, last, squares)

        states = ((w_gate, m_gate, v_gate), (w_up, m_up, v_up), (w_down, m_down, v_down))
        moments, whole, sent, count = [[], [], []], [[], [], []], [], 3 * w_gate.size
        for which, first, blocks in PIECES:
            own, moments[which] = adam(
                me, squares, *states[which], g_top, g_bottom, which, count, chunks, which == 2, first, blocks, moments[which]
            )
            squares = lax.optimization_barrier((squares, *own))[0]
            sent.append((own, *send_around(n, own)))
        for k, (which, first, blocks) in enumerate(PIECES):
            own, left, right, _ = sent[k]
            near = [(one, (layer, turn)) for turn, pair in ((0, own), (n - 1, left), (1, right)) for layer, one in enumerate(pair)]
            whole[which] = [place(me, states[which][0].shape, near, first, blocks, whole[which])]
        for k, (which, first, blocks) in enumerate(PIECES):
            far = [(one, (layer, 2)) for layer, one in enumerate(sent[k][3]())]
            whole[which] = [place(me, states[which][0].shape, far, first, blocks, whole[which])]
        return (*(one[0] for one in whole), *(one[0] for one in moments), *(one[1] for one in moments))

    seq, part, rows = P(("rep", "dp"), None, None), P("rep", None, None), P("rep", "dp", None)
    state = P(None, "dp", None)
    step = jax.shard_map(
        step,
        mesh=mesh,
        in_specs=(seq, seq) + (P(None, None, None),) * 3 + (state,) * 6,
        out_specs=(part,) * 3 + (rows,) * 6,
        check_vma=False,
    )
    return step
```

```python
import functools

import jax
import jax.numpy as jnp
from jax import lax
from jax.experimental import pallas as pl
from jax.experimental.pallas import tpu as pltpu
from jax.sharding import PartitionSpec as P


F32, BF16 = jnp.float32, jnp.bfloat16
STRIPE = 128
VMEM_LIMIT = 60 << 20
EARLY = 0
PIECES = ((0, 0, 1, False), (0, 1, 3, False), (2, 0, 2, True), (1, 0, 3, True), (1, 3, 1, False))


def dot(a, b):
    return jnp.dot(a, b, preferred_element_type=F32)


def dot_nt(a, b):
    return lax.dot_general(a, b, (((1,), (1,)), ((), ())), preferred_element_type=F32)


def sigmoid(x):
    return 0.5 * jnp.tanh(0.5 * x) + 0.5


def normed(h):
    wide = h.astype(F32)
    scale = lax.rsqrt(jnp.mean(wide * wide, -1, keepdims=True) + 1e-6)
    return (wide * scale).astype(BF16)


def cost(flops, read_and_written):
    return pl.CostEstimate(flops=int(flops), bytes_accessed=int(read_and_written), transcendentals=0)


def params(**more):
    return pltpu.CompilerParams(vmem_limit_bytes=VMEM_LIMIT, **more)


def nbytes(*arrays):
    return sum(a.size * jnp.dtype(a.dtype).itemsize for a in arrays)


def once(shape, index_map):
    return pl.BlockSpec(shape, index_map, pipeline_mode=pl.Buffered(1))


def stripes(n, chunks, c):
    return [slice((o * chunks + c) * STRIPE, (o * chunks + c + 1) * STRIPE) for o in range(n)]


def forward_kernel(n, chunks, tiles, *refs):
    x_first, x_next, x_before, dy, wg, wu, wd, *refs = refs
    moments, (gate, up, a_t, h1, a1, a1_t, dy_t, near_a, near_b), refs = refs[:6], refs[6:15], refs[15:]
    act, normal, y, pack_a, pack_b, packed, own, send, recv = refs
    m = pl.program_id(0)
    width = n * STRIPE
    right, _, left = neighbours(n)

    def packing():
        for k, ref in enumerate(moments[:4]):
            for o, s in enumerate(stripes(n, chunks, EARLY)):
                yield pltpu.make_async_copy(
                    ref.at[1, :, s], pack_a.at[k, :, o * STRIPE : (o + 1) * STRIPE], packed.at[k * n + o]
                )
        for k, ref in enumerate(moments[4:]):
            rows = slice(EARLY * STRIPE, (EARLY + 1) * STRIPE)
            yield pltpu.make_async_copy(ref.at[1, rows, :], pack_b.at[k], packed.at[4 * n + k])

    def copies():
        for k, (part, near) in enumerate(((pack_a, near_a), (pack_b, near_b))):
            yield remote(part, near.at[0], send.at[k], recv.at[k], right)
            yield remote(part, near.at[1], send.at[2 + k], recv.at[2 + k], left)
            yield pltpu.make_async_copy(part, near.at[2], own.at[k])

    def finish():
        h = (x_before[...].astype(F32) + y[...].astype(F32)).astype(BF16)
        h1[...] = h
        out = normed(h)
        a1[...] = out
        a1_t[...] = out.T

    @pl.when(m == 0)
    def _():
        for copy in packing():
            copy.start()
        hail((right, left))
        normal[0] = normed(x_first[...])

    @pl.when(m == 1)
    def _():
        pl.semaphore_wait(pltpu.get_barrier_semaphore(), 2)
        for copy in packing():
            copy.wait()
        for copy in copies():
            copy.start()

    @pl.when(m < tiles)
    def _():
        a = normal[lax.rem(m, 2)]

        def dots(c):
            for o, w in ((gate, wg), (up, wu)):
                o[c] = dot(a, jnp.concatenate([w[0, :, s] for s in stripes(n, chunks, c)], 1))

        dots(0)
        for c in range(chunks):
            if c + 1 < chunks:
                dots(c + 1)
            g = gate[c]
            act[:, c * width : (c + 1) * width] = (g * sigmoid(g) * up[c]).astype(BF16)
        a_t[...] = a.T
        dy_t[...] = dy[...].T
        finish()
        down = jnp.concatenate([wd[0, s, :] for c in range(chunks) for s in stripes(n, chunks, c)], 0)
        y[...] = dot(act[...], down).astype(BF16)
        normal[lax.rem(m + 1, 2)] = normed(x_next[...])

    @pl.when(m == tiles)
    def _():
        finish()
        for copy in copies():
            copy.wait()


def forward(n, chunks, x, dy, w_gate, w_up, w_down, moments, tm=256):
    t, d = x.shape
    ff, tiles, width = w_gate.shape[2], t // tm, n * STRIPE
    here, before = lambda m: jnp.minimum(m, tiles - 1), lambda m: jnp.maximum(m - 1, 0)
    row = lambda at: pl.BlockSpec((tm, d), lambda m: (at(m), 0))
    col = lambda at: pl.BlockSpec((d, tm), lambda m: (0, at(m)))
    wide = pl.BlockSpec((chunks, tm, width), lambda m: (0, here(m), 0))
    pack_a, pack_b = (4, d // n, width), (2, STRIPE, d)
    out = [jax.ShapeDtypeStruct((chunks, t, width), F32)] * 2
    out += [jax.ShapeDtypeStruct(s, BF16) for s in ((d, t), (t, d), (t, d), (d, t), (d, t))]
    out += [jax.ShapeDtypeStruct((3, *s), F32) for s in (pack_a, pack_b)]
    whole = pl.BlockSpec(memory_space=pl.ANY)
    return pl.pallas_call(
        functools.partial(forward_kernel, n, chunks, tiles),
        grid=(tiles + 1,),
        in_specs=[once((tm, d), lambda m: (0, 0)), row(lambda m: jnp.minimum(m + 1, tiles - 1)), row(before), row(here)]
        + [once((1, d, ff), lambda m: (0, 0, 0))] * 2
        + [once((1, ff, d), lambda m: (0, 0, 0))]
        + [whole] * 6,
        out_specs=[wide] * 2 + [col(here), row(before), row(before), col(before), col(here), whole, whole],
        out_shape=out,
        scratch_shapes=[
            pltpu.VMEM((tm, ff), BF16),
            pltpu.VMEM((2, tm, d), BF16),
            pltpu.VMEM((tm, d), BF16),
            pltpu.VMEM(pack_a, F32),
            pltpu.VMEM(pack_b, F32),
            pltpu.SemaphoreType.DMA((4 * n + 2,)),
            pltpu.SemaphoreType.DMA((2,)),
            pltpu.SemaphoreType.DMA((4,)),
            pltpu.SemaphoreType.DMA((4,)),
        ],
        compiler_params=params(collective_id=2, has_side_effects=True),
        cost_estimate=cost(6 * t * d * ff, nbytes(*out)),
        name="forward",
    )(x, x, x, dy, w_gate, w_up, w_down, *moments)


def neighbours(n):
    me = lax.axis_index("dp")
    return lax.rem(me + 1, n), lax.rem(me + 2, n), lax.rem(me + n - 1, n)


def hail(devices):
    barrier = pltpu.get_barrier_semaphore()
    for device in devices:
        pl.semaphore_signal(barrier, inc=1, device_id={"dp": device}, device_id_type=pl.DeviceIdType.MESH)


def greet(devices):
    hail(devices)
    pl.semaphore_wait(pltpu.get_barrier_semaphore(), len(devices))


def remote(src, dst, send, recv, device):
    return pltpu.make_async_remote_copy(
        src_ref=src, dst_ref=dst, send_sem=send, recv_sem=recv, device_id={"dp": device}, device_id_type=pl.DeviceIdType.MESH
    )


class Ring:
    def __init__(self, n, raw, got, mid, send, recv):
        half = raw.shape[1] // 2
        self.a, self.b = pl.ds(0, half), pl.ds(half, half)
        self.raw, self.got, self.mid = raw, got, mid
        self.send, self.recv = send, recv
        self.right, _, self.left = neighbours(n)

    def copy(self, k):
        source = (
            lambda: self.raw.at[2, self.a],
            lambda: self.raw.at[1, self.b],
            lambda: self.mid.at[0],
            lambda: self.raw.at[2, self.b],
            lambda: self.raw.at[3, self.a],
            lambda: self.mid.at[1],
        )[k]()
        return remote(source, self.got.at[k], self.send.at[k], self.recv.at[k], self.right if k < 3 else self.left)

    def begin(self, which=(0, 3, 1, 4)):
        for k in which:
            self.copy(k).start()

    def go_on(self):
        for k, owner, half in ((0, 1, self.a), (3, 3, self.b)):
            self.copy(k).wait_recv()
            self.mid[k // 3] = (self.raw[owner, half].astype(F32) + self.got[k].astype(F32)).astype(BF16)
            self.copy(k + 2).start()

    def end(self, out, squares):
        for plain, summed, half in ((4, 2, self.a), (1, 5, self.b)):
            self.copy(plain).wait_recv()
            self.copy(summed).wait_recv()
            total = self.raw[0, half].astype(F32) + self.got[plain].astype(F32) + self.got[summed].astype(F32)
            total = total.astype(BF16)
            out[0, half] = total
            total = total.astype(F32)
            squares[...] += jnp.sum((total * total).reshape(-1, 8, total.shape[1]), 0)

    def sent(self, *which):
        for k in which:
            self.copy(k).wait_send()


def lay_out(n, raw, gacc, uacc, dacc):
    me = lax.axis_index("dp")
    rows = gacc.shape[0] // n

    @pl.loop(0, n)
    def _(o):
        turn = lax.rem(o - me + n, n)
        mine, stripe = pl.ds(pl.multiple_of(o * rows, rows), rows), pl.ds(pl.multiple_of(o * STRIPE, STRIPE), STRIPE)
        raw[turn, :rows] = gacc[mine].astype(BF16)
        raw[turn, rows : 2 * rows] = uacc[mine].astype(BF16)
        for q in range(n):
            raw[turn, 2 * rows :, q * STRIPE : (q + 1) * STRIPE] = dacc[q * rows : (q + 1) * rows, stripe].astype(BF16)


def backward_parts(g, u, dact):
    dact = dact.astype(BF16).astype(F32)
    s = sigmoid(g)
    silu = g * s
    act = (silu * u).astype(BF16)
    du = (dact * silu).astype(BF16)
    dg = (dact * u * (s + silu * (1 - s))).astype(BF16)
    return act, dg, du


def states_gradient(da, h, dy):
    da = da.astype(BF16).astype(F32)
    wide = h.astype(F32)
    mean = jnp.mean(wide * wide, -1, keepdims=True) + 1e-6
    scale = lax.rsqrt(mean)
    dmean = jnp.sum(da * wide, -1, keepdims=True) * (-0.5 * scale / mean)
    back = (da * scale + wide * (dmean * (2.0 / wide.shape[1]))).astype(BF16)
    return (dy.astype(F32) + back.astype(F32)).astype(BF16)


def fetch(chunks, layer, whole, part, sems, c):
    n = sems.shape[0]
    for o in range(n):
        at = pl.ds(pl.multiple_of((o * chunks + c) * STRIPE, STRIPE), STRIPE)
        yield pltpu.make_async_copy(whole.at[layer, :, at], part.at[:, o * STRIPE : (o + 1) * STRIPE], sems.at[o])


def top_kernel(n, chunks, tiles, layer, *refs):
    a, a_t, dy, dy_t, h, wd, wg, wu, near_a, near_b, *refs = refs
    dh, dh_t, g_out, last, squares_out, far_a, far_b, g_all, *refs = refs
    gacc, uacc, dacc, da, raw, got, mid, squares, send, recv, local, wg_part, wu_part, w_sems, mine, e_send, e_recv = refs
    c, i = pl.program_id(0), pl.program_id(1)
    tm = a.shape[0]
    right, _, left = neighbours(n)
    before = jnp.maximum(c - 1, 0)
    slot, here, there = lax.rem(before, 2), lax.rem(c, 2), lax.rem(c + 1, 2)
    ring = Ring(n, raw, got.at[slot], mid, send.at[slot], recv.at[slot])

    def moments():
        for k, (near, far) in enumerate(((near_a, far_a), (near_b, far_b))):
            half = far.shape[0] // 2
            one, other = slice(0, half), slice(half, None)
            yield remote(near.at[0, one], far.at[one], e_send.at[0, k], e_recv.at[0, k], right)
            yield remote(near.at[1, other], far.at[other], e_send.at[1, k], e_recv.at[1, k], left)

    def early():
        yield remote(mine, g_all.at[0], e_send.at[2, 0], e_recv.at[2, 0], right)
        yield remote(mine, g_all.at[1], e_send.at[2, 1], e_recv.at[2, 1], left)

    def early_on():
        half = mine.shape[0] // 2
        one, other = pl.ds(0, half), pl.ds(half, half)
        yield remote(g_all.at[0, one], g_all.at[2, one], e_send.at[3, 0], e_recv.at[3, 0], right)
        yield remote(g_all.at[1, other], g_all.at[2, other], e_send.at[3, 1], e_recv.at[3, 1], left)

    def weights(c, slot):
        yield from fetch(chunks, layer, wg, wg_part.at[slot], w_sems.at[slot, 0], c)
        yield from fetch(chunks, layer, wu, wu_part.at[slot], w_sems.at[slot, 1], c)

    @pl.when(i == 0)
    def _():
        @pl.when(c == 0)
        def _():
            for copy in weights(c, here):
                copy.start()
            greet((right, left))
            for copy in moments():
                copy.start()
            squares[...] = jnp.zeros_like(squares)

        @pl.when(c > 0)
        def _():
            ring.begin((0, 3))

        for copy in weights(c, here):
            copy.wait()

        @pl.when(c < chunks - 1)
        def _():
            for copy in weights(c + 1, there):
                copy.start()

    rows = pl.ds(pl.multiple_of(i * tm, tm), tm)
    pair = 2

    def work(at_end):
        parts = []
        for j in range(0, n, pair):
            to = slice(j * STRIPE, (j + pair) * STRIPE)
            w1, w2 = wg_part[here, :, to], wu_part[here, :, to]
            w3 = wd[0, j : j + pair, 0].reshape(pair * STRIPE, wd.shape[4])
            parts.append((to, w1, w2, dot(a[...], w1), dot(a[...], w2), dot_nt(dy[...], w3)))

        def states(fresh, dg, du, w1, w2):
            more = dot_nt(jnp.concatenate([dg, du], 1), jnp.concatenate([w1, w2], 1))
            da[rows, :] = jnp.where(fresh, 0.0, da[rows, :]) + more

        def weight_gradients(to, act, dg, du):
            for acc, left, right in ((gacc, a_t, dg), (uacc, a_t, du), (dacc, dy_t, act)):
                acc[:, to] = jnp.where(i == 0, 0.0, acc[:, to]) + dot(left[...], right)

        later = []
        for k, (to, w1, w2, g, u, dact) in enumerate(parts):
            fresh = (c == 0) & (k == 0)
            act, dg, du = backward_parts(g, u, dact)
            if at_end:
                states(fresh, dg, du, w1, w2)
                later.append((to, act, dg, du))
            else:
                weight_gradients(to, act, dg, du)
                states(fresh, dg, du, w1, w2)
        for one in later:
            weight_gradients(*one)
        if at_end:
            out = states_gradient(da[rows, :], h[...], dy[...])
            dh[...] = out
            dh_t[...] = out.T

    pl.when(c < chunks - 1)(lambda: work(False))
    pl.when(c == chunks - 1)(lambda: work(True))
    pl.when((c > 0) & (i == 0))(lambda: ring.begin((1, 4)))

    @pl.when((c > 0) & (i == tiles // 2 - 1))
    def _():
        ring.go_on()

        @pl.when(c == 1)
        def _():
            for copy in moments():
                copy.wait()

        @pl.when(c == EARLY + 2)
        def _():
            for copy in early():
                copy.start()

        @pl.when(c == EARLY + 3)
        def _():
            for copy in early():
                copy.wait()
            for copy in early_on():
                copy.start()

        @pl.when(c == EARLY + 4)
        def _():
            for copy in early_on():
                copy.wait()

    @pl.when(i == tiles - 1)
    def _():
        @pl.when(c > 0)
        def _():
            ring.end(g_out, squares)
            ring.sent(*range(6))

        @pl.when(c == EARLY + 1)
        def _():
            mine[...] = g_out[0]

        lay_out(n, raw, gacc, uacc, dacc)

        @pl.when(c == chunks - 1)
        def _():
            copy = pltpu.make_async_copy(raw, last, local)
            copy.start()
            squares_out[...] = squares[...]
            copy.wait()


def by_owner(n, w_down):
    layers, ff, d = w_down.shape
    return w_down.reshape(layers, n, ff // (n * STRIPE), STRIPE, d)


def top(n, chunks, layer, a, a_t, dy, dy_t, h, w_gate, w_up, w_down, near_a, near_b, tm=1024):
    t, d = a.shape
    width, tiles, block = n * STRIPE, t // tm, 3 * d // n
    row, col = pl.BlockSpec((tm, d), lambda c, i: (i, 0)), pl.BlockSpec((d, tm), lambda c, i: (0, i))
    at_end = lambda c, i: jnp.where(c == chunks - 1, i, 0)
    row_end, col_end = pl.BlockSpec((tm, d), lambda c, i: (at_end(c, i), 0)), pl.BlockSpec((d, tm), lambda c, i: (0, at_end(c, i)))
    down = pl.BlockSpec((1, n, 1, STRIPE, d), lambda c, i: (layer, 0, c, 0, 0))
    shapes = [
        jax.ShapeDtypeStruct((t, d), BF16),
        jax.ShapeDtypeStruct((d, t), BF16),
        jax.ShapeDtypeStruct((chunks - 1, block, width), BF16),
        jax.ShapeDtypeStruct((n, block, width), BF16),
        jax.ShapeDtypeStruct((8, width), F32),
        jax.ShapeDtypeStruct(near_a.shape[1:], F32),
        jax.ShapeDtypeStruct(near_b.shape[1:], F32),
        jax.ShapeDtypeStruct((3, block, width), BF16),
    ]
    return pl.pallas_call(
        functools.partial(top_kernel, n, chunks, tiles, layer),
        grid=(chunks, tiles),
        in_specs=[row, col, row, col, row_end, down] + [pl.BlockSpec(memory_space=pl.ANY)] * 4,
        out_specs=[
            row_end,
            col_end,
            pl.BlockSpec((1, block, width), lambda c, i: (jnp.maximum(c - 1, 0), 0, 0)),
            pl.BlockSpec(memory_space=pl.ANY),
            pl.BlockSpec((8, width), lambda c, i: (0, 0)),
        ]
        + [pl.BlockSpec(memory_space=pl.ANY)] * 3,
        out_shape=shapes,
        scratch_shapes=[pltpu.VMEM((d, width), F32)] * 3
        + [
            pltpu.VMEM((t, d), F32),
            pltpu.VMEM((n, block, width), BF16),
            pltpu.VMEM((2, 6, block // 2, width), BF16),
            pltpu.VMEM((2, block // 2, width), BF16),
            pltpu.VMEM((8, width), F32),
            pltpu.SemaphoreType.DMA((2, 6)),
            pltpu.SemaphoreType.DMA((2, 6)),
            pltpu.SemaphoreType.DMA,
            pltpu.VMEM((2, d, width), BF16),
            pltpu.VMEM((2, d, width), BF16),
            pltpu.SemaphoreType.DMA((2, 2, n)),
            pltpu.VMEM((block, width), BF16),
            pltpu.SemaphoreType.DMA((4, 2)),
            pltpu.SemaphoreType.DMA((4, 2)),
        ],
        compiler_params=pltpu.CompilerParams(vmem_limit_bytes=67043328, collective_id=0, has_side_effects=True),
        cost_estimate=cost(16 * t * d * width * chunks, chunks * nbytes(a, a_t, dy, dy_t)),
        name="top",
    )(a, a_t, dy, dy_t, h, by_owner(n, w_down), w_gate, w_up, near_a, near_b)


def bottom_kernel(n, chunks, tiles, *refs):
    a_t, dy, dy_t, gate, up, *refs = refs
    wd, *refs = refs
    first, squares_in, g_out, squares_out, gacc, uacc, dacc, raw, got, mid, squares, send, recv, local, all_squares, to, fro = refs
    c, i = pl.program_id(0), pl.program_id(1)
    right, opposite, left = neighbours(n)

    def ring(k):
        slot = lax.rem(k, 2)
        return Ring(n, raw.at[slot], got.at[k], mid.at[slot], send.at[k], recv.at[k])

    @pl.when((c == 0) & (i == 0))
    def _():
        copy = pltpu.make_async_copy(first, raw.at[0], local)
        copy.start()
        greet((right, opposite, left))
        squares[...] = squares_in[...]
        copy.wait()

    @pl.when(i == 0)
    def _():
        ring(c).begin((0, 3))

    @pl.when(c < chunks)
    def _():
        pair = 2
        parts = []
        for j in range(0, n, pair):
            w = wd[0, j : j + pair, 0].reshape(pair * STRIPE, wd.shape[4])
            parts.append((slice(j * STRIPE, (j + pair) * STRIPE), dot_nt(dy[...], w)))
        for to, dact in parts:
            act, dg, du = backward_parts(gate[0, :, to], up[0, :, to], dact)
            for acc, left, right in ((gacc, a_t, dg), (uacc, a_t, du), (dacc, dy_t, act)):
                acc[:, to] = jnp.where(i == 0, 0.0, acc[:, to]) + dot(left[...], right)

    @pl.when(i == tiles // 4)
    def _():
        @pl.when(c > 0)
        def _():
            before = ring(c - 1)
            before.end(g_out, squares)
            before.sent(*range(6))

        ring(c).begin((1, 4))

    pl.when(i == tiles // 2)(lambda: ring(c).go_on())

    @pl.when((c < chunks) & (i == tiles - 1))
    def _():
        lay_out(n, raw.at[lax.rem(c + 1, 2)], gacc, uacc, dacc)

    @pl.when((c == chunks) & (i == tiles - 1))
    def _():
        final = ring(c)
        final.end(g_out, squares)
        final.sent(*range(6))
        me = lax.axis_index("dp")
        all_squares[me] = squares[...]
        copies = [
            remote(squares, all_squares.at[me], to.at[k], fro.at[k], device) for k, device in enumerate((right, opposite, left))
        ]
        for copy in copies:
            copy.start()
        for copy in copies:
            copy.wait()
        total = all_squares[0]
        for k in range(1, n):
            total += all_squares[k]
        squares_out[...] = total


def bottom(n, chunks, layer, a_t, dy, dy_t, gate, up, w_down, first, squares, tm=1024):
    d, t = a_t.shape
    width, tiles, block = n * STRIPE, t // tm, 3 * d // n
    tile = lambda c, i: jnp.where(c < chunks, i, tiles - 1)
    chunk = lambda c: jnp.minimum(c, chunks - 1)
    row, col = pl.BlockSpec((tm, d), lambda c, i: (tile(c, i), 0)), pl.BlockSpec((d, tm), lambda c, i: (0, tile(c, i)))
    wide = pl.BlockSpec((1, tm, width), lambda c, i: (chunk(c), tile(c, i), 0))
    small = pl.BlockSpec((8, width), lambda c, i: (0, 0))
    down = pl.BlockSpec((1, n, 1, STRIPE, d), lambda c, i: (layer, 0, chunk(c), 0, 0))
    done = lambda c, i: jnp.where((c == chunks) & (i == tiles - 1), chunks, jnp.maximum(c - 1, 0))
    return pl.pallas_call(
        functools.partial(bottom_kernel, n, chunks, tiles),
        grid=(chunks + 1, tiles),
        in_specs=[col, row, col, wide, wide, down, pl.BlockSpec(memory_space=pl.ANY), small],
        out_specs=[pl.BlockSpec((1, block, width), lambda c, i: (done(c, i), 0, 0)), small],
        out_shape=[
            jax.ShapeDtypeStruct((chunks + 1, block, width), BF16),
            jax.ShapeDtypeStruct((8, width), F32),
        ],
        scratch_shapes=[pltpu.VMEM((d, width), F32)] * 3
        + [
            pltpu.VMEM((2, n, block, width), BF16),
            pltpu.VMEM((chunks + 1, 6, block // 2, width), BF16),
            pltpu.VMEM((2, 2, block // 2, width), BF16),
            pltpu.VMEM((8, width), F32),
            pltpu.SemaphoreType.DMA((chunks + 1, 6)),
            pltpu.SemaphoreType.DMA((chunks + 1, 6)),
            pltpu.SemaphoreType.DMA,
            pltpu.VMEM((n, 8, width), F32),
            pltpu.SemaphoreType.DMA((3,)),
            pltpu.SemaphoreType.DMA((3,)),
        ],
        compiler_params=pltpu.CompilerParams(vmem_limit_bytes=VMEM_LIMIT, collective_id=1, has_side_effects=True),
        cost_estimate=cost(8 * t * d * width * chunks, nbytes(gate, up) + chunks * nbytes(a_t, dy, dy_t)),
        name="bottom",
    )(a_t, dy, dy_t, gate, up, by_owner(n, w_down), first, squares)


def clip(squares, count):
    return jnp.minimum(1.0, 0.5 * lax.rsqrt(jnp.full((1, 1), jnp.sum(squares)) / count + 1e-30))


def adamw(w, m, v, g):
    m = 0.9 * m + 0.1 * g
    v = 0.95 * v + 0.05 * g * g
    old = w.astype(F32)
    step = m * lax.rsqrt(v + 1e-8) + 0.1 * old
    return (old - 0.02 * step).astype(BF16), m, v


def upright(g):
    return jnp.concatenate([g[:, q : q + STRIPE].T for q in range(0, g.shape[1], STRIPE)], 1)


def adam_kernel(chunks, tall, count, squares, w, m, v, g_top, g_bottom, *refs):
    *w_out, m_out, v_out = refs
    factor = clip(squares[...], count)

    def work(layer, c, g, to):
        def at(c):
            rows = pl.ds(pl.multiple_of(c * STRIPE, STRIPE), STRIPE)
            return (rows, slice(None)) if tall else (slice(None), rows)

        g = upright(g.astype(F32)) if tall else g.astype(F32)
        new, m_new, v_new = adamw(w[layer, *at(c)], m[layer, *at(c)], v[layer, *at(c)], g * factor)
        if to is not None:
            w_out[layer][at(to)] = new
        m_out[layer, *at(c)] = m_new
        v_out[layer, *at(c)] = v_new

    work(0, EARLY, g_bottom[EARLY + 1], EARLY)
    work(1, EARLY, g_top[EARLY], None)

    @pl.loop(EARLY + 1, chunks - 1)
    def _(c):
        work(0, c, g_bottom[c + 1], c)
        work(1, c, g_top[c], c - 1)

    work(0, chunks - 1, g_bottom[chunks], chunks - 1)
    work(1, chunks - 1, g_bottom[0], chunks - 2)


def adam(me, squares, w, m, v, g_top, g_bottom, which, count, chunks, tall, first, blocks, begun):
    layers, rows, _ = m.shape
    g_rows = g_top.shape[1] // 3
    g_width, width = (2 * STRIPE, 2 * g_rows) if tall else (STRIPE, STRIPE * chunks)
    block = pl.BlockSpec((layers, rows, width), lambda i, me: (0, 0, first + i))
    new = [(rows, width), (rows - STRIPE, width) if tall else (rows, width - STRIPE)]
    out = [jax.ShapeDtypeStruct((r, c * blocks), BF16) for r, c in new] + [jax.ShapeDtypeStruct(m.shape, F32)] * 2
    fixed = list(begun)

    def body(me_ref, *refs):
        adam_kernel(chunks, tall, count, *refs[:6], *refs[6 + len(fixed) :])

    outs = pl.pallas_call(
        body,
        grid_spec=pltpu.PrefetchScalarGridSpec(
            num_scalar_prefetch=1,
            grid=(blocks,),
            in_specs=[pl.BlockSpec(squares.shape, lambda i, me: (0, 0))]
            + [pl.BlockSpec((layers, rows, width), lambda i, me: (0, me[0], first + i)), block, block]
            + [pl.BlockSpec((g.shape[0], g_rows, g_width), lambda i, me: (0, which, first + i)) for g in (g_top, g_bottom)]
            + [pl.BlockSpec(memory_space=pl.ANY)] * len(fixed),
            out_specs=[pl.BlockSpec(one, lambda i, me: (0, i)) for one in new] + [block, block],
        ),
        out_shape=out,
        input_output_aliases={7 + k: layers + k for k in range(len(fixed))},
        compiler_params=params(),
        cost_estimate=cost(16 * rows * width * blocks * layers, 22 * rows * width * blocks * layers),
        name="adam",
    )(me, squares, w, m, v, g_top, g_bottom, *fixed)
    return outs[:layers], outs[layers:]


def early_kernel(n, chunks, count, squares, *refs):
    wg, wu, (wd, near_a, near_b, far_a, far_b, g_own, g_all), refs = refs[:n], refs[n : 2 * n], refs[2 * n : 2 * n + 7], refs[2 * n + 7 :]
    outs, (across, down, sems) = refs[:3], refs[3:]
    factor = clip(squares[...], count)
    me = lax.axis_index("dp")
    rows = near_a.shape[2]
    held = ((near_a.at[2], near_b.at[2], g_own.at[0]), (near_a.at[1], near_b.at[1], g_all.at[1]))
    held += ((far_a, far_b, g_all.at[2]), (near_a.at[0], near_b.at[0], g_all.at[0]))
    for turn, (a, b, g) in enumerate(held):
        o = lax.rem(me + turn, n)
        at = pl.ds(pl.multiple_of(o * rows, rows), rows)
        for k, w in enumerate((wg, wu)):
            old = jnp.concatenate([one[0, at, :] for one in w], 1)
            grad = g[k * rows : (k + 1) * rows, :].astype(F32) * factor
            across[k, at, :] = adamw(old, a[2 * k], a[2 * k + 1], grad)[0]
        grad = upright(g[2 * rows :, :].astype(F32)) * factor
        down[o] = adamw(wd[0, o, 0], b[0], b[1], grad)[0]
    copies = []
    for o, s in enumerate(stripes(n, chunks, EARLY)):
        for k in range(2):
            copies.append((across.at[k, :, o * STRIPE : (o + 1) * STRIPE], outs[k].at[1, :, s]))
        copies.append((down.at[o], outs[2].at[1, s, :]))
    copies = [pltpu.make_async_copy(src, dst, sems.at[k]) for k, (src, dst) in enumerate(copies)]
    for copy in copies:
        copy.start()
    for copy in copies:
        copy.wait()


def early_step(n, chunks, squares, weights, near_a, near_b, far_a, far_b, g_top, g_all, count):
    w_gate, w_up, w_down = weights
    d = w_gate.shape[1]
    whole = lambda one: pl.BlockSpec(one.shape, lambda i: (0,) * one.ndim)
    across = [pl.BlockSpec((1, d, STRIPE), lambda i, o=o: (1, 0, o * chunks + EARLY)) for o in range(n)]
    down = pl.BlockSpec((1, n, 1, STRIPE, d), lambda i: (1, 0, EARLY, 0, 0))
    own = pl.BlockSpec((1, *g_top.shape[1:]), lambda i: (EARLY, 0, 0))
    arrays = (near_a, near_b, far_a, far_b)
    return pl.pallas_call(
        functools.partial(early_kernel, n, chunks, count),
        grid=(1,),
        in_specs=[whole(squares)] + across + across + [down] + [whole(one) for one in arrays] + [own, whole(g_all)],
        out_specs=[pl.BlockSpec(memory_space=pl.ANY)] * 3,
        out_shape=[jax.ShapeDtypeStruct(w.shape, BF16) for w in weights],
        scratch_shapes=[
            pltpu.VMEM((2, d, n * STRIPE), BF16),
            pltpu.VMEM((n, STRIPE, d), BF16),
            pltpu.SemaphoreType.DMA((3 * n,)),
        ],
        compiler_params=params(),
        cost_estimate=cost(16 * 3 * d * n * STRIPE, nbytes(*arrays)),
        name="early",
    )(squares, *[w_gate] * n, *[w_up] * n, by_owner(n, w_down), *arrays, g_top, g_all)


def place_kernel(n, pieces, regions, *refs):
    arrays, out, sems = refs[: len(pieces)], refs[-2], refs[-1]
    me = lax.axis_index("dp")
    copies = []
    for array, (layer, turn) in zip(arrays, pieces, strict=True):
        o = lax.rem(me + turn, n)
        for from_column, rows_before, columns, region in regions(layer):
            rows = array.shape[0]
            step = rows + rows_before
            to = out.at[layer, pl.ds(pl.multiple_of(o * step + rows_before, 16), rows), region]
            copies.append((array.at[:, from_column : from_column + columns], to))
    copies = [pltpu.make_async_copy(src, dst, sems.at[k]) for k, (src, dst) in enumerate(copies)]
    for copy in copies:
        copy.start()
    for copy in copies:
        copy.wait()


def place(n, chunks, whole, pieces, tall, first, blocks):
    arrays, where = zip(*pieces, strict=True)
    full = STRIPE * chunks

    def regions(layer):
        if tall:
            columns = arrays[0].shape[1]
            return [(0, layer * STRIPE, columns, slice(first * columns // blocks, (first + blocks) * columns // blocks))]
        columns = full - layer * STRIPE
        return [
            (j * columns, 0, columns, slice((first + j) * full + layer * STRIPE, (first + j + 1) * full)) for j in range(blocks)
        ]

    return pl.pallas_call(
        functools.partial(place_kernel, n, where, regions),
        grid=(1,),
        in_specs=[pl.BlockSpec(one.shape, lambda i: (0, 0)) for one in arrays] + [pl.BlockSpec(memory_space=pl.ANY)],
        out_specs=pl.BlockSpec(memory_space=pl.ANY),
        out_shape=jax.ShapeDtypeStruct(whole.shape, whole.dtype),
        input_output_aliases={len(arrays): 0},
        scratch_shapes=[pltpu.SemaphoreType.DMA((len(arrays) * blocks,))],
        compiler_params=params(),
        cost_estimate=cost(arrays[0].size, 4 * nbytes(*arrays)),
        name="place",
    )(*arrays, whole)


def send_around(n, own, swap):
    right, left = [(i, (i + 1) % n) for i in range(n)], [(i, (i - 1) % n) for i in range(n)]

    def send(one, way):
        return lax.ppermute(one, "dp", way)

    def in_order(a, b):
        return (b, a) if swap else (a, b)

    a, b = in_order(*own)
    left_a, right_b = send(a, right), send(b, left)
    left_b, right_a = send(b, right), send(a, left)
    return in_order(left_a, left_b), in_order(right_a, right_b), lambda: in_order(send(left_a, right), send(right_b, left))


def solution(mesh):
    n = mesh.shape["dp"]

    def step(x, dy, w_gate, w_up, w_down, m_gate, m_up, m_down, v_gate, v_up, v_down):
        x, dy = x[0], dy[0]
        chunks = w_gate.shape[2] // (n * STRIPE)
        me = lax.axis_index("dp").astype(jnp.int32).reshape(1)

        weights, moments = (w_gate, w_up, w_down), ((m_gate, v_gate), (m_up, v_up), (m_down, v_down))
        *parts, near_a, near_b = forward(n, chunks, x, dy, *weights, sum(moments, ()))
        gate, up, a0_t, h1, a1, a1_t, dy_t = parts
        *parts, far_a, far_b, g_all = top(n, chunks, 1, a1, a1_t, dy, dy_t, h1, *weights, near_a, near_b)
        dh, dh_t, g_top, last, squares = parts
        g_bottom, squares = bottom(n, chunks, 0, a0_t, dh, dh_t, gate, up, w_down, last, squares)

        new, sent, count = [[], [], []], [], 3 * w_gate.size
        for which, first, blocks, swap in PIECES:
            own, new[which] = adam(
                me, squares, weights[which], *moments[which], g_top, g_bottom, which, count, chunks, which == 2, first, blocks, new[which]
            )
            squares = lax.optimization_barrier((squares, *own))[0]
            sent.append((own, *send_around(n, own, swap)))
        whole = list(early_step(n, chunks, squares, weights, near_a, near_b, far_a, far_b, g_top, g_all, count))
        for k, (which, first, blocks, swap) in enumerate(PIECES):
            own, left, right, _ = sent[k]
            near = [(one, (layer, turn)) for turn, pair in ((0, own), (n - 1, left), (1, right)) for layer, one in enumerate(pair)]
            whole[which] = place(n, chunks, whole[which], near, which == 2, first, blocks)
        for k, (which, first, blocks, swap) in enumerate(PIECES):
            far = [(one, (layer, 2)) for layer, one in enumerate(sent[k][3]())]
            whole[which] = place(n, chunks, whole[which], far, which == 2, first, blocks)
        return (*whole, *(one[0] for one in new), *(one[1] for one in new))

    seq, part, rows = P(("rep", "dp"), None, None), P("rep", None, None), P("rep", "dp", None)
    state = P(None, "dp", None)
    step = jax.shard_map(
        step,
        mesh=mesh,
        in_specs=(seq, seq) + (P(None, None, None),) * 3 + (state,) * 6,
        out_specs=(part,) * 3 + (rows,) * 6,
        check_vma=False,
    )
    return step
```

```python
import functools

import jax
import jax.numpy as jnp
from jax import lax
from jax.experimental import pallas as pl
from jax.experimental.pallas import tpu as pltpu
from jax.sharding import PartitionSpec as P


F32, BF16 = jnp.float32, jnp.bfloat16
STRIPE = 128
VMEM_LIMIT = 60 << 20
EARLY_DOWN = 2
PIECES = ((0, 0, 1, False), (0, 1, 3, False), (2, 0, 2, True), (1, 0, 3, False), (1, 3, 1, False))


def dot(a, b):
    return jnp.dot(a, b, preferred_element_type=F32)


def dot_nt(a, b):
    return lax.dot_general(a, b, (((1,), (1,)), ((), ())), preferred_element_type=F32)


def sigmoid(x):
    return 0.5 * jnp.tanh(0.5 * x) + 0.5


def normed(h):
    wide = h.astype(F32)
    scale = lax.rsqrt(jnp.mean(wide * wide, -1, keepdims=True) + 1e-6)
    return (wide * scale).astype(BF16)


def cost(flops, read_and_written):
    return pl.CostEstimate(flops=int(flops), bytes_accessed=int(read_and_written), transcendentals=0)


def params(**more):
    return pltpu.CompilerParams(vmem_limit_bytes=VMEM_LIMIT, **more)


def nbytes(*arrays):
    return sum(a.size * jnp.dtype(a.dtype).itemsize for a in arrays)


def once(shape, index_map):
    return pl.BlockSpec(shape, index_map, pipeline_mode=pl.Buffered(1))


def stripes(n, chunks, c):
    return [slice((o * chunks + c) * STRIPE, (o * chunks + c + 1) * STRIPE) for o in range(n)]


def forward_kernel(n, chunks, tiles, *refs):
    x_first, x_next, x_before, dy, wg, wu, wd, *refs = refs
    moments, (gate, up, a_t, h1, a1, a1_t, dy_t, near_a, near_b), refs = refs[:6], refs[6:15], refs[15:]
    act, normal, y, pack_a, pack_b, packed, own, send, recv = refs
    m = pl.program_id(0)
    width = n * STRIPE
    right, _, left = neighbours(n)

    def packing():
        for k, ref in enumerate(moments[:4]):
            for o, s in enumerate(stripes(n, chunks, 0)):
                yield pltpu.make_async_copy(
                    ref.at[1, :, s], pack_a.at[k, :, o * STRIPE : (o + 1) * STRIPE], packed.at[k * n + o]
                )
        for k, ref in enumerate(moments[4:]):
            yield pltpu.make_async_copy(ref.at[1, : pack_b.shape[1], :], pack_b.at[k], packed.at[4 * n + k])

    def copies():
        parts = ((pack_a, near_a, ()), (pack_b.at[0], near_b, (0,)), (pack_b.at[1, :STRIPE], near_b, (1, slice(0, STRIPE))))
        for k, (part, near, where) in enumerate(parts):
            yield remote(part, near.at[0, *where], send.at[k], recv.at[k], right)
            yield remote(part, near.at[1, *where], send.at[3 + k], recv.at[3 + k], left)
        for k, (part, near) in enumerate(((pack_a, near_a), (pack_b, near_b))):
            yield pltpu.make_async_copy(part, near.at[2], own.at[k])

    def finish():
        h = (x_before[...].astype(F32) + y[...].astype(F32)).astype(BF16)
        h1[...] = h
        out = normed(h)
        a1[...] = out
        a1_t[...] = out.T

    @pl.when(m == 0)
    def _():
        for copy in packing():
            copy.start()
        hail((right, left))
        normal[0] = normed(x_first[...])

    @pl.when(m == 1)
    def _():
        pl.semaphore_wait(pltpu.get_barrier_semaphore(), 2)
        for copy in packing():
            copy.wait()
        for copy in copies():
            copy.start()

    @pl.when(m < tiles)
    def _():
        a = normal[lax.rem(m, 2)]

        def dots(c):
            for o, w in ((gate, wg), (up, wu)):
                o[c] = dot(a, jnp.concatenate([w[0, :, s] for s in stripes(n, chunks, c)], 1))

        dots(0)
        for c in range(chunks):
            if c + 1 < chunks:
                dots(c + 1)
            g = gate[c]
            act[:, c * width : (c + 1) * width] = (g * sigmoid(g) * up[c]).astype(BF16)
        a_t[...] = a.T
        dy_t[...] = dy[...].T
        finish()
        down = jnp.concatenate([wd[0, s, :] for c in range(chunks) for s in stripes(n, chunks, c)], 0)
        y[...] = dot(act[...], down).astype(BF16)
        normal[lax.rem(m + 1, 2)] = normed(x_next[...])

    @pl.when(m == tiles)
    def _():
        finish()
        for copy in copies():
            copy.wait()


def forward(n, chunks, x, dy, w_gate, w_up, w_down, moments, tm=256):
    t, d = x.shape
    ff, tiles, width = w_gate.shape[2], t // tm, n * STRIPE
    here, before = lambda m: jnp.minimum(m, tiles - 1), lambda m: jnp.maximum(m - 1, 0)
    row = lambda at: pl.BlockSpec((tm, d), lambda m: (at(m), 0))
    col = lambda at: pl.BlockSpec((d, tm), lambda m: (0, at(m)))
    wide = pl.BlockSpec((chunks, tm, width), lambda m: (0, here(m), 0))
    pack_a, pack_b = (4, d // n, width), (2, EARLY_DOWN * STRIPE, d)
    out = [jax.ShapeDtypeStruct((chunks, t, width), F32)] * 2
    out += [jax.ShapeDtypeStruct(s, BF16) for s in ((d, t), (t, d), (t, d), (d, t), (d, t))]
    out += [jax.ShapeDtypeStruct((3, *s), F32) for s in (pack_a, pack_b)]
    whole = pl.BlockSpec(memory_space=pl.ANY)
    return pl.pallas_call(
        functools.partial(forward_kernel, n, chunks, tiles),
        grid=(tiles + 1,),
        in_specs=[once((tm, d), lambda m: (0, 0)), row(lambda m: jnp.minimum(m + 1, tiles - 1)), row(before), row(here)]
        + [once((1, d, ff), lambda m: (0, 0, 0))] * 2
        + [once((1, ff, d), lambda m: (0, 0, 0))]
        + [whole] * 6,
        out_specs=[wide] * 2 + [col(here), row(before), row(before), col(before), col(here), whole, whole],
        out_shape=out,
        scratch_shapes=[
            pltpu.VMEM((tm, ff), BF16),
            pltpu.VMEM((2, tm, d), BF16),
            pltpu.VMEM((tm, d), BF16),
            pltpu.VMEM(pack_a, F32),
            pltpu.VMEM(pack_b, F32),
            pltpu.SemaphoreType.DMA((4 * n + 2,)),
            pltpu.SemaphoreType.DMA((2,)),
            pltpu.SemaphoreType.DMA((6,)),
            pltpu.SemaphoreType.DMA((6,)),
        ],
        compiler_params=params(collective_id=2, has_side_effects=True),
        cost_estimate=cost(6 * t * d * ff, nbytes(*out)),
        name="forward",
    )(x, x, x, dy, w_gate, w_up, w_down, *moments)


def neighbours(n):
    me = lax.axis_index("dp")
    return lax.rem(me + 1, n), lax.rem(me + 2, n), lax.rem(me + n - 1, n)


def hail(devices):
    barrier = pltpu.get_barrier_semaphore()
    for device in devices:
        pl.semaphore_signal(barrier, inc=1, device_id={"dp": device}, device_id_type=pl.DeviceIdType.MESH)


def greet(devices):
    hail(devices)
    pl.semaphore_wait(pltpu.get_barrier_semaphore(), len(devices))


def remote(src, dst, send, recv, device):
    return pltpu.make_async_remote_copy(
        src_ref=src, dst_ref=dst, send_sem=send, recv_sem=recv, device_id={"dp": device}, device_id_type=pl.DeviceIdType.MESH
    )


class Ring:
    def __init__(self, n, raw, got, mid, send, recv):
        half = raw.shape[1] // 2
        self.a, self.b = pl.ds(0, half), pl.ds(half, half)
        self.raw, self.got, self.mid = raw, got, mid
        self.send, self.recv = send, recv
        self.right, _, self.left = neighbours(n)

    def copy(self, k):
        source = (
            lambda: self.raw.at[2, self.a],
            lambda: self.raw.at[1, self.b],
            lambda: self.mid.at[0],
            lambda: self.raw.at[2, self.b],
            lambda: self.raw.at[3, self.a],
            lambda: self.mid.at[1],
        )[k]()
        return remote(source, self.got.at[k], self.send.at[k], self.recv.at[k], self.right if k < 3 else self.left)

    def begin(self, which=(0, 3, 1, 4)):
        for k in which:
            self.copy(k).start()

    def go_on(self):
        for k, owner, half in ((0, 1, self.a), (3, 3, self.b)):
            self.copy(k).wait_recv()
            self.mid[k // 3] = (self.raw[owner, half].astype(F32) + self.got[k].astype(F32)).astype(BF16)
            self.copy(k + 2).start()

    def end(self, out, squares):
        for plain, summed, half in ((4, 2, self.a), (1, 5, self.b)):
            self.copy(plain).wait_recv()
            self.copy(summed).wait_recv()
            total = self.raw[0, half].astype(F32) + self.got[plain].astype(F32) + self.got[summed].astype(F32)
            total = total.astype(BF16)
            out[0, half] = total
            total = total.astype(F32)
            squares[...] += jnp.sum((total * total).reshape(-1, 8, total.shape[1]), 0)

    def sent(self, *which):
        for k in which:
            self.copy(k).wait_send()


def lay_out(n, raw, gacc, uacc, dacc):
    me = lax.axis_index("dp")
    rows = gacc.shape[0] // n

    @pl.loop(0, n)
    def _(o):
        turn = lax.rem(o - me + n, n)
        mine, stripe = pl.ds(pl.multiple_of(o * rows, rows), rows), pl.ds(pl.multiple_of(o * STRIPE, STRIPE), STRIPE)
        raw[turn, :rows] = gacc[mine].astype(BF16)
        raw[turn, rows : 2 * rows] = uacc[mine].astype(BF16)
        for q in range(n):
            raw[turn, 2 * rows :, q * STRIPE : (q + 1) * STRIPE] = dacc[q * rows : (q + 1) * rows, stripe].astype(BF16)


def backward_parts(g, u, dact):
    dact = dact.astype(BF16).astype(F32)
    s = sigmoid(g)
    silu = g * s
    act = (silu * u).astype(BF16)
    du = (dact * silu).astype(BF16)
    dg = (dact * u * (s + silu * (1 - s))).astype(BF16)
    return act, dg, du


def states_gradient(da, h, dy):
    da = da.astype(BF16).astype(F32)
    wide = h.astype(F32)
    mean = jnp.mean(wide * wide, -1, keepdims=True) + 1e-6
    scale = lax.rsqrt(mean)
    dmean = jnp.sum(da * wide, -1, keepdims=True) * (-0.5 * scale / mean)
    back = (da * scale + wide * (dmean * (2.0 / wide.shape[1]))).astype(BF16)
    return (dy.astype(F32) + back.astype(F32)).astype(BF16)


def fetch(chunks, layer, whole, part, sems, c):
    n = sems.shape[0]
    for o in range(n):
        at = pl.ds(pl.multiple_of((o * chunks + c) * STRIPE, STRIPE), STRIPE)
        yield pltpu.make_async_copy(whole.at[layer, :, at], part.at[:, o * STRIPE : (o + 1) * STRIPE], sems.at[o])


def top_kernel(n, chunks, tiles, layer, *refs):
    wholes, (h, wd, wg, wu, near_a, near_b), refs = refs[:4], refs[4:10], refs[10:]
    dh, dh_t, g_out, last, squares_out, far_a, far_b, late, *refs = refs
    alls, refs = refs[:2], refs[2:]
    gacc, uacc, dacc, da, raw, got, mid, squares, send, recv, local, wg_part, wu_part, w_sems, *mines, e_send, e_recv = refs[:-5]
    slots, loaded = refs[-5:-1], refs[-1]
    c, i = pl.program_id(0), pl.program_id(1)
    tm = h.shape[0]
    right, _, left = neighbours(n)
    before = jnp.maximum(c - 1, 0)
    slot, here, there = lax.rem(before, 2), lax.rem(c, 2), lax.rem(c + 1, 2)
    ring = Ring(n, raw, got.at[slot], mid, send.at[slot], recv.at[slot])

    def moments():
        half, rows = far_a.shape[0] // 2, 3 * STRIPE // 2
        parts = (
            (near_a, far_a, (slice(0, half),), 0),
            (near_b, far_b, (0, slice(0, rows)), 0),
            (near_a, far_a, (slice(half, None),), 1),
            (near_b, far_b, (0, slice(rows, None)), 1),
            (near_b, far_b, (1, slice(0, STRIPE)), 1),
        )
        for k, (near, far, where, side) in enumerate(parts):
            yield remote(near.at[side, *where], far.at[*where], e_send.at[8, k], e_recv.at[8, k], (right, left)[side])

    block = mines[0].shape[0]
    across = 2 * block // 3
    rounds = (
        (near_b.at[2, 1, STRIPE:], late, 0, STRIPE, 1),
        (mines[0].at[across:], alls[0], across, block - across, 2),
        (mines[0].at[:across], alls[0], 0, across, 3),
        (mines[1], alls[1], 0, block - across, 4),
    )

    def out(k):
        mine, every, start, rows, _ = rounds[k]
        for side in range(2):
            to = every.at[side, pl.ds(start, rows)]
            yield remote(mine, to, e_send.at[2 * k, side], e_recv.at[2 * k, side], (right, left)[side])

    def on(k):
        _, every, start, rows, _ = rounds[k]
        half, at = rows // 2, 2 * k + 1
        for side in range(2):
            part = pl.ds(start + side * half, half)
            yield remote(every.at[side, part], every.at[2, part], e_send.at[at, side], e_recv.at[at, side], (right, left)[side])

    def weights(c, slot):
        yield from fetch(chunks, layer, wg, wg_part.at[slot], w_sems.at[slot, 0], c)
        yield from fetch(chunks, layer, wu, wu_part.at[slot], w_sems.at[slot, 1], c)

    def loads(i):
        at, slot = pl.ds(pl.multiple_of(i * tm, tm), tm), lax.rem(i, 2)
        for k, (whole, part) in enumerate(zip(wholes, slots, strict=True)):
            source = whole.at[:, at] if k % 2 else whole.at[at]
            yield pltpu.make_async_copy(source, part.at[slot], loaded.at[k, slot])

    @pl.when(i == 0)
    def _():
        @pl.when(c == 0)
        def _():
            for copy in (*weights(c, here), *loads(i)):
                copy.start()
            greet((right, left))
            for copy in moments():
                copy.start()
            squares[...] = jnp.zeros_like(squares)

        @pl.when(c > 0)
        def _():
            ring.begin((0, 3))

        for copy in weights(c, here):
            copy.wait()

        @pl.when(c < chunks - 1)
        def _():
            for copy in weights(c + 1, there):
                copy.start()

    @pl.when((c < chunks - 1) | (i < tiles - 1))
    def _():
        for load in loads(lax.rem(i + 1, tiles)):
            load.start()

    for load in loads(i):
        load.wait()
    a, a_t, dy, dy_t = (part.at[lax.rem(i, 2)] for part in slots)
    rows = pl.ds(pl.multiple_of(i * tm, tm), tm)
    pair = 2

    def work(at_end):
        parts = []
        for j in range(0, n, pair):
            to = slice(j * STRIPE, (j + pair) * STRIPE)
            w1, w2 = wg_part[here, :, to], wu_part[here, :, to]
            w3 = wd[0, j : j + pair, 0].reshape(pair * STRIPE, wd.shape[4])
            parts.append((to, w1, w2, dot(a[...], w1), dot(a[...], w2), dot_nt(dy[...], w3)))

        def states(fresh, dg, du, w1, w2):
            more = dot_nt(jnp.concatenate([dg, du], 1), jnp.concatenate([w1, w2], 1))
            da[rows, :] = jnp.where(fresh, 0.0, da[rows, :]) + more

        def weight_gradients(to, act, dg, du):
            for acc, left, right in ((gacc, a_t, dg), (uacc, a_t, du), (dacc, dy_t, act)):
                acc[:, to] = jnp.where(i == 0, 0.0, acc[:, to]) + dot(left[...], right)

        later = []
        for k, (to, w1, w2, g, u, dact) in enumerate(parts):
            fresh = (c == 0) & (k == 0)
            act, dg, du = backward_parts(g, u, dact)
            if at_end:
                states(fresh, dg, du, w1, w2)
                later.append((to, act, dg, du))
            else:
                weight_gradients(to, act, dg, du)
                states(fresh, dg, du, w1, w2)
        for one in later:
            weight_gradients(*one)
        if at_end:
            out = states_gradient(da[rows, :], h[...], dy[...])
            dh[...] = out
            dh_t[...] = out.T

    pl.when(c < chunks - 1)(lambda: work(False))
    pl.when(c == chunks - 1)(lambda: work(True))
    pl.when((c > 0) & (i == 0))(lambda: ring.begin((1, 4)))

    @pl.when((c > 0) & (i == tiles // 2 - 1))
    def _():
        ring.go_on()

    @pl.when(i == tiles // 2)
    def _():
        for k, (*_, first) in enumerate(rounds):

            @pl.when(c == first)
            def _(k=k):
                for copy in out(k):
                    copy.start()

            @pl.when(c == first + 1)
            def _(k=k):
                for copy in out(k):
                    copy.wait()
                for copy in on(k):
                    copy.start()

            if first + 2 < chunks:

                @pl.when(c == first + 2)
                def _(k=k):
                    for copy in on(k):
                        copy.wait()

    @pl.when((c == chunks - 1) & (i == tiles - 1))
    def _():
        for copy in moments():
            copy.wait()
        for k, (*_, first) in enumerate(rounds):
            if first + 2 >= chunks:
                for copy in on(k):
                    copy.wait()

    @pl.when(i == tiles - 1)
    def _():
        @pl.when(c > 0)
        def _():
            ring.end(g_out, squares)
            ring.sent(*range(6))

        for k, mine in enumerate(mines):

            @pl.when(c == k + 1)
            def _(mine=mine):
                mine[...] = g_out[0, g_out.shape[1] - mine.shape[0] :]

        lay_out(n, raw, gacc, uacc, dacc)

        @pl.when(c == chunks - 1)
        def _():
            copy = pltpu.make_async_copy(raw, last, local)
            copy.start()
            squares_out[...] = squares[...]
            copy.wait()


def by_owner(n, w_down):
    layers, ff, d = w_down.shape
    return w_down.reshape(layers, n, ff // (n * STRIPE), STRIPE, d)


def top(n, chunks, layer, a, a_t, dy, dy_t, h, w_gate, w_up, w_down, near_a, near_b, tm=1024):
    t, d = a.shape
    width, tiles, block = n * STRIPE, t // tm, 3 * d // n
    assert tiles % 2 == 0
    at_end = lambda c, i: jnp.where(c == chunks - 1, i, 0)
    row_end, col_end = pl.BlockSpec((tm, d), lambda c, i: (at_end(c, i), 0)), pl.BlockSpec((d, tm), lambda c, i: (0, at_end(c, i)))
    down = pl.BlockSpec((1, n, 1, STRIPE, d), lambda c, i: (layer, 0, c, 0, 0))
    shapes = [
        jax.ShapeDtypeStruct((t, d), BF16),
        jax.ShapeDtypeStruct((d, t), BF16),
        jax.ShapeDtypeStruct((chunks - 1, block, width), BF16),
        jax.ShapeDtypeStruct((n, block, width), BF16),
        jax.ShapeDtypeStruct((8, width), F32),
        jax.ShapeDtypeStruct(near_a.shape[1:], F32),
        jax.ShapeDtypeStruct(near_b.shape[1:], F32),
        jax.ShapeDtypeStruct((3, STRIPE, d), F32),
        jax.ShapeDtypeStruct((3, block, width), BF16),
        jax.ShapeDtypeStruct((3, block // 3, width), BF16),
    ]
    return pl.pallas_call(
        functools.partial(top_kernel, n, chunks, tiles, layer),
        grid=(chunks, tiles),
        in_specs=[pl.BlockSpec(memory_space=pl.ANY)] * 4 + [row_end, down] + [pl.BlockSpec(memory_space=pl.ANY)] * 4,
        out_specs=[
            row_end,
            col_end,
            pl.BlockSpec((1, block, width), lambda c, i: (jnp.maximum(c - 1, 0), 0, 0)),
            pl.BlockSpec(memory_space=pl.ANY),
            pl.BlockSpec((8, width), lambda c, i: (0, 0)),
        ]
        + [pl.BlockSpec(memory_space=pl.ANY)] * 5,
        out_shape=shapes,
        scratch_shapes=[pltpu.VMEM((d, width), F32)] * 3
        + [
            pltpu.VMEM((t, d), F32),
            pltpu.VMEM((n, block, width), BF16),
            pltpu.VMEM((2, 6, block // 2, width), BF16),
            pltpu.VMEM((2, block // 2, width), BF16),
            pltpu.VMEM((8, width), F32),
            pltpu.SemaphoreType.DMA((2, 6)),
            pltpu.SemaphoreType.DMA((2, 6)),
            pltpu.SemaphoreType.DMA,
            pltpu.VMEM((2, d, width), BF16),
            pltpu.VMEM((2, d, width), BF16),
            pltpu.SemaphoreType.DMA((2, 2, n)),
            pltpu.VMEM((block, width), BF16),
            pltpu.VMEM((block // 3, width), BF16),
            pltpu.SemaphoreType.DMA((9, 5)),
            pltpu.SemaphoreType.DMA((9, 5)),
        ]
        + [pltpu.VMEM((2, *one), BF16) for one in ((tm, d), (d, tm)) * 2]
        + [pltpu.SemaphoreType.DMA((4, 2))],
        compiler_params=pltpu.CompilerParams(vmem_limit_bytes=67043328, collective_id=0, has_side_effects=True),
        cost_estimate=cost(16 * t * d * width * chunks, chunks * nbytes(a, a_t, dy, dy_t)),
        name="top",
    )(a, a_t, dy, dy_t, h, by_owner(n, w_down), w_gate, w_up, near_a, near_b)


def bottom_kernel(n, chunks, tiles, *refs):
    wholes, (wd, first, squares_in, g_out, squares_out), refs = refs[:5], refs[5:10], refs[10:]
    gacc, uacc, dacc, raw, got, mid, squares, send, recv, local, all_squares, to, fro, *slots, loaded = refs
    c, i = pl.program_id(0), pl.program_id(1)
    right, opposite, left = neighbours(n)
    tm = slots[0].shape[2]

    def loads(c, i):
        at, slot = pl.ds(pl.multiple_of(i * tm, tm), tm), lax.rem(i, 2)
        tiles_at = ((slice(None), at), (at,), (slice(None), at), (c, at), (c, at))
        for k, (whole, where, part) in enumerate(zip(wholes, tiles_at, slots, strict=True)):
            yield pltpu.make_async_copy(whole.at[*where], part.at[slot], loaded.at[k, slot])

    def ring(k):
        slot = lax.rem(k, 2)
        return Ring(n, raw.at[slot], got.at[k], mid.at[slot], send.at[k], recv.at[k])

    held = pltpu.make_async_copy(first, raw.at[0], local)

    @pl.when((c == 0) & (i == 0))
    def _():
        hail((right, opposite, left))
        held.start()
        for load in loads(c, i):
            load.start()
        squares[...] = squares_in[...]
        pl.semaphore_wait(pltpu.get_barrier_semaphore(), 3)
        Ring(n, first, got.at[0], mid.at[0], send.at[0], recv.at[0]).begin((0, 3))

    @pl.when((c > 0) & (i == 0))
    def _():
        ring(c).begin((0, 3))

    @pl.when((c < chunks - 1) | ((c == chunks - 1) & (i < tiles - 1)))
    def _():
        for load in loads(jnp.where(i == tiles - 1, c + 1, c), lax.rem(i + 1, tiles)):
            load.start()

    @pl.when(c < chunks)
    def _():
        for load in loads(c, i):
            load.wait()
        a_t, dy, dy_t, gate, up = (part.at[lax.rem(i, 2)] for part in slots)
        pair = 2
        parts = []
        for j in range(0, n, pair):
            w = wd[0, j : j + pair, 0].reshape(pair * STRIPE, wd.shape[4])
            parts.append((slice(j * STRIPE, (j + pair) * STRIPE), dot_nt(dy[...], w)))
        for to, dact in parts:
            act, dg, du = backward_parts(gate[:, to], up[:, to], dact)
            for acc, left, right in ((gacc, a_t, dg), (uacc, a_t, du), (dacc, dy_t, act)):
                acc[:, to] = jnp.where(i == 0, 0.0, acc[:, to]) + dot(left[...], right)

    @pl.when(i == tiles // 4)
    def _():
        @pl.when(c > 0)
        def _():
            before = ring(c - 1)
            before.end(g_out, squares)
            before.sent(*range(6))

        pl.when(c == 0)(held.wait)
        ring(c).begin((1, 4))

    pl.when(i == tiles // 2)(lambda: ring(c).go_on())

    @pl.when((c < chunks) & (i == tiles - 1))
    def _():
        lay_out(n, raw.at[lax.rem(c + 1, 2)], gacc, uacc, dacc)

    @pl.when((c == chunks) & (i == tiles - 1))
    def _():
        final = ring(c)
        final.end(g_out, squares)
        final.sent(*range(6))
        me = lax.axis_index("dp")
        all_squares[me] = squares[...]
        copies = [
            remote(squares, all_squares.at[me], to.at[k], fro.at[k], device) for k, device in enumerate((right, opposite, left))
        ]
        for copy in copies:
            copy.start()
        for copy in copies:
            copy.wait()
        total = all_squares[0]
        for k in range(1, n):
            total += all_squares[k]
        squares_out[...] = total


def bottom(n, chunks, layer, a_t, dy, dy_t, gate, up, w_down, first, squares, tm=1024):
    d, t = a_t.shape
    width, tiles, block = n * STRIPE, t // tm, 3 * d // n
    assert tiles % 2 == 0
    small = pl.BlockSpec((8, width), lambda c, i: (0, 0))
    down = pl.BlockSpec((1, n, 1, STRIPE, d), lambda c, i: (layer, 0, jnp.minimum(c, chunks - 1), 0, 0))
    done = lambda c, i: jnp.where((c == chunks) & (i == tiles - 1), chunks, jnp.maximum(c - 1, 0))
    return pl.pallas_call(
        functools.partial(bottom_kernel, n, chunks, tiles),
        grid=(chunks + 1, tiles),
        in_specs=[pl.BlockSpec(memory_space=pl.ANY)] * 5 + [down, pl.BlockSpec(memory_space=pl.ANY), small],
        out_specs=[pl.BlockSpec((1, block, width), lambda c, i: (done(c, i), 0, 0)), small],
        out_shape=[
            jax.ShapeDtypeStruct((chunks + 1, block, width), BF16),
            jax.ShapeDtypeStruct((8, width), F32),
        ],
        scratch_shapes=[pltpu.VMEM((d, width), F32)] * 3
        + [
            pltpu.VMEM((2, n, block, width), BF16),
            pltpu.VMEM((chunks + 1, 6, block // 2, width), BF16),
            pltpu.VMEM((2, 2, block // 2, width), BF16),
            pltpu.VMEM((8, width), F32),
            pltpu.SemaphoreType.DMA((chunks + 1, 6)),
            pltpu.SemaphoreType.DMA((chunks + 1, 6)),
            pltpu.SemaphoreType.DMA,
            pltpu.VMEM((n, 8, width), F32),
            pltpu.SemaphoreType.DMA((3,)),
            pltpu.SemaphoreType.DMA((3,)),
        ]
        + [pltpu.VMEM((2, *one), BF16) for one in ((d, tm), (tm, d), (d, tm))]
        + [pltpu.VMEM((2, tm, width), F32)] * 2
        + [pltpu.SemaphoreType.DMA((5, 2))],
        compiler_params=pltpu.CompilerParams(vmem_limit_bytes=VMEM_LIMIT, collective_id=1, has_side_effects=True),
        cost_estimate=cost(8 * t * d * width * chunks, nbytes(gate, up) + chunks * nbytes(a_t, dy, dy_t)),
        name="bottom",
    )(a_t, dy, dy_t, gate, up, by_owner(n, w_down), first, squares)


def clip(squares, count):
    return jnp.minimum(1.0, 0.5 * lax.rsqrt(jnp.full((1, 1), jnp.sum(squares)) / count + 1e-30))


def adamw(w, m, v, g):
    m = 0.9 * m + 0.1 * g
    v = 0.95 * v + 0.05 * g * g
    old = w.astype(F32)
    step = m * lax.rsqrt(v + 1e-8) + 0.1 * old
    return (old - 0.02 * step).astype(BF16), m, v


def upright(g):
    return jnp.concatenate([g[:, q : q + STRIPE].T for q in range(0, g.shape[1], STRIPE)], 1)


def adam_kernel(chunks, tall, count, squares, w, m, v, g_top, g_bottom, *refs):
    *w_out, m_out, v_out = refs
    factor = clip(squares[...], count)

    def work(layer, c, g, to):
        def at(c):
            rows = pl.ds(pl.multiple_of(c * STRIPE, STRIPE), STRIPE)
            return (rows, slice(None)) if tall else (slice(None), rows)

        g = upright(g.astype(F32)) if tall else g.astype(F32)
        new, m_new, v_new = adamw(w[layer, *at(c)], m[layer, *at(c)], v[layer, *at(c)], g * factor)
        if to is not None:
            w_out[layer][at(to)] = new
        m_out[layer, *at(c)] = m_new
        v_out[layer, *at(c)] = v_new

    early = EARLY_DOWN if tall else 1

    @pl.loop(0, early)
    def _(c):
        work(0, c, g_bottom[c + 1], c)
        work(1, c, g_top[c], None)

    @pl.loop(early, chunks - 1)
    def _(c):
        work(0, c, g_bottom[c + 1], c)
        work(1, c, g_top[c], c - early)

    work(0, chunks - 1, g_bottom[chunks], chunks - 1)
    work(1, chunks - 1, g_bottom[0], chunks - 1 - early)


def adam(me, squares, w, m, v, g_top, g_bottom, which, count, chunks, tall, first, blocks, begun):
    layers, rows, _ = m.shape
    g_rows = g_top.shape[1] // 3
    g_width, width = (2 * STRIPE, 2 * g_rows) if tall else (STRIPE, STRIPE * chunks)
    block = pl.BlockSpec((layers, rows, width), lambda i, me: (0, 0, first + i))
    new = [(rows, width), (rows - EARLY_DOWN * STRIPE, width) if tall else (rows, width - STRIPE)]
    out = [jax.ShapeDtypeStruct((r, c * blocks), BF16) for r, c in new] + [jax.ShapeDtypeStruct(m.shape, F32)] * 2
    fixed = list(begun)

    def body(me_ref, *refs):
        adam_kernel(chunks, tall, count, *refs[:6], *refs[6 + len(fixed) :])

    outs = pl.pallas_call(
        body,
        grid_spec=pltpu.PrefetchScalarGridSpec(
            num_scalar_prefetch=1,
            grid=(blocks,),
            in_specs=[pl.BlockSpec(squares.shape, lambda i, me: (0, 0))]
            + [pl.BlockSpec((layers, rows, width), lambda i, me: (0, me[0], first + i)), block, block]
            + [pl.BlockSpec((g.shape[0], g_rows, g_width), lambda i, me: (0, which, first + i)) for g in (g_top, g_bottom)]
            + [pl.BlockSpec(memory_space=pl.ANY)] * len(fixed),
            out_specs=[pl.BlockSpec(one, lambda i, me: (0, i)) for one in new] + [block, block],
        ),
        out_shape=out,
        input_output_aliases={7 + k: layers + k for k in range(len(fixed))},
        compiler_params=params(),
        cost_estimate=cost(16 * rows * width * blocks * layers, 22 * rows * width * blocks * layers),
        name="adam",
    )(me, squares, w, m, v, g_top, g_bottom, *fixed)
    return outs[:layers], outs[layers:]


def early_kernel(n, chunks, count, squares, *refs):
    wg, wu, refs = refs[:n], refs[n : 2 * n], refs[2 * n :]
    (wd, near_a, near_b, far_a, far_b, late, g_top, g_all, g_all_down), refs = refs[:9], refs[9:]
    outs, (a, b, g, g_down, loaded, across, down, sems) = refs[:3], refs[3:]
    rows = g_down.shape[1]
    g_near, g_near_down = g_top.at[0], g_top.at[1, 2 * rows :, :]
    loads = []
    of_chunk = [pl.ds(k * STRIPE, STRIPE) for k in range(EARLY_DOWN)]
    parts = [(a.at[turn], b.at[turn, 0], b.at[turn, 1, of_chunk[0]], b.at[turn, 1, of_chunk[1]], g.at[turn], g_down.at[turn]) for turn in range(n)]

    def held(near_a, near_b, late, *sums):
        return near_a, near_b.at[0], near_b.at[1, of_chunk[0]], late, *sums

    sources = (
        held(near_a.at[2], near_b.at[2], near_b.at[2, 1, of_chunk[1]], g_near, g_near_down),
        held(near_a.at[1], near_b.at[1], late.at[1], g_all.at[1], g_all_down.at[1]),
        held(far_a, far_b, late.at[2], g_all.at[2], g_all_down.at[2]),
        held(near_a.at[0], near_b.at[0], late.at[0], g_all.at[0], g_all_down.at[0]),
    )
    for source, part in zip(sources, parts, strict=True):
        loads += zip(source, part, strict=True)
    loads = [pltpu.make_async_copy(src, dst, loaded.at[k]) for k, (src, dst) in enumerate(loads)]
    for copy in loads:
        copy.start()
    factor = clip(squares[...], count)
    me = lax.axis_index("dp")
    for copy in loads:
        copy.wait()

    @pl.loop(0, n)
    def _(turn):
        o = lax.rem(me + turn, n)
        at = pl.ds(pl.multiple_of(o * rows, rows), rows)
        for k, w in enumerate((wg, wu)):
            old = jnp.concatenate([one[0, at, :] for one in w], 1)
            grad = g[turn, k * rows : (k + 1) * rows, :].astype(F32) * factor
            across[k, at, :] = adamw(old, a[turn, 2 * k], a[turn, 2 * k + 1], grad)[0]
        for k, part in enumerate((g[turn, 2 * rows :, :], g_down[turn])):
            grad = upright(part.astype(F32)) * factor
            down[o, of_chunk[k], :] = adamw(wd[0, o, k], b[turn, 0, of_chunk[k], :], b[turn, 1, of_chunk[k], :], grad)[0]

    copies = []
    for o, s in enumerate(stripes(n, chunks, 0)):
        for k in range(2):
            copies.append((across.at[k, :, o * STRIPE : (o + 1) * STRIPE], outs[k].at[1, :, s]))
        copies.append((down.at[o], outs[2].at[1, s.start : s.start + down.shape[1], :]))
    copies = [pltpu.make_async_copy(src, dst, sems.at[k]) for k, (src, dst) in enumerate(copies)]
    for copy in copies:
        copy.start()
    for copy in copies:
        copy.wait()


def early_step(n, chunks, squares, weights, near_a, near_b, far_a, far_b, late, g_top, g_all, g_all_down, count):
    w_gate, w_up, w_down = weights
    d = w_gate.shape[1]
    whole = lambda one: pl.BlockSpec(one.shape, lambda i: (0,) * one.ndim)
    across = [pl.BlockSpec((1, d, STRIPE), lambda i, o=o: (1, 0, o * chunks)) for o in range(n)]
    down = pl.BlockSpec((1, n, EARLY_DOWN, STRIPE, d), lambda i: (1, 0, 0, 0, 0))
    arrays = (near_a, near_b, far_a, far_b, late, g_top, g_all, g_all_down)
    return pl.pallas_call(
        functools.partial(early_kernel, n, chunks, count),
        grid=(1,),
        in_specs=[whole(squares)] + across + across + [down] + [pl.BlockSpec(memory_space=pl.ANY)] * len(arrays),
        out_specs=[pl.BlockSpec(memory_space=pl.ANY)] * 3,
        out_shape=[jax.ShapeDtypeStruct(w.shape, BF16) for w in weights],
        scratch_shapes=[
            pltpu.VMEM((n, *far_a.shape), F32),
            pltpu.VMEM((n, *far_b.shape), F32),
            pltpu.VMEM((n, *g_all.shape[1:]), BF16),
            pltpu.VMEM((n, *g_all_down.shape[1:]), BF16),
            pltpu.SemaphoreType.DMA((6 * n,)),
            pltpu.VMEM((2, d, n * STRIPE), BF16),
            pltpu.VMEM((n, EARLY_DOWN * STRIPE, d), BF16),
            pltpu.SemaphoreType.DMA((3 * n,)),
        ],
        compiler_params=params(),
        cost_estimate=cost(16 * 3 * d * n * STRIPE, nbytes(*arrays)),
        name="early",
    )(squares, *[w_gate] * n, *[w_up] * n, by_owner(n, w_down), *arrays)


def place_kernel(n, pieces, regions, *refs):
    arrays, out, sems = refs[: len(pieces)], refs[-2], refs[-1]
    me = lax.axis_index("dp")
    copies = []
    for array, (layer, turn) in zip(arrays, pieces, strict=True):
        o = lax.rem(me + turn, n)
        for from_column, rows_before, columns, region in regions(layer):
            rows = array.shape[0]
            step = rows + rows_before
            to = out.at[layer, pl.ds(pl.multiple_of(o * step + rows_before, 16), rows), region]
            copies.append((array.at[:, from_column : from_column + columns], to))
    copies = [pltpu.make_async_copy(src, dst, sems.at[k]) for k, (src, dst) in enumerate(copies)]
    for copy in copies:
        copy.start()
    for copy in copies:
        copy.wait()


def place(n, chunks, whole, pieces, tall, first, blocks):
    arrays, where = zip(*pieces, strict=True)
    full = STRIPE * chunks

    def regions(layer):
        if tall:
            columns = arrays[0].shape[1]
            return [(0, layer * EARLY_DOWN * STRIPE, columns, slice(first * columns // blocks, (first + blocks) * columns // blocks))]
        columns = full - layer * STRIPE
        return [
            (j * columns, 0, columns, slice((first + j) * full + layer * STRIPE, (first + j + 1) * full)) for j in range(blocks)
        ]

    return pl.pallas_call(
        functools.partial(place_kernel, n, where, regions),
        grid=(1,),
        in_specs=[pl.BlockSpec(one.shape, lambda i: (0, 0)) for one in arrays] + [pl.BlockSpec(memory_space=pl.ANY)],
        out_specs=pl.BlockSpec(memory_space=pl.ANY),
        out_shape=jax.ShapeDtypeStruct(whole.shape, whole.dtype),
        input_output_aliases={len(arrays): 0},
        scratch_shapes=[pltpu.SemaphoreType.DMA((len(arrays) * blocks,))],
        compiler_params=params(),
        cost_estimate=cost(arrays[0].size, 4 * nbytes(*arrays)),
        name="place",
    )(*arrays, whole)


def send_around(n, own, swap):
    right, left = [(i, (i + 1) % n) for i in range(n)], [(i, (i - 1) % n) for i in range(n)]

    def send(one, way):
        return lax.ppermute(one, "dp", way)

    def in_order(a, b):
        return (b, a) if swap else (a, b)

    a, b = in_order(*own)
    left_a, right_b = send(a, right), send(b, left)
    left_b, right_a = send(b, right), send(a, left)
    return in_order(left_a, left_b), in_order(right_a, right_b), lambda: in_order(send(left_a, right), send(right_b, left))


def solution(mesh):
    n = mesh.shape["dp"]

    def step(x, dy, w_gate, w_up, w_down, m_gate, m_up, m_down, v_gate, v_up, v_down):
        x, dy = x[0], dy[0]
        chunks = w_gate.shape[2] // (n * STRIPE)
        me = lax.axis_index("dp").astype(jnp.int32).reshape(1)

        weights, moments = (w_gate, w_up, w_down), ((m_gate, v_gate), (m_up, v_up), (m_down, v_down))
        *parts, near_a, near_b = forward(n, chunks, x, dy, *weights, sum(moments, ()))
        gate, up, a0_t, h1, a1, a1_t, dy_t = parts
        *parts, far_a, far_b, late, g_all, g_all_down = top(n, chunks, 1, a1, a1_t, dy, dy_t, h1, *weights, near_a, near_b)
        dh, dh_t, g_top, last, squares = parts
        g_bottom, squares = bottom(n, chunks, 0, a0_t, dh, dh_t, gate, up, w_down, last, squares)

        new, sent, count = [[], [], []], [], 3 * w_gate.size
        for which, first, blocks, swap in PIECES:
            own, new[which] = adam(
                me, squares, weights[which], *moments[which], g_top, g_bottom, which, count, chunks, which == 2, first, blocks, new[which]
            )
            squares = lax.optimization_barrier((squares, *own))[0]
            sent.append((own, *send_around(n, own, swap)))
        whole = list(early_step(n, chunks, squares, weights, near_a, near_b, far_a, far_b, late, g_top, g_all, g_all_down, count))
        for k, (which, first, blocks, swap) in enumerate(PIECES):
            own, left, right, _ = sent[k]
            near = [(one, (layer, turn)) for turn, pair in ((0, own), (n - 1, left), (1, right)) for layer, one in enumerate(pair)]
            whole[which] = place(n, chunks, whole[which], near, which == 2, first, blocks)
        for k, (which, first, blocks, swap) in enumerate(PIECES):
            far = [(one, (layer, 2)) for layer, one in enumerate(sent[k][3]())]
            whole[which] = place(n, chunks, whole[which], far, which == 2, first, blocks)
        return (*whole, *(one[0] for one in new), *(one[1] for one in new))

    seq, part, rows = P(("rep", "dp"), None, None), P("rep", None, None), P("rep", "dp", None)
    state = P(None, "dp", None)
    step = jax.shard_map(
        step,
        mesh=mesh,
        in_specs=(seq, seq) + (P(None, None, None),) * 3 + (state,) * 6,
        out_specs=(part,) * 3 + (rows,) * 6,
        check_vma=False,
    )
    return step
```

```python
import functools

import jax
import jax.numpy as jnp
from jax import lax
from jax.experimental import pallas as pl
from jax.experimental.pallas import tpu as pltpu
from jax.sharding import PartitionSpec as P


F32, BF16 = jnp.float32, jnp.bfloat16
STRIPE = 128
VMEM_LIMIT = 60 << 20
EARLY = 2
PIECES = ((0, 0, 1, False), (0, 1, 3, True), (2, 0, 2, False), (1, 0, 3, True), (1, 3, 1, False))


def dot(a, b):
    return jnp.dot(a, b, preferred_element_type=F32)


def dot_nt(a, b):
    return lax.dot_general(a, b, (((1,), (1,)), ((), ())), preferred_element_type=F32)


def sigmoid(x):
    return 0.5 * jnp.tanh(0.5 * x) + 0.5


def normed(h):
    wide = h.astype(F32)
    scale = lax.rsqrt(jnp.mean(wide * wide, -1, keepdims=True) + 1e-6)
    return (wide * scale).astype(BF16)


def cost(flops, read_and_written):
    return pl.CostEstimate(flops=int(flops), bytes_accessed=int(read_and_written), transcendentals=0)


def params(**more):
    return pltpu.CompilerParams(vmem_limit_bytes=VMEM_LIMIT, **more)


def nbytes(*arrays):
    return sum(a.size * jnp.dtype(a.dtype).itemsize for a in arrays)


def once(shape, index_map):
    return pl.BlockSpec(shape, index_map, pipeline_mode=pl.Buffered(1))


def stripes(n, chunks, c):
    return [slice((o * chunks + c) * STRIPE, (o * chunks + c + 1) * STRIPE) for o in range(n)]


def forward_kernel(n, chunks, tiles, *refs):
    x_first, x_next, x_before, dy, wg, wu, wd, *refs = refs
    moments, (gate, up, a_t, h1, a1, a1_t, dy_t, near_a, near_b), refs = refs[:6], refs[6:15], refs[15:]
    act, normal, y, pack_a, pack_b, packed, own, send, recv = refs
    m = pl.program_id(0)
    width = n * STRIPE
    right, _, left = neighbours(n)

    def packing():
        each = pack_a.shape[2] // n
        for k, ref in enumerate(moments[:4]):
            for o in range(n):
                part = pack_a.at[k, :, o * each : (o + 1) * each]
                start = o * chunks * STRIPE
                yield pltpu.make_async_copy(ref.at[1, :, start : start + each], part, packed.at[k * n + o])
        for k, ref in enumerate(moments[4:]):
            yield pltpu.make_async_copy(ref.at[1, : pack_b.shape[1], :], pack_b.at[k], packed.at[4 * n + k])

    def copies():
        _, (half_a, half_b), _ = share()
        for k, (part, near, half) in enumerate(((pack_a, near_a, half_a), (pack_b, near_b, half_b))):
            yield remote(part.at[half], near.at[0, half], send.at[k], recv.at[k], right)
            yield remote(part.at[half], near.at[1, half], send.at[2 + k], recv.at[2 + k], left)
            yield pltpu.make_async_copy(part, near.at[2], own.at[k])

    def finish():
        h = (x_before[...].astype(F32) + y[...].astype(F32)).astype(BF16)
        h1[...] = h
        out = normed(h)
        a1[...] = out
        a1_t[...] = out.T

    @pl.when(m == 0)
    def _():
        for copy in packing():
            copy.start()
        hail((right, left))
        normal[0] = normed(x_first[...])

    @pl.when(m == 1)
    def _():
        pl.semaphore_wait(pltpu.get_barrier_semaphore(), 2)
        for copy in packing():
            copy.wait()
        for copy in copies():
            copy.start()

    @pl.when(m < tiles)
    def _():
        a = normal[lax.rem(m, 2)]

        def dots(c):
            for o, w in ((gate, wg), (up, wu)):
                o[c] = dot(a, jnp.concatenate([w[0, :, s] for s in stripes(n, chunks, c)], 1))

        dots(0)
        for c in range(chunks):
            if c + 1 < chunks:
                dots(c + 1)
            g = gate[c]
            act[:, c * width : (c + 1) * width] = (g * sigmoid(g) * up[c]).astype(BF16)
        a_t[...] = a.T
        dy_t[...] = dy[...].T
        finish()
        down = jnp.concatenate([wd[0, s, :] for c in range(chunks) for s in stripes(n, chunks, c)], 0)
        y[...] = dot(act[...], down).astype(BF16)
        normal[lax.rem(m + 1, 2)] = normed(x_next[...])

    @pl.when(m == tiles)
    def _():
        finish()
        for copy in copies():
            copy.wait()


def forward(n, chunks, x, dy, w_gate, w_up, w_down, moments, tm=256):
    t, d = x.shape
    ff, tiles, width = w_gate.shape[2], t // tm, n * STRIPE
    here, before = lambda m: jnp.minimum(m, tiles - 1), lambda m: jnp.maximum(m - 1, 0)
    row = lambda at: pl.BlockSpec((tm, d), lambda m: (at(m), 0))
    col = lambda at: pl.BlockSpec((d, tm), lambda m: (0, at(m)))
    wide = pl.BlockSpec((chunks, tm, width), lambda m: (0, here(m), 0))
    pack_a, pack_b = (4, d // n, EARLY * width), (2, EARLY * STRIPE, d)
    out = [jax.ShapeDtypeStruct((chunks, t, width), F32)] * 2
    out += [jax.ShapeDtypeStruct(s, BF16) for s in ((d, t), (t, d), (t, d), (d, t), (d, t))]
    out += [jax.ShapeDtypeStruct((3, *s), F32) for s in (pack_a, pack_b)]
    whole = pl.BlockSpec(memory_space=pl.ANY)
    return pl.pallas_call(
        functools.partial(forward_kernel, n, chunks, tiles),
        grid=(tiles + 1,),
        in_specs=[once((tm, d), lambda m: (0, 0)), row(lambda m: jnp.minimum(m + 1, tiles - 1)), row(before), row(here)]
        + [once((1, d, ff), lambda m: (0, 0, 0))] * 2
        + [once((1, ff, d), lambda m: (0, 0, 0))]
        + [whole] * 6,
        out_specs=[wide] * 2 + [col(here), row(before), row(before), col(before), col(here), whole, whole],
        out_shape=out,
        scratch_shapes=[
            pltpu.VMEM((tm, ff), BF16),
            pltpu.VMEM((2, tm, d), BF16),
            pltpu.VMEM((tm, d), BF16),
            pltpu.VMEM(pack_a, F32),
            pltpu.VMEM(pack_b, F32),
            pltpu.SemaphoreType.DMA((4 * n + 2,)),
            pltpu.SemaphoreType.DMA((2,)),
            pltpu.SemaphoreType.DMA((4,)),
            pltpu.SemaphoreType.DMA((4,)),
        ],
        compiler_params=params(collective_id=2, has_side_effects=True),
        cost_estimate=cost(6 * t * d * ff, nbytes(*out)),
        name="forward",
    )(x, x, x, dy, w_gate, w_up, w_down, *moments)


def neighbours(n):
    me = lax.axis_index("dp")
    return lax.rem(me + 1, n), lax.rem(me + 2, n), lax.rem(me + n - 1, n)


def hail(devices):
    barrier = pltpu.get_barrier_semaphore()
    for device in devices:
        pl.semaphore_signal(barrier, inc=1, device_id={"dp": device}, device_id_type=pl.DeviceIdType.MESH)


def remote(src, dst, send, recv, device, axis="dp"):
    return pltpu.make_async_remote_copy(
        src_ref=src, dst_ref=dst, send_sem=send, recv_sem=recv, device_id={axis: device}, device_id_type=pl.DeviceIdType.MESH
    )


def share():
    rep = lax.axis_index("rep")
    core = lax.rem(rep, 2)
    halves = [(pl.ds(2 * one, 2), pl.ds(one, 1)) for one in (core, 1 - core)]
    return rep + 1 - 2 * core, *halves


class Ring:
    def __init__(self, n, raw, got, mid, send, recv):
        half = raw.shape[1] // 2
        self.a, self.b = pl.ds(0, half), pl.ds(half, half)
        self.raw, self.got, self.mid = raw, got, mid
        self.send, self.recv = send, recv
        self.right, _, self.left = neighbours(n)

    def copy(self, k):
        source = (
            lambda: self.raw.at[2, self.a],
            lambda: self.raw.at[1, self.b],
            lambda: self.mid.at[0],
            lambda: self.raw.at[2, self.b],
            lambda: self.raw.at[3, self.a],
            lambda: self.mid.at[1],
        )[k]()
        return remote(source, self.got.at[k], self.send.at[k], self.recv.at[k], self.right if k < 3 else self.left)

    def begin(self, which=(0, 3, 1, 4)):
        for k in which:
            self.copy(k).start()

    def go_on(self):
        for k, owner, half in ((0, 1, self.a), (3, 3, self.b)):
            self.copy(k).wait_recv()
            self.mid[k // 3] = (self.raw[owner, half].astype(F32) + self.got[k].astype(F32)).astype(BF16)
            self.copy(k + 2).start()

    def end(self, out, squares):
        for plain, summed, half in ((4, 2, self.a), (1, 5, self.b)):
            self.copy(plain).wait_recv()
            self.copy(summed).wait_recv()
            total = self.raw[0, half].astype(F32) + self.got[plain].astype(F32) + self.got[summed].astype(F32)
            total = total.astype(BF16)
            out[0, half] = total
            total = total.astype(F32)
            squares[...] += jnp.sum((total * total).reshape(-1, 8, total.shape[1]), 0)

    def sent(self, *which):
        for k in which:
            self.copy(k).wait_send()


def lay_out(n, raw, gacc, uacc, dacc):
    me = lax.axis_index("dp")
    rows = gacc.shape[0] // n

    @pl.loop(0, n)
    def _(o):
        turn = lax.rem(o - me + n, n)
        mine, stripe = pl.ds(pl.multiple_of(o * rows, rows), rows), pl.ds(pl.multiple_of(o * STRIPE, STRIPE), STRIPE)
        raw[turn, :rows] = gacc[mine].astype(BF16)
        raw[turn, rows : 2 * rows] = uacc[mine].astype(BF16)
        for q in range(n):
            raw[turn, 2 * rows :, q * STRIPE : (q + 1) * STRIPE] = dacc[q * rows : (q + 1) * rows, stripe].astype(BF16)


def backward_parts(g, u, dact):
    dact = dact.astype(BF16).astype(F32)
    s = sigmoid(g)
    silu = g * s
    act = (silu * u).astype(BF16)
    du = (dact * silu).astype(BF16)
    dg = (dact * u * (s + silu * (1 - s))).astype(BF16)
    return act, dg, du


def states_gradient(da, h, dy):
    da = da.astype(BF16).astype(F32)
    wide = h.astype(F32)
    mean = jnp.mean(wide * wide, -1, keepdims=True) + 1e-6
    scale = lax.rsqrt(mean)
    dmean = jnp.sum(da * wide, -1, keepdims=True) * (-0.5 * scale / mean)
    back = (da * scale + wide * (dmean * (2.0 / wide.shape[1]))).astype(BF16)
    return (dy.astype(F32) + back.astype(F32)).astype(BF16)


def fetch(chunks, layer, whole, part, sems, c):
    n = sems.shape[0]
    for o in range(n):
        at = pl.ds(pl.multiple_of((o * chunks + c) * STRIPE, STRIPE), STRIPE)
        yield pltpu.make_async_copy(whole.at[layer, :, at], part.at[:, o * STRIPE : (o + 1) * STRIPE], sems.at[o])


def top_kernel(n, chunks, tiles, layer, *refs):
    wholes, (h, wd, wg, wu, near_a, near_b), refs = refs[:4], refs[4:10], refs[10:]
    dh, dh_t, g_out, last, squares_out, other_a, other_b, far_a, far_b, *refs = refs
    alls, refs = refs[:2], refs[2:]
    gacc, uacc, dacc, da, raw, got, mid, squares, send, recv, local, wg_part, wu_part, w_sems, *mines, e_send, e_recv = refs[:-5]
    slots, loaded = refs[-5:-1], refs[-1]
    c, i = pl.program_id(0), pl.program_id(1)
    tm = h.shape[0]
    right, _, left = neighbours(n)
    before = jnp.maximum(c - 1, 0)
    slot, here, there = lax.rem(before, 2), lax.rem(c, 2), lax.rem(c + 1, 2)
    ring = Ring(n, raw, got.at[slot], mid, send.at[slot], recv.at[slot])

    other, (half_a, half_b), _ = share()

    def moments():
        kind, rows = half_a.start, far_b.shape[1] // 2
        for side in range(2):
            part, way = pl.ds(side * rows, rows), (right, left)[side]
            yield remote(near_a.at[side, kind + side], far_a.at[kind + side], e_send.at[6, side], e_recv.at[6, side], way)
            yield remote(near_b.at[side, half_b, part], far_b.at[half_b, part], e_send.at[7, side], e_recv.at[7, side], way)

    def exchange(far):
        pairs = [(near_a.at[side, half_a], other_a.at[side]) for side in range(2)]
        pairs += [(near_b.at[side, half_b], other_b.at[side]) for side in range(2)]
        if far:
            pairs = [(far_a.at[half_a], far_a.at[half_a]), (far_b.at[half_b], far_b.at[half_b])]
        for k, (src, dst) in enumerate(pairs):
            yield remote(src, dst, e_send.at[8 + far, k], e_recv.at[8 + far, k], other, "rep")

    block = mines[0].shape[0]
    across = 2 * block // 3
    rounds = ((0, 0, block, 2), (1, across, block - across, 3), (1, 0, across, 4))

    def out(k):
        early, start, rows, _ = rounds[k]
        part = pl.ds(start, rows)
        for side in range(2):
            to = alls[early].at[side, part]
            yield remote(mines[early].at[part], to, e_send.at[2 * k, side], e_recv.at[2 * k, side], (right, left)[side])

    def on(k):
        early, start, rows, _ = rounds[k]
        every, half, at = alls[early], rows // 2, 2 * k + 1
        for side in range(2):
            part = pl.ds(start + side * half, half)
            yield remote(every.at[side, part], every.at[2, part], e_send.at[at, side], e_recv.at[at, side], (right, left)[side])

    def weights(c, slot):
        yield from fetch(chunks, layer, wg, wg_part.at[slot], w_sems.at[slot, 0], c)
        yield from fetch(chunks, layer, wu, wu_part.at[slot], w_sems.at[slot, 1], c)

    def loads(i):
        at, slot = pl.ds(pl.multiple_of(i * tm, tm), tm), lax.rem(i, 2)
        for k, (whole, part) in enumerate(zip(wholes, slots, strict=True)):
            source = whole.at[:, at] if k % 2 else whole.at[at]
            yield pltpu.make_async_copy(source, part.at[slot], loaded.at[k, slot])

    @pl.when(i == 0)
    def _():
        @pl.when(c == 0)
        def _():
            for copy in (*weights(c, here), *loads(i)):
                copy.start()
            barrier = pltpu.get_barrier_semaphore()
            pl.semaphore_signal(barrier, inc=1, device_id={"rep": other}, device_id_type=pl.DeviceIdType.MESH)
            hail((right, left))
            pl.semaphore_wait(barrier, 3)
            for copy in (*moments(), *exchange(False)):
                copy.start()
            squares[...] = jnp.zeros_like(squares)

        @pl.when(c > 0)
        def _():
            ring.begin((0, 3))

        for copy in weights(c, here):
            copy.wait()

        @pl.when(c < chunks - 1)
        def _():
            for copy in weights(c + 1, there):
                copy.start()

    @pl.when((c < chunks - 1) | (i < tiles - 1))
    def _():
        for load in loads(lax.rem(i + 1, tiles)):
            load.start()

    for load in loads(i):
        load.wait()
    a, a_t, dy, dy_t = (part.at[lax.rem(i, 2)] for part in slots)
    rows = pl.ds(pl.multiple_of(i * tm, tm), tm)
    pair = 2

    def work(at_end):
        parts = []
        for j in range(0, n, pair):
            to = slice(j * STRIPE, (j + pair) * STRIPE)
            w1, w2 = wg_part[here, :, to], wu_part[here, :, to]
            w3 = wd[0, j : j + pair, 0].reshape(pair * STRIPE, wd.shape[4])
            parts.append((to, w1, w2, dot(a[...], w1), dot(a[...], w2), dot_nt(dy[...], w3)))

        def states(fresh, dg, du, w1, w2):
            more = dot_nt(jnp.concatenate([dg, du], 1), jnp.concatenate([w1, w2], 1))
            da[rows, :] = jnp.where(fresh, 0.0, da[rows, :]) + more

        def weight_gradients(to, act, dg, du):
            for acc, left, right in ((gacc, a_t, dg), (uacc, a_t, du), (dacc, dy_t, act)):
                acc[:, to] = jnp.where(i == 0, 0.0, acc[:, to]) + dot(left[...], right)

        later = []
        for k, (to, w1, w2, g, u, dact) in enumerate(parts):
            fresh = (c == 0) & (k == 0)
            act, dg, du = backward_parts(g, u, dact)
            if at_end:
                states(fresh, dg, du, w1, w2)
                later.append((to, act, dg, du))
            else:
                weight_gradients(to, act, dg, du)
                states(fresh, dg, du, w1, w2)
        for one in later:
            weight_gradients(*one)
        if at_end:
            out = states_gradient(da[rows, :], h[...], dy[...])
            dh[...] = out
            dh_t[...] = out.T

    pl.when(c < chunks - 1)(lambda: work(False))
    pl.when(c == chunks - 1)(lambda: work(True))
    pl.when((c > 0) & (i == 0))(lambda: ring.begin((1, 4)))

    @pl.when((c > 0) & (i == tiles // 2 - 1))
    def _():
        ring.go_on()

    @pl.when(i == tiles // 2)
    def _():
        @pl.when(c == 1)
        def _():
            for copy in moments():
                copy.wait()
            for copy in exchange(True):
                copy.start()

        @pl.when(c == 2)
        def _():
            for copy in (*exchange(False), *exchange(True)):
                copy.wait()

        for k, (*_, first) in enumerate(rounds):

            @pl.when(c == first)
            def _(k=k):
                for copy in out(k):
                    copy.start()

            @pl.when(c == first + 1)
            def _(k=k):
                for copy in out(k):
                    copy.wait()
                for copy in on(k):
                    copy.start()

            if first + 2 < chunks:

                @pl.when(c == first + 2)
                def _(k=k):
                    for copy in on(k):
                        copy.wait()

    @pl.when((c == chunks - 1) & (i == tiles - 1))
    def _():
        for k, (*_, first) in enumerate(rounds):
            if first + 2 >= chunks:
                for copy in on(k):
                    copy.wait()

    @pl.when(i == tiles - 1)
    def _():
        @pl.when(c > 0)
        def _():
            ring.end(g_out, squares)
            ring.sent(*range(6))

        for k, mine in enumerate(mines):

            @pl.when(c == k + 1)
            def _(mine=mine):
                mine[...] = g_out[0]

        lay_out(n, raw, gacc, uacc, dacc)

        @pl.when(c == chunks - 1)
        def _():
            copy = pltpu.make_async_copy(raw, last, local)
            copy.start()
            squares_out[...] = squares[...]
            copy.wait()


def by_owner(n, w_down):
    layers, ff, d = w_down.shape
    return w_down.reshape(layers, n, ff // (n * STRIPE), STRIPE, d)


def top(n, chunks, layer, a, a_t, dy, dy_t, h, w_gate, w_up, w_down, near_a, near_b, tm=1024):
    t, d = a.shape
    width, tiles, block = n * STRIPE, t // tm, 3 * d // n
    assert tiles % 2 == 0
    at_end = lambda c, i: jnp.where(c == chunks - 1, i, 0)
    row_end, col_end = pl.BlockSpec((tm, d), lambda c, i: (at_end(c, i), 0)), pl.BlockSpec((d, tm), lambda c, i: (0, at_end(c, i)))
    down = pl.BlockSpec((1, n, 1, STRIPE, d), lambda c, i: (layer, 0, c, 0, 0))
    shapes = [
        jax.ShapeDtypeStruct((t, d), BF16),
        jax.ShapeDtypeStruct((d, t), BF16),
        jax.ShapeDtypeStruct((chunks - 1, block, width), BF16),
        jax.ShapeDtypeStruct((n, block, width), BF16),
        jax.ShapeDtypeStruct((8, width), F32),
        *(jax.ShapeDtypeStruct((2, one.shape[1] // 2, *one.shape[2:]), F32) for one in (near_a, near_b)),
        *(jax.ShapeDtypeStruct(one.shape[1:], F32) for one in (near_a, near_b)),
        *[jax.ShapeDtypeStruct((3, block, width), BF16)] * EARLY,
    ]
    return pl.pallas_call(
        functools.partial(top_kernel, n, chunks, tiles, layer),
        grid=(chunks, tiles),
        in_specs=[pl.BlockSpec(memory_space=pl.ANY)] * 4 + [row_end, down] + [pl.BlockSpec(memory_space=pl.ANY)] * 4,
        out_specs=[
            row_end,
            col_end,
            pl.BlockSpec((1, block, width), lambda c, i: (jnp.maximum(c - 1, 0), 0, 0)),
            pl.BlockSpec(memory_space=pl.ANY),
            pl.BlockSpec((8, width), lambda c, i: (0, 0)),
        ]
        + [pl.BlockSpec(memory_space=pl.ANY)] * (4 + EARLY),
        out_shape=shapes,
        scratch_shapes=[pltpu.VMEM((d, width), F32)] * 3
        + [
            pltpu.VMEM((t, d), F32),
            pltpu.VMEM((n, block, width), BF16),
            pltpu.VMEM((2, 6, block // 2, width), BF16),
            pltpu.VMEM((2, block // 2, width), BF16),
            pltpu.VMEM((8, width), F32),
            pltpu.SemaphoreType.DMA((2, 6)),
            pltpu.SemaphoreType.DMA((2, 6)),
            pltpu.SemaphoreType.DMA,
            pltpu.VMEM((2, d, width), BF16),
            pltpu.VMEM((2, d, width), BF16),
            pltpu.SemaphoreType.DMA((2, 2, n)),
            *[pltpu.VMEM((block, width), BF16)] * EARLY,
            pltpu.SemaphoreType.DMA((10, 4)),
            pltpu.SemaphoreType.DMA((10, 4)),
        ]
        + [pltpu.VMEM((2, *one), BF16) for one in ((tm, d), (d, tm)) * 2]
        + [pltpu.SemaphoreType.DMA((4, 2))],
        compiler_params=pltpu.CompilerParams(vmem_limit_bytes=67043328, collective_id=0, has_side_effects=True),
        cost_estimate=cost(16 * t * d * width * chunks, chunks * nbytes(a, a_t, dy, dy_t)),
        name="top",
    )(a, a_t, dy, dy_t, h, by_owner(n, w_down), w_gate, w_up, near_a, near_b)


def bottom_kernel(n, chunks, tiles, *refs):
    wholes, (wd, first, squares_in, g_out, squares_out), refs = refs[:5], refs[5:10], refs[10:]
    gacc, uacc, dacc, raw, got, mid, squares, send, recv, local, all_squares, to, fro, *slots, loaded = refs
    c, i = pl.program_id(0), pl.program_id(1)
    right, opposite, left = neighbours(n)
    tm = slots[0].shape[2]

    def loads(c, i):
        at, slot = pl.ds(pl.multiple_of(i * tm, tm), tm), lax.rem(i, 2)
        tiles_at = ((slice(None), at), (at,), (slice(None), at), (c, at), (c, at))
        for k, (whole, where, part) in enumerate(zip(wholes, tiles_at, slots, strict=True)):
            yield pltpu.make_async_copy(whole.at[*where], part.at[slot], loaded.at[k, slot])

    def ring(k):
        slot = lax.rem(k, 2)
        return Ring(n, raw.at[slot], got.at[k], mid.at[slot], send.at[k], recv.at[k])

    held = pltpu.make_async_copy(first, raw.at[0], local)

    @pl.when((c == 0) & (i == 0))
    def _():
        hail((right, opposite, left))
        held.start()
        for load in loads(c, i):
            load.start()
        squares[...] = squares_in[...]
        pl.semaphore_wait(pltpu.get_barrier_semaphore(), 3)
        Ring(n, first, got.at[0], mid.at[0], send.at[0], recv.at[0]).begin((0, 3))

    @pl.when((c > 0) & (i == 0))
    def _():
        ring(c).begin((0, 3))

    @pl.when((c < chunks - 1) | ((c == chunks - 1) & (i < tiles - 1)))
    def _():
        for load in loads(jnp.where(i == tiles - 1, c + 1, c), lax.rem(i + 1, tiles)):
            load.start()

    @pl.when(c < chunks)
    def _():
        for load in loads(c, i):
            load.wait()
        a_t, dy, dy_t, gate, up = (part.at[lax.rem(i, 2)] for part in slots)
        pair = 2
        parts = []
        for j in range(0, n, pair):
            w = wd[0, j : j + pair, 0].reshape(pair * STRIPE, wd.shape[4])
            parts.append((slice(j * STRIPE, (j + pair) * STRIPE), dot_nt(dy[...], w)))
        for to, dact in parts:
            act, dg, du = backward_parts(gate[:, to], up[:, to], dact)
            for acc, left, right in ((gacc, a_t, dg), (uacc, a_t, du), (dacc, dy_t, act)):
                acc[:, to] = jnp.where(i == 0, 0.0, acc[:, to]) + dot(left[...], right)

    @pl.when(i == tiles // 4)
    def _():
        @pl.when(c > 0)
        def _():
            before = ring(c - 1)
            before.end(g_out, squares)
            before.sent(*range(6))

        pl.when(c == 0)(held.wait)
        ring(c).begin((1, 4))

    pl.when(i == tiles // 2)(lambda: ring(c).go_on())

    @pl.when((c < chunks) & (i == tiles - 1))
    def _():
        lay_out(n, raw.at[lax.rem(c + 1, 2)], gacc, uacc, dacc)

    @pl.when((c == chunks) & (i == tiles - 1))
    def _():
        final = ring(c)
        final.end(g_out, squares)
        final.sent(*range(6))
        me = lax.axis_index("dp")
        all_squares[me] = squares[...]
        copies = [
            remote(squares, all_squares.at[me], to.at[k], fro.at[k], device) for k, device in enumerate((right, opposite, left))
        ]
        for copy in copies:
            copy.start()
        for copy in copies:
            copy.wait()
        total = all_squares[0]
        for k in range(1, n):
            total += all_squares[k]
        squares_out[...] = total


def bottom(n, chunks, layer, a_t, dy, dy_t, gate, up, w_down, first, squares, tm=1024):
    d, t = a_t.shape
    width, tiles, block = n * STRIPE, t // tm, 3 * d // n
    assert tiles % 2 == 0
    small = pl.BlockSpec((8, width), lambda c, i: (0, 0))
    down = pl.BlockSpec((1, n, 1, STRIPE, d), lambda c, i: (layer, 0, jnp.minimum(c, chunks - 1), 0, 0))
    done = lambda c, i: jnp.where((c == chunks) & (i == tiles - 1), chunks, jnp.maximum(c - 1, 0))
    return pl.pallas_call(
        functools.partial(bottom_kernel, n, chunks, tiles),
        grid=(chunks + 1, tiles),
        in_specs=[pl.BlockSpec(memory_space=pl.ANY)] * 5 + [down, pl.BlockSpec(memory_space=pl.ANY), small],
        out_specs=[pl.BlockSpec((1, block, width), lambda c, i: (done(c, i), 0, 0)), small],
        out_shape=[
            jax.ShapeDtypeStruct((chunks + 1, block, width), BF16),
            jax.ShapeDtypeStruct((8, width), F32),
        ],
        scratch_shapes=[pltpu.VMEM((d, width), F32)] * 3
        + [
            pltpu.VMEM((2, n, block, width), BF16),
            pltpu.VMEM((chunks + 1, 6, block // 2, width), BF16),
            pltpu.VMEM((2, 2, block // 2, width), BF16),
            pltpu.VMEM((8, width), F32),
            pltpu.SemaphoreType.DMA((chunks + 1, 6)),
            pltpu.SemaphoreType.DMA((chunks + 1, 6)),
            pltpu.SemaphoreType.DMA,
            pltpu.VMEM((n, 8, width), F32),
            pltpu.SemaphoreType.DMA((3,)),
            pltpu.SemaphoreType.DMA((3,)),
        ]
        + [pltpu.VMEM((2, *one), BF16) for one in ((d, tm), (tm, d), (d, tm))]
        + [pltpu.VMEM((2, tm, width), F32)] * 2
        + [pltpu.SemaphoreType.DMA((5, 2))],
        compiler_params=pltpu.CompilerParams(vmem_limit_bytes=VMEM_LIMIT, collective_id=1, has_side_effects=True),
        cost_estimate=cost(8 * t * d * width * chunks, nbytes(gate, up) + chunks * nbytes(a_t, dy, dy_t)),
        name="bottom",
    )(a_t, dy, dy_t, gate, up, by_owner(n, w_down), first, squares)


def clip(squares, count):
    return jnp.minimum(1.0, 0.5 * lax.rsqrt(jnp.full((1, 1), jnp.sum(squares)) / count + 1e-30))


def adamw(w, m, v, g):
    m = 0.9 * m + 0.1 * g
    v = 0.95 * v + 0.05 * g * g
    old = w.astype(F32)
    step = m * lax.rsqrt(v + 1e-8) + 0.1 * old
    return (old - 0.02 * step).astype(BF16), m, v


def upright(g):
    return jnp.concatenate([g[:, q : q + STRIPE].T for q in range(0, g.shape[1], STRIPE)], 1)


def adam_kernel(chunks, tall, count, squares, w, m, v, g_top, g_bottom, *refs):
    *w_out, m_out, v_out = refs
    factor = clip(squares[...], count)

    def work(layer, c, g, to):
        def at(c):
            rows = pl.ds(pl.multiple_of(c * STRIPE, STRIPE), STRIPE)
            return (rows, slice(None)) if tall else (slice(None), rows)

        g = upright(g.astype(F32)) if tall else g.astype(F32)
        new, m_new, v_new = adamw(w[layer, *at(c)], m[layer, *at(c)], v[layer, *at(c)], g * factor)
        if to is not None:
            w_out[layer][at(to)] = new
        m_out[layer, *at(c)] = m_new
        v_out[layer, *at(c)] = v_new

    @pl.loop(0, EARLY)
    def _(c):
        work(0, c, g_bottom[c + 1], c)
        work(1, c, g_top[c], None)

    @pl.loop(EARLY, chunks - 1)
    def _(c):
        work(0, c, g_bottom[c + 1], c)
        work(1, c, g_top[c], c - EARLY)

    work(0, chunks - 1, g_bottom[chunks], chunks - 1)
    work(1, chunks - 1, g_bottom[0], chunks - 1 - EARLY)


def adam(me, squares, w, m, v, g_top, g_bottom, which, count, chunks, tall, first, blocks, begun):
    layers, rows, _ = m.shape
    g_rows = g_top.shape[1] // 3
    g_width, width = (2 * STRIPE, 2 * g_rows) if tall else (STRIPE, STRIPE * chunks)
    block = pl.BlockSpec((layers, rows, width), lambda i, me: (0, 0, first + i))
    rest = EARLY * STRIPE
    new = [(rows, width), (rows - rest, width) if tall else (rows, width - rest)]
    out = [jax.ShapeDtypeStruct((r, c * blocks), BF16) for r, c in new] + [jax.ShapeDtypeStruct(m.shape, F32)] * 2
    fixed = list(begun)

    def body(me_ref, *refs):
        adam_kernel(chunks, tall, count, *refs[:6], *refs[6 + len(fixed) :])

    outs = pl.pallas_call(
        body,
        grid_spec=pltpu.PrefetchScalarGridSpec(
            num_scalar_prefetch=1,
            grid=(blocks,),
            in_specs=[pl.BlockSpec(squares.shape, lambda i, me: (0, 0))]
            + [pl.BlockSpec((layers, rows, width), lambda i, me: (0, me[0], first + i)), block, block]
            + [pl.BlockSpec((g.shape[0], g_rows, g_width), lambda i, me: (0, which, first + i)) for g in (g_top, g_bottom)]
            + [pl.BlockSpec(memory_space=pl.ANY)] * len(fixed),
            out_specs=[pl.BlockSpec(one, lambda i, me: (0, i)) for one in new] + [block, block],
        ),
        out_shape=out,
        input_output_aliases={7 + k: layers + k for k in range(len(fixed))},
        compiler_params=params(),
        cost_estimate=cost(16 * rows * width * blocks * layers, 22 * rows * width * blocks * layers),
        name="adam",
    )(me, squares, w, m, v, g_top, g_bottom, *fixed)
    return outs[:layers], outs[layers:]


def early_kernel(n, count, squares, *refs):
    wg, wu, (wd, near_a, near_b, other_a, other_b, far_a, far_b, g_top), refs = refs[:n], refs[n : 2 * n], refs[2 * n : 2 * n + 8], refs[2 * n + 8 :]
    alls, outs, (a, b, g, loaded, across, down, sems) = refs[:EARLY], refs[EARLY : EARLY + 3], refs[EARLY + 3 :]
    rows, each = a.shape[2], EARLY * STRIPE
    _, mine, others = share()
    loads = []
    for k, (part, near, other, far) in enumerate(((a, near_a, other_a, far_a), (b, near_b, other_b, far_b))):
        loads += [(near.at[2], part.at[0]), (far, part.at[2])]
        for turn, side in ((1, 1), (3, 0)):
            loads += [(near.at[side, mine[k]], part.at[turn, mine[k]]), (other.at[side], part.at[turn, others[k]])]
    for k, every in enumerate(alls):
        loads += [(source, g.at[turn, k]) for turn, source in enumerate((g_top.at[k], every.at[1], every.at[2], every.at[0]))]
    loads = [pltpu.make_async_copy(src, dst, loaded.at[k]) for k, (src, dst) in enumerate(loads)]
    for copy in loads:
        copy.start()
    factor = clip(squares[...], count)
    me = lax.axis_index("dp")
    for copy in loads:
        copy.wait()

    @pl.loop(0, n)
    def _(turn):
        o = lax.rem(me + turn, n)
        at = pl.ds(pl.multiple_of(o * rows, rows), rows)
        for k, w in enumerate((wg, wu)):
            for j in range(n):
                to = slice(j * each, (j + 1) * each)
                grad = jnp.concatenate([g[turn, e, k * rows : (k + 1) * rows, j * STRIPE : (j + 1) * STRIPE] for e in range(EARLY)], 1)
                across[k, at, to] = adamw(w[j][0, at, :], a[turn, 2 * k, :, to], a[turn, 2 * k + 1, :, to], grad.astype(F32) * factor)[0]
        for e in range(EARLY):
            part = slice(e * STRIPE, (e + 1) * STRIPE)
            grad = upright(g[turn, e, 2 * rows :, :].astype(F32)) * factor
            down[o, part, :] = adamw(wd[0, o, e], b[turn, 0, part, :], b[turn, 1, part, :], grad)[0]

    copies, whole = [], outs[0].shape[2] // n
    for o in range(n):
        for k in range(2):
            copies.append((across.at[k, :, o * each : (o + 1) * each], outs[k].at[1, :, o * whole : o * whole + each]))
        copies.append((down.at[o], outs[2].at[1, o * whole : o * whole + each, :]))
    copies = [pltpu.make_async_copy(src, dst, sems.at[k]) for k, (src, dst) in enumerate(copies)]
    for copy in copies:
        copy.start()
    for copy in copies:
        copy.wait()


def early_step(n, chunks, squares, weights, moments, g_top, alls, count):
    w_gate, w_up, w_down = weights
    d, each = w_gate.shape[1], EARLY * STRIPE
    assert chunks % EARLY == 0
    across = [pl.BlockSpec((1, d, each), lambda i, o=o: (1, 0, o * (chunks // EARLY))) for o in range(n)]
    down = pl.BlockSpec((1, n, EARLY, STRIPE, d), lambda i: (1, 0, 0, 0, 0))
    arrays = (*moments, g_top, *alls)
    held = [(n, *one.shape) for one in moments[-2:]]
    return pl.pallas_call(
        functools.partial(early_kernel, n, count),
        grid=(1,),
        in_specs=[pl.BlockSpec(squares.shape, lambda i: (0, 0))] + across + across + [down] + [pl.BlockSpec(memory_space=pl.ANY)] * len(arrays),
        out_specs=[pl.BlockSpec(memory_space=pl.ANY)] * 3,
        out_shape=[jax.ShapeDtypeStruct(w.shape, BF16) for w in weights],
        scratch_shapes=[
            *(pltpu.VMEM(one, F32) for one in held),
            pltpu.VMEM((n, EARLY, *g_top.shape[1:]), BF16),
            pltpu.SemaphoreType.DMA((12 + n * EARLY,)),
            pltpu.VMEM((2, d, n * each), BF16),
            pltpu.VMEM((n, each, d), BF16),
            pltpu.SemaphoreType.DMA((3 * n,)),
        ],
        compiler_params=params(),
        cost_estimate=cost(16 * 3 * d * n * each, nbytes(*moments)),
        name="early",
    )(squares, *[w_gate] * n, *[w_up] * n, by_owner(n, w_down), *arrays)


def place_kernel(n, pieces, regions, *refs):
    arrays, out, sems = refs[: len(pieces)], refs[-2], refs[-1]
    me = lax.axis_index("dp")
    copies = []
    for array, (layer, turn) in zip(arrays, pieces, strict=True):
        o = lax.rem(me + turn, n)
        for from_column, rows_before, columns, region in regions(layer):
            rows = array.shape[0]
            step = rows + rows_before
            to = out.at[layer, pl.ds(pl.multiple_of(o * step + rows_before, 16), rows), region]
            copies.append((array.at[:, from_column : from_column + columns], to))
    copies = [pltpu.make_async_copy(src, dst, sems.at[k]) for k, (src, dst) in enumerate(copies)]
    for copy in copies:
        copy.start()
    for copy in copies:
        copy.wait()


def place(n, chunks, whole, pieces, tall, first, blocks):
    arrays, where = zip(*pieces, strict=True)
    full = STRIPE * chunks

    def regions(layer):
        if tall:
            columns = arrays[0].shape[1]
            return [(0, layer * EARLY * STRIPE, columns, slice(first * columns // blocks, (first + blocks) * columns // blocks))]
        there = layer * EARLY * STRIPE
        columns = full - there
        return [(j * columns, 0, columns, slice((first + j) * full + there, (first + j + 1) * full)) for j in range(blocks)]

    return pl.pallas_call(
        functools.partial(place_kernel, n, where, regions),
        grid=(1,),
        in_specs=[pl.BlockSpec(one.shape, lambda i: (0, 0)) for one in arrays] + [pl.BlockSpec(memory_space=pl.ANY)],
        out_specs=pl.BlockSpec(memory_space=pl.ANY),
        out_shape=jax.ShapeDtypeStruct(whole.shape, whole.dtype),
        input_output_aliases={len(arrays): 0},
        scratch_shapes=[pltpu.SemaphoreType.DMA((len(arrays) * blocks,))],
        compiler_params=params(),
        cost_estimate=cost(arrays[0].size, 4 * nbytes(*arrays)),
        name="place",
    )(*arrays, whole)


def send_around(n, own, swap):
    right, left = [(i, (i + 1) % n) for i in range(n)], [(i, (i - 1) % n) for i in range(n)]

    def send(one, way):
        return lax.ppermute(one, "dp", way)

    def in_order(a, b):
        return (b, a) if swap else (a, b)

    a, b = in_order(*own)
    left_a, right_b = send(a, right), send(b, left)
    left_b, right_a = send(b, right), send(a, left)
    return in_order(left_a, left_b), in_order(right_a, right_b), lambda: in_order(send(left_a, right), send(right_b, left))


def solution(mesh):
    n = mesh.shape["dp"]

    def step(x, dy, w_gate, w_up, w_down, m_gate, m_up, m_down, v_gate, v_up, v_down):
        x, dy = x[0], dy[0]
        chunks = w_gate.shape[2] // (n * STRIPE)
        me = lax.axis_index("dp").astype(jnp.int32).reshape(1)

        weights, moments = (w_gate, w_up, w_down), ((m_gate, v_gate), (m_up, v_up), (m_down, v_down))
        *parts, near_a, near_b = forward(n, chunks, x, dy, *weights, sum(moments, ()))
        gate, up, a0_t, h1, a1, a1_t, dy_t = parts
        parts = top(n, chunks, 1, a1, a1_t, dy, dy_t, h1, *weights, near_a, near_b)
        (dh, dh_t, g_top, last, squares), early, alls = parts[:5], parts[5:9], parts[9:]
        g_bottom, squares = bottom(n, chunks, 0, a0_t, dh, dh_t, gate, up, w_down, last, squares)

        new, sent, count = [[], [], []], [], 3 * w_gate.size
        for which, first, blocks, swap in PIECES:
            own, new[which] = adam(
                me, squares, weights[which], *moments[which], g_top, g_bottom, which, count, chunks, which == 2, first, blocks, new[which]
            )
            squares = lax.optimization_barrier((squares, *own))[0]
            sent.append((own, *send_around(n, own, swap)))
        whole = list(early_step(n, chunks, squares, weights, (near_a, near_b, *early), g_top, alls, count))
        for k, (which, first, blocks, swap) in enumerate(PIECES):
            own, left, right, _ = sent[k]
            near = [(one, (layer, turn)) for turn, pair in ((0, own), (n - 1, left), (1, right)) for layer, one in enumerate(pair)]
            whole[which] = place(n, chunks, whole[which], near, which == 2, first, blocks)
        for k, (which, first, blocks, swap) in enumerate(PIECES):
            far = [(one, (layer, 2)) for layer, one in enumerate(sent[k][3]())]
            whole[which] = place(n, chunks, whole[which], far, which == 2, first, blocks)
        return (*whole, *(one[0] for one in new), *(one[1] for one in new))

    seq, part, rows = P(("rep", "dp"), None, None), P("rep", None, None), P("rep", "dp", None)
    state = P(None, "dp", None)
    step = jax.shard_map(
        step,
        mesh=mesh,
        in_specs=(seq, seq) + (P(None, None, None),) * 3 + (state,) * 6,
        out_specs=(part,) * 3 + (rows,) * 6,
        check_vma=False,
    )
    return step
```

```python
import functools

import jax
import jax.numpy as jnp
from jax import lax
from jax.experimental import pallas as pl
from jax.experimental.pallas import tpu as pltpu
from jax.sharding import PartitionSpec as P


F32, BF16 = jnp.float32, jnp.bfloat16
STRIPE = 128
VMEM_LIMIT = 60 << 20
EARLY, EARLY_DOWN = 2, 3
PIECES = ((0, 0, 1, True), (0, 1, 2, False), (2, 0, 2, True), (1, 0, 4, False), (0, 3, 1, False))


def dot(a, b):
    return jnp.dot(a, b, preferred_element_type=F32)


def dot_nt(a, b):
    return lax.dot_general(a, b, (((1,), (1,)), ((), ())), preferred_element_type=F32)


def sigmoid(x):
    return 0.5 * jnp.tanh(0.5 * x) + 0.5


def normed(h):
    wide = h.astype(F32)
    scale = lax.rsqrt(jnp.mean(wide * wide, -1, keepdims=True) + 1e-6)
    return (wide * scale).astype(BF16)


def cost(flops, read_and_written):
    return pl.CostEstimate(flops=int(flops), bytes_accessed=int(read_and_written), transcendentals=0)


def params(**more):
    return pltpu.CompilerParams(vmem_limit_bytes=VMEM_LIMIT, **more)


def nbytes(*arrays):
    return sum(a.size * jnp.dtype(a.dtype).itemsize for a in arrays)


def once(shape, index_map):
    return pl.BlockSpec(shape, index_map, pipeline_mode=pl.Buffered(1))


def stripes(n, chunks, c):
    return [slice((o * chunks + c) * STRIPE, (o * chunks + c + 1) * STRIPE) for o in range(n)]


def forward_kernel(n, chunks, tiles, *refs):
    x_first, x_next, x_before, dy, wg, wu, wd, *refs = refs
    moments, (gate, up, a_t, h1, a1, a1_t, dy_t, near_a, near_b), refs = refs[:6], refs[6:15], refs[15:]
    act, normal, y, pack_a, pack_b, packed, own, send, recv = refs
    m = pl.program_id(0)
    width = n * STRIPE
    right, _, left = neighbours(n)

    def packing():
        each = pack_a.shape[2] // n
        for k, ref in enumerate(moments[:4]):
            for o in range(n):
                part = pack_a.at[k, :, o * each : (o + 1) * each]
                start = o * chunks * STRIPE
                yield pltpu.make_async_copy(ref.at[1, :, start : start + each], part, packed.at[k * n + o])
        for k, ref in enumerate(moments[4:]):
            yield pltpu.make_async_copy(ref.at[1, : pack_b.shape[1], :], pack_b.at[k], packed.at[4 * n + k])

    def copies():
        _, (half_a, half_b), _ = share()
        for k, (part, near, half) in enumerate(((pack_a, near_a, half_a), (pack_b, near_b, half_b))):
            yield remote(part.at[half], near.at[0, half], send.at[k], recv.at[k], right)
            yield remote(part.at[half], near.at[1, half], send.at[2 + k], recv.at[2 + k], left)
            yield pltpu.make_async_copy(part, near.at[2], own.at[k])

    def finish():
        h = (x_before[...].astype(F32) + y[...].astype(F32)).astype(BF16)
        h1[...] = h
        out = normed(h)
        a1[...] = out
        a1_t[...] = out.T

    @pl.when(m == 0)
    def _():
        for copy in packing():
            copy.start()
        hail((right, left))
        normal[0] = normed(x_first[...])

    @pl.when(m == 1)
    def _():
        pl.semaphore_wait(pltpu.get_barrier_semaphore(), 2)
        for copy in packing():
            copy.wait()
        for copy in copies():
            copy.start()

    @pl.when(m < tiles)
    def _():
        a = normal[lax.rem(m, 2)]

        def dots(c):
            for o, w in ((gate, wg), (up, wu)):
                o[c] = dot(a, jnp.concatenate([w[0, :, s] for s in stripes(n, chunks, c)], 1))

        dots(0)
        for c in range(chunks):
            if c + 1 < chunks:
                dots(c + 1)
            g = gate[c]
            act[:, c * width : (c + 1) * width] = (g * sigmoid(g) * up[c]).astype(BF16)
        a_t[...] = a.T
        dy_t[...] = dy[...].T
        finish()
        down = jnp.concatenate([wd[0, s, :] for c in range(chunks) for s in stripes(n, chunks, c)], 0)
        y[...] = dot(act[...], down).astype(BF16)
        normal[lax.rem(m + 1, 2)] = normed(x_next[...])

    @pl.when(m == tiles)
    def _():
        finish()
        for copy in copies():
            copy.wait()


def forward(n, chunks, x, dy, w_gate, w_up, w_down, moments, tm=256):
    t, d = x.shape
    ff, tiles, width = w_gate.shape[2], t // tm, n * STRIPE
    here, before = lambda m: jnp.minimum(m, tiles - 1), lambda m: jnp.maximum(m - 1, 0)
    row = lambda at: pl.BlockSpec((tm, d), lambda m: (at(m), 0))
    col = lambda at: pl.BlockSpec((d, tm), lambda m: (0, at(m)))
    wide = pl.BlockSpec((chunks, tm, width), lambda m: (0, here(m), 0))
    pack_a, pack_b = (4, d // n, EARLY * width), (2, EARLY_DOWN * STRIPE, d)
    out = [jax.ShapeDtypeStruct((chunks, t, width), F32)] * 2
    out += [jax.ShapeDtypeStruct(s, BF16) for s in ((d, t), (t, d), (t, d), (d, t), (d, t))]
    out += [jax.ShapeDtypeStruct((3, *s), F32) for s in (pack_a, pack_b)]
    whole = pl.BlockSpec(memory_space=pl.ANY)
    return pl.pallas_call(
        functools.partial(forward_kernel, n, chunks, tiles),
        grid=(tiles + 1,),
        in_specs=[once((tm, d), lambda m: (0, 0)), row(lambda m: jnp.minimum(m + 1, tiles - 1)), row(before), row(here)]
        + [once((1, d, ff), lambda m: (0, 0, 0))] * 2
        + [once((1, ff, d), lambda m: (0, 0, 0))]
        + [whole] * 6,
        out_specs=[wide] * 2 + [col(here), row(before), row(before), col(before), col(here), whole, whole],
        out_shape=out,
        scratch_shapes=[
            pltpu.VMEM((tm, ff), BF16),
            pltpu.VMEM((2, tm, d), BF16),
            pltpu.VMEM((tm, d), BF16),
            pltpu.VMEM(pack_a, F32),
            pltpu.VMEM(pack_b, F32),
            pltpu.SemaphoreType.DMA((4 * n + 2,)),
            pltpu.SemaphoreType.DMA((2,)),
            pltpu.SemaphoreType.DMA((4,)),
            pltpu.SemaphoreType.DMA((4,)),
        ],
        compiler_params=params(collective_id=2, has_side_effects=True),
        cost_estimate=cost(6 * t * d * ff, nbytes(*out)),
        name="forward",
    )(x, x, x, dy, w_gate, w_up, w_down, *moments)


def neighbours(n):
    me = lax.axis_index("dp")
    return lax.rem(me + 1, n), lax.rem(me + 2, n), lax.rem(me + n - 1, n)


def hail(devices):
    barrier = pltpu.get_barrier_semaphore()
    for device in devices:
        pl.semaphore_signal(barrier, inc=1, device_id={"dp": device}, device_id_type=pl.DeviceIdType.MESH)


def remote(src, dst, send, recv, device, axis="dp"):
    return pltpu.make_async_remote_copy(
        src_ref=src, dst_ref=dst, send_sem=send, recv_sem=recv, device_id={axis: device}, device_id_type=pl.DeviceIdType.MESH
    )


def share():
    rep = lax.axis_index("rep")
    core = lax.rem(rep, 2)
    halves = [(pl.ds(2 * one, 2), pl.ds(one, 1)) for one in (core, 1 - core)]
    return rep + 1 - 2 * core, *halves


class Ring:
    def __init__(self, n, raw, got, mid, send, recv):
        half = raw.shape[1] // 2
        self.a, self.b = pl.ds(0, half), pl.ds(half, half)
        self.raw, self.got, self.mid = raw, got, mid
        self.send, self.recv = send, recv
        self.right, _, self.left = neighbours(n)

    def copy(self, k):
        source = (
            lambda: self.raw.at[2, self.a],
            lambda: self.raw.at[1, self.b],
            lambda: self.mid.at[0],
            lambda: self.raw.at[2, self.b],
            lambda: self.raw.at[3, self.a],
            lambda: self.mid.at[1],
        )[k]()
        return remote(source, self.got.at[k], self.send.at[k], self.recv.at[k], self.right if k < 3 else self.left)

    def begin(self, which=(0, 3, 1, 4)):
        for k in which:
            self.copy(k).start()

    def go_on(self):
        for k, owner, half in ((0, 1, self.a), (3, 3, self.b)):
            self.copy(k).wait_recv()
            self.mid[k // 3] = (self.raw[owner, half].astype(F32) + self.got[k].astype(F32)).astype(BF16)
            self.copy(k + 2).start()

    def end(self, out, squares):
        for plain, summed, half in ((4, 2, self.a), (1, 5, self.b)):
            self.copy(plain).wait_recv()
            self.copy(summed).wait_recv()
            total = self.raw[0, half].astype(F32) + self.got[plain].astype(F32) + self.got[summed].astype(F32)
            total = total.astype(BF16)
            out[half] = total
            total = total.astype(F32)
            squares[...] += jnp.sum((total * total).reshape(-1, 8, total.shape[1]), 0)

    def sent(self, *which):
        for k in which:
            self.copy(k).wait_send()


def lay_out(n, raw, gacc, uacc, dacc):
    me = lax.axis_index("dp")
    rows = gacc.shape[0] // n

    @pl.loop(0, n)
    def _(o):
        turn = lax.rem(o - me + n, n)
        mine, stripe = pl.ds(pl.multiple_of(o * rows, rows), rows), pl.ds(pl.multiple_of(o * STRIPE, STRIPE), STRIPE)
        raw[turn, :rows] = gacc[mine].astype(BF16)
        raw[turn, rows : 2 * rows] = uacc[mine].astype(BF16)
        for q in range(n):
            raw[turn, 2 * rows :, q * STRIPE : (q + 1) * STRIPE] = dacc[q * rows : (q + 1) * rows, stripe].astype(BF16)


def backward_parts(g, u, dact):
    dact = dact.astype(BF16).astype(F32)
    s = sigmoid(g)
    silu = g * s
    act = (silu * u).astype(BF16)
    du = (dact * silu).astype(BF16)
    dg = (dact * u * (s + silu * (1 - s))).astype(BF16)
    return act, dg, du


def states_gradient(da, h, dy):
    da = da.astype(BF16).astype(F32)
    wide = h.astype(F32)
    mean = jnp.mean(wide * wide, -1, keepdims=True) + 1e-6
    scale = lax.rsqrt(mean)
    dmean = jnp.sum(da * wide, -1, keepdims=True) * (-0.5 * scale / mean)
    back = (da * scale + wide * (dmean * (2.0 / wide.shape[1]))).astype(BF16)
    return (dy.astype(F32) + back.astype(F32)).astype(BF16)


def fetch(chunks, layer, whole, part, sems, c):
    n = sems.shape[0]
    for o in range(n):
        at = pl.ds(pl.multiple_of((o * chunks + c) * STRIPE, STRIPE), STRIPE)
        yield pltpu.make_async_copy(whole.at[layer, :, at], part.at[:, o * STRIPE : (o + 1) * STRIPE], sems.at[o])


def top_kernel(n, chunks, tiles, layer, *refs):
    wholes, (h, wd, wg, wu, near_a, near_b), refs = refs[:4], refs[4:10], refs[10:]
    dh, dh_t, g_out, last, squares_out, other_a, other_b, far_a, far_b, *refs = refs
    alls, refs = refs[:EARLY_DOWN], refs[EARLY_DOWN:]
    gacc, uacc, dacc, da, raw, got, mid, squares, send, recv, local, wg_part, wu_part, w_sems, *mines, e_send, e_recv = refs[:-5]
    slots, loaded = refs[-5:-1], refs[-1]
    c, i = pl.program_id(0), pl.program_id(1)
    tm = h.shape[0]
    right, _, left = neighbours(n)
    before = jnp.maximum(c - 1, 0)
    slot, here, there = lax.rem(before, 2), lax.rem(c, 2), lax.rem(c + 1, 2)
    ring = Ring(n, raw, got.at[slot], mid, send.at[slot], recv.at[slot])

    other, (half_a, half_b), _ = share()

    def moments():
        kind, rows = half_a.start, far_b.shape[1] // 2
        for side in range(2):
            part, way = pl.ds(side * rows, rows), (right, left)[side]
            yield remote(near_a.at[side, kind + side], far_a.at[kind + side], e_send.at[10, side], e_recv.at[10, side], way)
            yield remote(near_b.at[side, half_b, part], far_b.at[half_b, part], e_send.at[11, side], e_recv.at[11, side], way)

    def exchange(far):
        pairs = [(near_a.at[side, half_a], other_a.at[side]) for side in range(2)]
        pairs += [(near_b.at[side, half_b], other_b.at[side]) for side in range(2)]
        if far:
            pairs = [(far_a.at[half_a], far_a.at[half_a]), (far_b.at[half_b], far_b.at[half_b])]
        for k, (src, dst) in enumerate(pairs):
            yield remote(src, dst, e_send.at[12 + far, k], e_recv.at[12 + far, k], other, "rep")

    block = mines[0].shape[0]
    across = 2 * block // 3
    down = block - across
    rounds = ((0, across, down, 1, True), (0, 0, across, 2, False), (1, across, down, 2, True), (2, 0, down, 3, True), (1, 0, across, 4, False))

    def out(k):
        early, start, rows, *_ = rounds[k]
        part = pl.ds(start, rows)
        for side in range(2):
            to = alls[early].at[side, part]
            yield remote(mines[early].at[part], to, e_send.at[2 * k, side], e_recv.at[2 * k, side], (right, left)[side])

    def on(k):
        early, start, rows, *_ = rounds[k]
        every, half, at = alls[early], rows // 2, 2 * k + 1
        for side in range(2):
            part = pl.ds(start + side * half, half)
            yield remote(every.at[side, part], every.at[2, part], e_send.at[at, side], e_recv.at[at, side], (right, left)[side])

    def weights(c, slot):
        yield from fetch(chunks, layer, wg, wg_part.at[slot], w_sems.at[slot, 0], c)
        yield from fetch(chunks, layer, wu, wu_part.at[slot], w_sems.at[slot, 1], c)

    def loads(i):
        at, slot = pl.ds(pl.multiple_of(i * tm, tm), tm), lax.rem(i, 2)
        for k, (whole, part) in enumerate(zip(wholes, slots, strict=True)):
            source = whole.at[:, at] if k % 2 else whole.at[at]
            yield pltpu.make_async_copy(source, part.at[slot], loaded.at[k, slot])

    @pl.when(i == 0)
    def _():
        @pl.when(c == 0)
        def _():
            for copy in (*weights(c, here), *loads(i)):
                copy.start()
            barrier = pltpu.get_barrier_semaphore()
            pl.semaphore_signal(barrier, inc=1, device_id={"rep": other}, device_id_type=pl.DeviceIdType.MESH)
            hail((right, left))
            pl.semaphore_wait(barrier, 3)
            for copy in (*moments(), *exchange(False)):
                copy.start()
            squares[...] = jnp.zeros_like(squares)

        @pl.when(c > 0)
        def _():
            ring.begin((0, 3))

        for copy in weights(c, here):
            copy.wait()

        @pl.when(c < chunks - 1)
        def _():
            for copy in weights(c + 1, there):
                copy.start()

    @pl.when((c < chunks - 1) | (i < tiles - 1))
    def _():
        for load in loads(lax.rem(i + 1, tiles)):
            load.start()

    for load in loads(i):
        load.wait()
    a, a_t, dy, dy_t = (part.at[lax.rem(i, 2)] for part in slots)
    rows = pl.ds(pl.multiple_of(i * tm, tm), tm)
    pair = 2

    def work(at_end):
        parts = []
        for j in range(0, n, pair):
            to = slice(j * STRIPE, (j + pair) * STRIPE)
            w1, w2 = wg_part[here, :, to], wu_part[here, :, to]
            w3 = wd[0, j : j + pair, 0].reshape(pair * STRIPE, wd.shape[4])
            parts.append((to, w1, w2, dot(a[...], w1), dot(a[...], w2), dot_nt(dy[...], w3)))

        def states(fresh, dg, du, w1, w2):
            more = dot_nt(jnp.concatenate([dg, du], 1), jnp.concatenate([w1, w2], 1))
            da[rows, :] = jnp.where(fresh, 0.0, da[rows, :]) + more

        def weight_gradients(to, act, dg, du):
            for acc, left, right in ((gacc, a_t, dg), (uacc, a_t, du), (dacc, dy_t, act)):
                acc[:, to] = jnp.where(i == 0, 0.0, acc[:, to]) + dot(left[...], right)

        later = []
        for k, (to, w1, w2, g, u, dact) in enumerate(parts):
            fresh = (c == 0) & (k == 0)
            act, dg, du = backward_parts(g, u, dact)
            if at_end:
                states(fresh, dg, du, w1, w2)
                later.append((to, act, dg, du))
            else:
                weight_gradients(to, act, dg, du)
                states(fresh, dg, du, w1, w2)
        for one in later:
            weight_gradients(*one)
        if at_end:
            out = states_gradient(da[rows, :], h[...], dy[...])
            dh[...] = out
            dh_t[...] = out.T

    pl.when(c < chunks - 1)(lambda: work(False))
    pl.when(c == chunks - 1)(lambda: work(True))
    pl.when((c > 0) & (i == 0))(lambda: ring.begin((1, 4)))

    @pl.when((c > 0) & (i == tiles // 2 - 1))
    def _():
        ring.go_on()

    @pl.when(i == tiles // 2)
    def _():
        @pl.when(c == 1)
        def _():
            for copy in moments():
                copy.wait()
            for copy in exchange(True):
                copy.start()

        @pl.when(c == 2)
        def _():
            for copy in (*exchange(False), *exchange(True)):
                copy.wait()

        for k, (*_, first, at_end) in enumerate(rounds):

            @pl.when((c == first) & (not at_end))
            def _(k=k):
                for copy in out(k):
                    copy.start()

            @pl.when(c == first + 1)
            def _(k=k):
                for copy in out(k):
                    copy.wait()
                for copy in on(k):
                    copy.start()

            if first + 2 < chunks:

                @pl.when(c == first + 2)
                def _(k=k):
                    for copy in on(k):
                        copy.wait()

    @pl.when((c == chunks - 1) & (i == tiles - 1))
    def _():
        for k, (*_, first, _) in enumerate(rounds):
            if first + 2 >= chunks:
                for copy in on(k):
                    copy.wait()

    @pl.when(i == tiles - 1)
    def _():
        @pl.when(c > 0)
        def _():
            ring.end(g_out.at[0], squares)
            ring.sent(*range(6))

        for k, mine in enumerate(mines):

            @pl.when(c == k + 1)
            def _(mine=mine):
                mine[...] = g_out[0, block - mine.shape[0] :]

        for k, (*_, first, at_end) in enumerate(rounds):

            @pl.when((c == first) & at_end)
            def _(k=k):
                for copy in out(k):
                    copy.start()

        lay_out(n, raw, gacc, uacc, dacc)

        @pl.when(c == chunks - 1)
        def _():
            copy = pltpu.make_async_copy(raw, last, local)
            copy.start()
            squares_out[...] = squares[...]
            copy.wait()


def by_owner(n, w_down):
    layers, ff, d = w_down.shape
    return w_down.reshape(layers, n, ff // (n * STRIPE), STRIPE, d)


def top(n, chunks, layer, a, a_t, dy, dy_t, h, w_gate, w_up, w_down, near_a, near_b, tm=1024):
    t, d = a.shape
    width, tiles, block = n * STRIPE, t // tm, 3 * d // n
    assert tiles % 2 == 0
    at_end = lambda c, i: jnp.where(c == chunks - 1, i, 0)
    row_end, col_end = pl.BlockSpec((tm, d), lambda c, i: (at_end(c, i), 0)), pl.BlockSpec((d, tm), lambda c, i: (0, at_end(c, i)))
    down = pl.BlockSpec((1, n, 1, STRIPE, d), lambda c, i: (layer, 0, c, 0, 0))
    shapes = [
        jax.ShapeDtypeStruct((t, d), BF16),
        jax.ShapeDtypeStruct((d, t), BF16),
        jax.ShapeDtypeStruct((chunks - 1, block, width), BF16),
        jax.ShapeDtypeStruct((n, block, width), BF16),
        jax.ShapeDtypeStruct((8, width), F32),
        *(jax.ShapeDtypeStruct((2, one.shape[1] // 2, *one.shape[2:]), F32) for one in (near_a, near_b)),
        *(jax.ShapeDtypeStruct(one.shape[1:], F32) for one in (near_a, near_b)),
        *[jax.ShapeDtypeStruct((3, block, width), BF16)] * EARLY,
        jax.ShapeDtypeStruct((3, block // 3, width), BF16),
    ]
    return pl.pallas_call(
        functools.partial(top_kernel, n, chunks, tiles, layer),
        grid=(chunks, tiles),
        in_specs=[pl.BlockSpec(memory_space=pl.ANY)] * 4 + [row_end, down] + [pl.BlockSpec(memory_space=pl.ANY)] * 4,
        out_specs=[
            row_end,
            col_end,
            pl.BlockSpec((1, block, width), lambda c, i: (jnp.maximum(c - 1, 0), 0, 0)),
            pl.BlockSpec(memory_space=pl.ANY),
            pl.BlockSpec((8, width), lambda c, i: (0, 0)),
        ]
        + [pl.BlockSpec(memory_space=pl.ANY)] * (4 + EARLY_DOWN),
        out_shape=shapes,
        scratch_shapes=[pltpu.VMEM((d, width), F32)] * 3
        + [
            pltpu.VMEM((t, d), F32),
            pltpu.VMEM((n, block, width), BF16),
            pltpu.VMEM((2, 6, block // 2, width), BF16),
            pltpu.VMEM((2, block // 2, width), BF16),
            pltpu.VMEM((8, width), F32),
            pltpu.SemaphoreType.DMA((2, 6)),
            pltpu.SemaphoreType.DMA((2, 6)),
            pltpu.SemaphoreType.DMA,
            pltpu.VMEM((2, d, width), BF16),
            pltpu.VMEM((2, d, width), BF16),
            pltpu.SemaphoreType.DMA((2, 2, n)),
            *[pltpu.VMEM((block, width), BF16)] * EARLY,
            pltpu.VMEM((block // 3, width), BF16),
            pltpu.SemaphoreType.DMA((14, 4)),
            pltpu.SemaphoreType.DMA((14, 4)),
        ]
        + [pltpu.VMEM((2, *one), BF16) for one in ((tm, d), (d, tm)) * 2]
        + [pltpu.SemaphoreType.DMA((4, 2))],
        compiler_params=pltpu.CompilerParams(vmem_limit_bytes=67043328, collective_id=0, has_side_effects=True),
        cost_estimate=cost(16 * t * d * width * chunks, chunks * nbytes(a, a_t, dy, dy_t)),
        name="top",
    )(a, a_t, dy, dy_t, h, by_owner(n, w_down), w_gate, w_up, near_a, near_b)


def bottom_kernel(n, chunks, tiles, *refs):
    wholes, (wd, first, squares_in, g_out, squares_out), refs = refs[:5], refs[5:10], refs[10:]
    gacc, uacc, dacc, raw, got, mid, squares, send, recv, local, all_squares, to, fro, g_part, g_sems, *slots, loaded = refs
    c, i = pl.program_id(0), pl.program_id(1)
    right, opposite, left = neighbours(n)
    tm = slots[0].shape[2]

    def loads(c, i):
        at, slot = pl.ds(pl.multiple_of(i * tm, tm), tm), lax.rem(i, 2)
        tiles_at = ((slice(None), at), (at,), (slice(None), at), (c, at), (c, at))
        for k, (whole, where, part) in enumerate(zip(wholes, tiles_at, slots, strict=True)):
            yield pltpu.make_async_copy(whole.at[*where], part.at[slot], loaded.at[k, slot])

    def ring(k):
        slot = lax.rem(k, 2)
        return Ring(n, raw.at[slot], got.at[k], mid.at[slot], send.at[k], recv.at[k])

    held = pltpu.make_async_copy(first, raw.at[0], local)

    def put(k):
        slot = lax.rem(k, 2)
        return pltpu.make_async_copy(g_part.at[slot], g_out.at[k], g_sems.at[slot])

    def end(k):
        pl.when(k > 1)(lambda: put(k - 2).wait())
        ring(k).end(g_part.at[lax.rem(k, 2)], squares)
        put(k).start()
        ring(k).sent(*range(6))

    @pl.when((c == 0) & (i == 0))
    def _():
        hail((right, opposite, left))
        held.start()
        for load in loads(c, i):
            load.start()
        squares[...] = squares_in[...]
        pl.semaphore_wait(pltpu.get_barrier_semaphore(), 3)
        Ring(n, first, got.at[0], mid.at[0], send.at[0], recv.at[0]).begin((0, 3))

    @pl.when((c > 0) & (i == 0))
    def _():
        ring(c).begin((0, 3))

    @pl.when((c < chunks - 1) | ((c == chunks - 1) & (i < tiles - 1)))
    def _():
        for load in loads(jnp.where(i == tiles - 1, c + 1, c), lax.rem(i + 1, tiles)):
            load.start()

    @pl.when(c < chunks)
    def _():
        for load in loads(c, i):
            load.wait()
        a_t, dy, dy_t, gate, up = (part.at[lax.rem(i, 2)] for part in slots)
        pair = 2
        parts = []
        for j in range(0, n, pair):
            w = wd[0, j : j + pair, 0].reshape(pair * STRIPE, wd.shape[4])
            parts.append((slice(j * STRIPE, (j + pair) * STRIPE), dot_nt(dy[...], w)))
        for to, dact in parts:
            act, dg, du = backward_parts(gate[:, to], up[:, to], dact)
            for acc, left, right in ((gacc, a_t, dg), (uacc, a_t, du), (dacc, dy_t, act)):
                acc[:, to] = jnp.where(i == 0, 0.0, acc[:, to]) + dot(left[...], right)

    @pl.when(i == tiles // 4)
    def _():
        pl.when(c > 0)(lambda: end(c - 1))
        pl.when(c == 0)(held.wait)
        ring(c).begin((1, 4))

    pl.when(i == tiles // 2)(lambda: ring(c).go_on())

    @pl.when((c < chunks) & (i == tiles - 1))
    def _():
        lay_out(n, raw.at[lax.rem(c + 1, 2)], gacc, uacc, dacc)

    @pl.when((c == chunks) & (i == tiles - 1))
    def _():
        end(c)
        me = lax.axis_index("dp")
        lanes = all_squares.shape[2]
        all_squares[me] = sum(squares[:, at : at + lanes] for at in range(0, squares.shape[1], lanes))
        mine = all_squares.at[me]
        copies = [remote(mine, mine, to.at[k], fro.at[k], device) for k, device in enumerate((right, opposite, left))]
        for copy in copies:
            copy.start()
        for copy in copies:
            copy.wait()
        total = all_squares[0]
        for k in range(1, n):
            total += all_squares[k]
        squares_out[...] = total
        put(c - 1).wait()
        put(c).wait()


def bottom(n, chunks, layer, a_t, dy, dy_t, gate, up, w_down, first, squares, tm=1024):
    d, t = a_t.shape
    width, tiles, block = n * STRIPE, t // tm, 3 * d // n
    assert tiles % 2 == 0
    small = pl.BlockSpec((8, width), lambda c, i: (0, 0))
    down = pl.BlockSpec((1, n, 1, STRIPE, d), lambda c, i: (layer, 0, jnp.minimum(c, chunks - 1), 0, 0))
    return pl.pallas_call(
        functools.partial(bottom_kernel, n, chunks, tiles),
        grid=(chunks + 1, tiles),
        in_specs=[pl.BlockSpec(memory_space=pl.ANY)] * 5 + [down, pl.BlockSpec(memory_space=pl.ANY), small],
        out_specs=[pl.BlockSpec(memory_space=pl.ANY), pl.BlockSpec((8, 128), lambda c, i: (0, 0))],
        out_shape=[
            jax.ShapeDtypeStruct((chunks + 1, block, width), BF16),
            jax.ShapeDtypeStruct((8, 128), F32),
        ],
        scratch_shapes=[pltpu.VMEM((d, width), F32)] * 3
        + [
            pltpu.VMEM((2, n, block, width), BF16),
            pltpu.VMEM((chunks + 1, 6, block // 2, width), BF16),
            pltpu.VMEM((2, 2, block // 2, width), BF16),
            pltpu.VMEM((8, width), F32),
            pltpu.SemaphoreType.DMA((chunks + 1, 6)),
            pltpu.SemaphoreType.DMA((chunks + 1, 6)),
            pltpu.SemaphoreType.DMA,
            pltpu.VMEM((n, 8, 128), F32),
            pltpu.SemaphoreType.DMA((3,)),
            pltpu.SemaphoreType.DMA((3,)),
            pltpu.VMEM((2, block, width), BF16),
            pltpu.SemaphoreType.DMA((2,)),
        ]
        + [pltpu.VMEM((2, *one), BF16) for one in ((d, tm), (tm, d), (d, tm))]
        + [pltpu.VMEM((2, tm, width), F32)] * 2
        + [pltpu.SemaphoreType.DMA((5, 2))],
        compiler_params=pltpu.CompilerParams(vmem_limit_bytes=VMEM_LIMIT, collective_id=1, has_side_effects=True),
        cost_estimate=cost(8 * t * d * width * chunks, nbytes(gate, up) + chunks * nbytes(a_t, dy, dy_t)),
        name="bottom",
    )(a_t, dy, dy_t, gate, up, by_owner(n, w_down), first, squares)


def clip(squares, count):
    return jnp.minimum(1.0, 0.5 * lax.rsqrt(jnp.full((1, 1), jnp.sum(squares)) / count + 1e-30))


def adamw(w, m, v, g):
    m = 0.9 * m + 0.1 * g
    v = 0.95 * v + 0.05 * g * g
    old = w.astype(F32)
    step = m * lax.rsqrt(v + 1e-8) + 0.1 * old
    return (old - 0.02 * step).astype(BF16), m, v


def upright(g):
    return jnp.concatenate([g[:, q : q + STRIPE].T for q in range(0, g.shape[1], STRIPE)], 1)


def adam_kernel(chunks, tall, count, squares, w, m, v, g_top, g_bottom, *refs):
    *w_out, m_out, v_out = refs
    factor = clip(squares[...], count)

    def work(layer, c, g, to):
        def at(c):
            rows = pl.ds(pl.multiple_of(c * STRIPE, STRIPE), STRIPE)
            return (rows, slice(None)) if tall else (slice(None), rows)

        g = upright(g.astype(F32)) if tall else g.astype(F32)
        new, m_new, v_new = adamw(w[layer, *at(c)], m[layer, *at(c)], v[layer, *at(c)], g * factor)
        if to is not None:
            w_out[layer][at(to)] = new
        m_out[layer, *at(c)] = m_new
        v_out[layer, *at(c)] = v_new

    early = EARLY_DOWN if tall else EARLY

    @pl.loop(0, early)
    def _(c):
        work(0, c, g_bottom[c + 1], c)
        work(1, c, g_top[c], None)

    @pl.loop(early, chunks - 1)
    def _(c):
        work(0, c, g_bottom[c + 1], c)
        work(1, c, g_top[c], c - early)

    work(0, chunks - 1, g_bottom[chunks], chunks - 1)
    work(1, chunks - 1, g_bottom[0], chunks - 1 - early)


def adam(me, squares, w, m, v, g_top, g_bottom, which, count, chunks, tall, first, blocks, begun):
    layers, rows, _ = m.shape
    g_rows = g_top.shape[1] // 3
    g_width, width = (2 * STRIPE, 2 * g_rows) if tall else (STRIPE, STRIPE * chunks)
    block = pl.BlockSpec((layers, rows, width), lambda i, me: (0, 0, first + i))
    rest = (EARLY_DOWN if tall else EARLY) * STRIPE
    new = [(rows, width), (rows - rest, width) if tall else (rows, width - rest)]
    out = [jax.ShapeDtypeStruct((r, c * blocks), BF16) for r, c in new] + [jax.ShapeDtypeStruct(m.shape, F32)] * 2
    fixed = list(begun)

    def body(me_ref, *refs):
        adam_kernel(chunks, tall, count, *refs[:6], *refs[6 + len(fixed) :])

    outs = pl.pallas_call(
        body,
        grid_spec=pltpu.PrefetchScalarGridSpec(
            num_scalar_prefetch=1,
            grid=(blocks,),
            in_specs=[pl.BlockSpec(squares.shape, lambda i, me: (0, 0))]
            + [pl.BlockSpec((layers, rows, width), lambda i, me: (0, me[0], first + i)), block, block]
            + [pl.BlockSpec((g.shape[0], g_rows, g_width), lambda i, me: (0, which, first + i)) for g in (g_top, g_bottom)]
            + [pl.BlockSpec(memory_space=pl.ANY)] * len(fixed),
            out_specs=[pl.BlockSpec(one, lambda i, me: (0, i)) for one in new] + [block, block],
        ),
        out_shape=out,
        input_output_aliases={7 + k: layers + k for k in range(len(fixed))},
        compiler_params=params(),
        cost_estimate=cost(16 * rows * width * blocks * layers, 22 * rows * width * blocks * layers),
        name="adam",
    )(me, squares, w, m, v, g_top, g_bottom, *fixed)
    return outs[:layers], outs[layers:]


def early_kernel(n, count, squares, *refs):
    wg, wu, (wd, near_a, near_b, other_a, other_b, far_a, far_b, g_top), refs = refs[:n], refs[n : 2 * n], refs[2 * n : 2 * n + 8], refs[2 * n + 8 :]
    alls, outs, (a, b, g, g_down, loaded, across, down, sems) = refs[:EARLY_DOWN], refs[EARLY_DOWN : EARLY_DOWN + 3], refs[EARLY_DOWN + 3 :]
    rows, each = a.shape[2], EARLY * STRIPE
    _, mine, others = share()
    loads = []
    for k, (part, near, other, far) in enumerate(((a, near_a, other_a, far_a), (b, near_b, other_b, far_b))):
        loads += [(near.at[2], part.at[0]), (far, part.at[2])]
        for turn, side in ((1, 1), (3, 0)):
            loads += [(near.at[side, mine[k]], part.at[turn, mine[k]]), (other.at[side], part.at[turn, others[k]])]
    for k, every in enumerate(alls):
        own = g_top.at[k] if k < EARLY else g_top.at[k, 2 * rows :]
        to = [g.at[turn, k] if k < EARLY else g_down.at[turn] for turn in range(n)]
        loads += zip((own, every.at[1], every.at[2], every.at[0]), to, strict=True)
    loads = [pltpu.make_async_copy(src, dst, loaded.at[k]) for k, (src, dst) in enumerate(loads)]
    for copy in loads:
        copy.start()
    factor = clip(squares[...], count)
    me = lax.axis_index("dp")
    for copy in loads:
        copy.wait()

    @pl.loop(0, n)
    def _(turn):
        o = lax.rem(me + turn, n)
        at = pl.ds(pl.multiple_of(o * rows, rows), rows)
        for k, w in enumerate((wg, wu)):
            for j in range(n):
                to = slice(j * each, (j + 1) * each)
                grad = jnp.concatenate([g[turn, e, k * rows : (k + 1) * rows, j * STRIPE : (j + 1) * STRIPE] for e in range(EARLY)], 1)
                across[k, at, to] = adamw(w[j][0, at, :], a[turn, 2 * k, :, to], a[turn, 2 * k + 1, :, to], grad.astype(F32) * factor)[0]
        for e in range(EARLY_DOWN):
            part = slice(e * STRIPE, (e + 1) * STRIPE)
            grad = upright((g[turn, e, 2 * rows :, :] if e < EARLY else g_down[turn]).astype(F32)) * factor
            down[o, part, :] = adamw(wd[0, o, e], b[turn, 0, part, :], b[turn, 1, part, :], grad)[0]

    copies, whole = [], outs[0].shape[2] // n
    for o in range(n):
        for k in range(2):
            copies.append((across.at[k, :, o * each : (o + 1) * each], outs[k].at[1, :, o * whole : o * whole + each]))
        copies.append((down.at[o], outs[2].at[1, o * whole : o * whole + down.shape[1], :]))
    copies = [pltpu.make_async_copy(src, dst, sems.at[k]) for k, (src, dst) in enumerate(copies)]
    for copy in copies:
        copy.start()
    for copy in copies:
        copy.wait()


def early_step(n, chunks, squares, weights, moments, g_top, alls, count):
    w_gate, w_up, w_down = weights
    d, each = w_gate.shape[1], EARLY * STRIPE
    assert chunks % EARLY == 0 and chunks % EARLY_DOWN == 0
    across = [pl.BlockSpec((1, d, each), lambda i, o=o: (1, 0, o * (chunks // EARLY))) for o in range(n)]
    down = pl.BlockSpec((1, n, EARLY_DOWN, STRIPE, d), lambda i: (1, 0, 0, 0, 0))
    arrays = (*moments, g_top, *alls)
    held = [(n, *one.shape) for one in moments[-2:]]
    return pl.pallas_call(
        functools.partial(early_kernel, n, count),
        grid=(1,),
        in_specs=[pl.BlockSpec(squares.shape, lambda i: (0, 0))] + across + across + [down] + [pl.BlockSpec(memory_space=pl.ANY)] * len(arrays),
        out_specs=[pl.BlockSpec(memory_space=pl.ANY)] * 3,
        out_shape=[jax.ShapeDtypeStruct(w.shape, BF16) for w in weights],
        scratch_shapes=[
            *(pltpu.VMEM(one, F32) for one in held),
            pltpu.VMEM((n, EARLY, *g_top.shape[1:]), BF16),
            pltpu.VMEM((n, *alls[-1].shape[1:]), BF16),
            pltpu.SemaphoreType.DMA((12 + n * EARLY_DOWN,)),
            pltpu.VMEM((2, d, n * each), BF16),
            pltpu.VMEM((n, EARLY_DOWN * STRIPE, d), BF16),
            pltpu.SemaphoreType.DMA((3 * n,)),
        ],
        compiler_params=params(),
        cost_estimate=cost(16 * 3 * d * n * each, nbytes(*moments)),
        name="early",
    )(squares, *[w_gate] * n, *[w_up] * n, by_owner(n, w_down), *arrays)


def place_kernel(n, pieces, regions, *refs):
    arrays, out, sems = refs[: len(pieces)], refs[-2], refs[-1]
    me = lax.axis_index("dp")
    copies = []
    for array, (layer, turn) in zip(arrays, pieces, strict=True):
        o = lax.rem(me + turn, n)
        for from_column, rows_before, columns, region in regions(layer):
            rows = array.shape[0]
            step = rows + rows_before
            to = out.at[layer, pl.ds(pl.multiple_of(o * step + rows_before, 16), rows), region]
            copies.append((array.at[:, from_column : from_column + columns], to))
    copies = [pltpu.make_async_copy(src, dst, sems.at[k]) for k, (src, dst) in enumerate(copies)]
    for copy in copies:
        copy.start()
    for copy in copies:
        copy.wait()


def place(n, chunks, whole, pieces, tall, first, blocks):
    arrays, where = zip(*pieces, strict=True)
    full = STRIPE * chunks

    def regions(layer):
        if tall:
            columns = arrays[0].shape[1]
            return [(0, layer * EARLY_DOWN * STRIPE, columns, slice(first * columns // blocks, (first + blocks) * columns // blocks))]
        there = layer * EARLY * STRIPE
        columns = full - there
        return [(j * columns, 0, columns, slice((first + j) * full + there, (first + j + 1) * full)) for j in range(blocks)]

    return pl.pallas_call(
        functools.partial(place_kernel, n, where, regions),
        grid=(1,),
        in_specs=[pl.BlockSpec(one.shape, lambda i: (0, 0)) for one in arrays] + [pl.BlockSpec(memory_space=pl.ANY)],
        out_specs=pl.BlockSpec(memory_space=pl.ANY),
        out_shape=jax.ShapeDtypeStruct(whole.shape, whole.dtype),
        input_output_aliases={len(arrays): 0},
        scratch_shapes=[pltpu.SemaphoreType.DMA((len(arrays) * blocks,))],
        compiler_params=params(),
        cost_estimate=cost(arrays[0].size, 4 * nbytes(*arrays)),
        name="place",
    )(*arrays, whole)


def send_around(n, own, swap):
    right, left = [(i, (i + 1) % n) for i in range(n)], [(i, (i - 1) % n) for i in range(n)]

    def send(one, way):
        return lax.ppermute(one, "dp", way)

    def in_order(a, b):
        return (b, a) if swap else (a, b)

    a, b = in_order(*own)
    left_a, right_b = send(a, right), send(b, left)
    left_b, right_a = send(b, right), send(a, left)
    return in_order(left_a, left_b), in_order(right_a, right_b), lambda: in_order(send(left_a, right), send(right_b, left))


def solution(mesh):
    n = mesh.shape["dp"]

    def step(x, dy, w_gate, w_up, w_down, m_gate, m_up, m_down, v_gate, v_up, v_down):
        x, dy = x[0], dy[0]
        chunks = w_gate.shape[2] // (n * STRIPE)
        me = lax.axis_index("dp").astype(jnp.int32).reshape(1)

        weights, moments = (w_gate, w_up, w_down), ((m_gate, v_gate), (m_up, v_up), (m_down, v_down))
        *parts, near_a, near_b = forward(n, chunks, x, dy, *weights, sum(moments, ()))
        gate, up, a0_t, h1, a1, a1_t, dy_t = parts
        parts = top(n, chunks, 1, a1, a1_t, dy, dy_t, h1, *weights, near_a, near_b)
        (dh, dh_t, g_top, last, squares), early, alls = parts[:5], parts[5:9], parts[9:]
        g_bottom, squares = bottom(n, chunks, 0, a0_t, dh, dh_t, gate, up, w_down, last, squares)

        new, sent, count = [[], [], []], [], 3 * w_gate.size
        for which, first, blocks, swap in PIECES:
            own, new[which] = adam(
                me, squares, weights[which], *moments[which], g_top, g_bottom, which, count, chunks, which == 2, first, blocks, new[which]
            )
            squares = lax.optimization_barrier((squares, *own))[0]
            sent.append((own, *send_around(n, own, swap)))
        whole = list(early_step(n, chunks, squares, weights, (near_a, near_b, *early), g_top, alls, count))
        for k, (which, first, blocks, swap) in enumerate(PIECES):
            own, left, right, _ = sent[k]
            near = [(one, (layer, turn)) for turn, pair in ((0, own), (n - 1, left), (1, right)) for layer, one in enumerate(pair)]
            whole[which] = place(n, chunks, whole[which], near, which == 2, first, blocks)
        for k, (which, first, blocks, swap) in enumerate(PIECES):
            far = [(one, (layer, 2)) for layer, one in enumerate(sent[k][3]())]
            whole[which] = place(n, chunks, whole[which], far, which == 2, first, blocks)
        return (*whole, *(one[0] for one in new), *(one[1] for one in new))

    seq, part, rows = P(("rep", "dp"), None, None), P("rep", None, None), P("rep", "dp", None)
    state = P(None, "dp", None)
    step = jax.shard_map(
        step,
        mesh=mesh,
        in_specs=(seq, seq) + (P(None, None, None),) * 3 + (state,) * 6,
        out_specs=(part,) * 3 + (rows,) * 6,
        check_vma=False,
    )
    return step
```
